512 devices in a mesh: members: 2 (over y), elem: 64 (over z, core), lev: 4 (over x).
Axes of the slice: x: 4, y: 2, z: 32, core: 2. Of those that a mesh axis runs over, the one named last changes fastest.
The devices are a block of a 4x8x32 slice.
Arguments:
- tracers: float32 [25, 8, 16, 32768], P(None, 'lev', None, ('members', 'elem')), parts along dimension 3, may hold values from -6 to 6
- layer_mass: float32 [8, 16, 32768], P('lev', None, ('members', 'elem')), parts along dimension 2, may hold values from 0.3 to 2.7
- winds: float32 [2, 8, 16, 32768], P(None, 'lev', None, ('members', 'elem')), parts along dimension 3, may hold values from 0.5 to 1.5
- metric: float32 [16, 16384], P(None, 'elem'), may hold values from 0.6 to 1.6
- neighbours: int32 [16384, 8], P('elem'), may hold values from 0 to 16383, as said below
Outputs:
- tracers_out: float32 [25, 8, 16, 32768], P(None, 'lev', None, ('members', 'elem')), parts along dimension 3
- surface: float32 [16, 32768], P(None, ('members', 'elem')), parts along dimension 1
The draws below stay inside these ranges and needn't reach their ends.
There are 2 independent parts, one for each index of `members`. The reference program is written for one: setup_inputs(seed, part) draws one part's arguments, and reference() takes and returns one part's arrays. A program takes and returns all parts, laid end to end along the dimension named above; an argument that names none is the same for every part. Nothing has to cross between parts.
Inputs may be any that keep to these rules, and one draw needn't show every extreme that they name: `neighbours`: the grid has 128 columns and 128 rows of elements; it is periodic north to south, and east of column 127 of row y lies column 0 of row y + 16 (rows modulo 128). Block b of 256 elements along elem is the square patch of 16 by 16 elements in patch row b // 8 and patch column b % 8, its elements in a drawn order; so the east, west, north and south patches of block b are blocks b + 1, b - 1, b + 8, b - 8 and the diagonal ones b + 9, b + 7, b - 7, b - 8 - 1 (all modulo the number of blocks). Adjacency is symmetric.
All inputs are finite; a program needn't handle non-finite values.
Results may differ from the reference program's by a relative error of at most 0.0003.
Values sent between devices are 32-bit elements; how exact they have to be, the bound alone decides.
A program may use at most 128 MiB of HBM per device.

```python
import math
import jax
import jax.numpy as jnp
import numpy as np
from jax import lax

NTRC = 25
PSIDE = 16
E_DEV = 256
PGX = 8
GX = 128
GY = 128
NE = 16384
NLEV = 8
N_ELEM = 64


def draw_layer_mass(key, part):
    first = jax.random.fold_in(key, 0)
    level = jnp.arange(NLEV).astype(jnp.float32)[:, None, None]
    profile = 0.5 * (1.0 + 2.0 * level / max(NLEV - 1, 1))
    rough = jax.random.uniform(first, (NLEV, 16, NE), jnp.float32, 0.8, 1.2)
    return profile * rough


def draw_neighbours(key, part):
    keys = jax.random.split(jax.random.fold_in(key, 7), N_ELEM)

    def shuffle(block_key):
        return jax.random.permutation(block_key, E_DEV).astype(jnp.int32)
    orders = jax.vmap(shuffle)(keys)
    rows_grid = jnp.broadcast_to(jnp.arange(GY, dtype=jnp.int32)[:, None], (GY, GX))
    cols_grid = jnp.broadcast_to(jnp.arange(GX, dtype=jnp.int32)[None, :], (GY, GX))

    def identity_of(column, row):
        device = row // PSIDE * PGX + column // PSIDE
        inside = row % PSIDE * PSIDE + column % PSIDE
        return device * E_DEV + orders[device, inside]

    def beside(step_x, step_y):
        column = cols_grid + step_x
        row = rows_grid + step_y
        row = jnp.where(column >= GX, row + PSIDE, row)
        row = jnp.where(column < 0, row - PSIDE, row)
        return identity_of(column % GX, row % GY)
    table = jnp.stack([beside(1, 0), beside(-1, 0), beside(0, 1), beside(0, -1), beside(1, 1), beside(-1, 1), beside(1, -1), beside(-1, -1)], axis=-1)
    own = identity_of(cols_grid, rows_grid)
    result = jnp.zeros((NE, 8), jnp.int32)
    return result.at[own.reshape(-1)].set(table.reshape(-1, 8))


def steps_of(key, dims, shards, least, top_value):
    def one(position, shards_of):
        draws = jax.random.uniform(jax.random.fold_in(jax.random.fold_in(key, 6), position), (shards_of,), jnp.float32, least / len(shards), top_value / len(shards))
        return jnp.repeat(jnp.exp(draws), dims[position] // shards_of).reshape((-1,) + (1,) * (len(dims) - position - 1))

    loudness = one(*shards[0])
    for cut in shards[1:]:
        loudness = loudness * one(*cut)
    return loudness


def bell_draw(own_key, dims, deviation, limit, cuts=(), held_as=jnp.bfloat16):
    drawn = jax.random.normal(own_key, dims, jnp.float32) * deviation
    if len(cuts) > 0:
        drawn = steps_of(own_key, dims, cuts, -0.22, 0.18) * drawn
    return jnp.clip(drawn, min=-limit, max=limit).astype(held_as)


def setup_inputs(seed: int = 0, part: int = 0) -> dict:
    seeds = jax.random.split(jax.random.key(seed), 6)
    part_splits = jax.random.split(jax.random.fold_in(seeds[5], part), 6)
    tracers = bell_draw(part_splits[0], (NTRC, NLEV, 16, NE), 1.0, 6.0, ((1, 4), (3, 64)), jnp.float32)
    layer_mass = draw_layer_mass(jax.random.fold_in(jax.random.fold_in(seeds[5], part), 71), part)
    winds = jnp.clip(0.5 + 1.0 * jax.random.uniform(part_splits[2], (2, NLEV, 16, NE), jnp.float32) ** steps_of(part_splits[2], (2, NLEV, 16, NE), ((1, 4), (3, 64)), -0.2, 0.2), 0.5, 1.5)
    metric = jnp.clip(jnp.exp(math.log(1.6) - 0.98082923 * jax.random.uniform(seeds[3], (16, NE), jnp.float32) ** steps_of(seeds[3], (16, NE), ((1, 64),), -0.2, 0.2)), 0.6, 1.6)
    neighbours = draw_neighbours(jax.random.fold_in(seeds[5], 71), part)
    return {"tracers": tracers, "layer_mass": layer_mass, "winds": winds, "metric": metric, "neighbours": neighbours}


time_step = 0.035

def lagrange_scale(points, which):
    product = 1.0
    for other in range(4):
        if other != which:
            product = product * (points[which] - points[other])
    return product

def node_tables():
    points = np.array([-1.0, -1.0 / math.sqrt(5.0), 1.0 / math.sqrt(5.0), 1.0])
    weights = np.array([1.0, 5.0, 5.0, 1.0]) / 6.0
    derivative = np.zeros((4, 4))
    for target in range(4):
        for source in range(4):
            if target == source:
                derivative[target, source] = sum((1.0 / (points[target] - points[other]) for other in range(4) if other != target))
            else:
                derivative[target, source] = lagrange_scale(points, target) / (lagrange_scale(points, source) * (points[target] - points[source]))
    return (np.kron(np.eye(4), derivative), np.kron(derivative, np.eye(4)), np.kron(weights, weights))

def side_links():
    column = list(range(4))
    return [([4 * step + 3 for step in column], [4 * step for step in column]), ([4 * step for step in column], [4 * step + 3 for step in column]), ([12 + step for step in column], [step for step in column]), ([step for step in column], [12 + step for step in column]), ([15], [0]), ([12], [3]), ([3], [12]), ([0], [15])]

def apply_table(table, field):
    return jnp.einsum('nm,...me->...ne', jnp.asarray(table, jnp.float32), field, precision=lax.Precision.HIGHEST)

def tendency(state, winds, metric):
    along_east, along_north, weights = node_tables()
    east_flux = metric * winds[0] * state
    north_flux = metric * winds[1] * state
    return -(apply_table(along_east, east_flux) + apply_table(along_north, north_flux)) / metric

def assemble(weighted, extended, positions):
    total = weighted
    for direction, pair in enumerate(side_links()):
        picked = jnp.take(extended[:, pair[1], :], positions[:, direction], axis=2)
        total = total.at[:, pair[0], :].add(picked)
    return total

def assembled_rate(state, winds, metric, mass, shared, neighbours):
    rate = tendency(state, winds, metric)
    flat = (mass * rate).reshape((-1,) + rate.shape[2:])
    return (assemble(flat, flat, neighbours) / shared).reshape(rate.shape)

def reference(tracers, layer_mass, winds, metric, neighbours):
    weights = node_tables()[2]
    mass = jnp.asarray(weights, jnp.float32)[:, None] * metric
    shared = assemble(mass[None], mass[None], neighbours)[0]
    start_state = jnp.concatenate([layer_mass[None], tracers * layer_mass[None]], axis=0)
    middle_state = start_state + time_step * assembled_rate(start_state, winds, metric, mass, shared, neighbours)
    final_state = 0.5 * (start_state + middle_state + time_step * assembled_rate(middle_state, winds, metric, mass, shared, neighbours))
    thick = final_state[0]
    carried = final_state[1:]
    levels = thick.shape[0]
    surface = lax.optimization_barrier(jnp.sum(thick, axis=0))
    edges = jnp.arange(levels + 1).astype(jnp.float32)
    fraction = (edges + edges * (edges - 1.0) / (levels - 1)) / (2.0 * levels)
    layers = edges[:-1]
    share = (1.0 + 2.0 * layers / (levels - 1)) / (2.0 * levels)
    above_mass = jnp.concatenate([jnp.zeros_like(surface)[None], jnp.cumsum(thick, axis=0)], axis=0)
    delta = above_mass - surface * fraction[:, None, None]
    ratio = carried / thick
    padded = jnp.pad(ratio, ((0, 0), (1, 1), (0, 0), (0, 0)))
    flux = delta * jnp.where(delta > 0.0, padded[:, :-1], padded[:, 1:])
    result = (carried + flux[:, :-1] - flux[:, 1:]) / (surface * share[:, None, None])
    return (result, surface)
```

```python
import functools
import math

import jax
import jax.numpy as jnp
import numpy as np
from jax import lax
from jax.experimental import pallas as pl
from jax.experimental.pallas import tpu as pltpu
from jax.sharding import PartitionSpec as P

MESH = pl.DeviceIdType.MESH
PSIDE = 16
ACROSS = 8
NODES = 16
HALF = 128
time_step = 0.035

OPPOSITE = (1, 0, 3, 2, 7, 6, 5, 4)
CORNERS = ((15, 1, 127), (12, 1, 112), (3, 0, 15), (0, 0, 0))


def lagrange_scale(points, which):
    product = 1.0
    for other in range(4):
        if other != which:
            product = product * (points[which] - points[other])
    return product


def node_tables():
    points = np.array([-1.0, -1.0 / math.sqrt(5.0), 1.0 / math.sqrt(5.0), 1.0])
    weights = np.array([1.0, 5.0, 5.0, 1.0]) / 6.0
    derivative = np.zeros((4, 4))
    for target in range(4):
        for source in range(4):
            if target == source:
                derivative[target, source] = sum(
                    1.0 / (points[target] - points[other]) for other in range(4) if other != target
                )
            else:
                derivative[target, source] = lagrange_scale(points, target) / (
                    lagrange_scale(points, source) * (points[target] - points[source])
                )
    return weights, derivative


WEIGHTS, DERIVATIVE = node_tables()
STIFF = WEIGHTS[:, None] * DERIVATIVE


def weighted_difference(f):
    total, gap = f[0] + f[3], f[3] - f[0]
    inner, inner_gap = f[1] + f[2], f[2] - f[1]
    result = [None] * 4
    for i in range(2):
        q = 0.5 * STIFF[i]
        odd = float(q[3] - q[0]) * gap + float(q[2] - q[1]) * inner_gap
        even = float(q[0] + q[3]) * total + float(q[1] + q[2]) * inner
        result[i] = odd + even
        result[3 - i] = odd - even
    return result


def weighted_tendency(h, a, b):
    f = [a[n] * h[n] for n in range(NODES)]
    g = [b[n] * h[n] for n in range(NODES)]
    rows = [weighted_difference(f[4 * j : 4 * j + 4]) for j in range(4)]
    columns = [weighted_difference(g[i::4]) for i in range(4)]
    return [rows[n // 4][n % 4] + columns[n % 4][n // 4] for n in range(NODES)]


def lanes():
    return lax.broadcasted_iota(jnp.int32, (8, HALF), 1)


def sublanes():
    return lax.broadcasted_iota(jnp.int32, (8, HALF), 0)


def roll(x, shift):
    return pltpu.roll(x, (shift + 2 * HALF) % HALF, 1)


def assembled_in_patch(v):
    lane = lanes()
    column = lane % PSIDE
    for half in range(2):
        for j in range(4):
            left, right = v[half][4 * j], v[half][4 * j + 3]
            v[half][4 * j + 3] = right + jnp.where(column < PSIDE - 1, roll(left, -1), 0.0)
            v[half][4 * j] = left + jnp.where(column > 0, roll(right, 1), 0.0)
    edge = HALF - PSIDE
    for i in range(4):
        low = [v[0][i], v[1][i]]
        high = [v[0][12 + i], v[1][12 + i]]
        down = [roll(low[0], -PSIDE), roll(low[1], -PSIDE)]
        up = [roll(high[0], PSIDE), roll(high[1], PSIDE)]
        v[0][12 + i] = high[0] + jnp.where(lane < edge, down[0], down[1])
        v[1][12 + i] = high[1] + jnp.where(lane < edge, down[1], 0.0)
        v[0][i] = low[0] + jnp.where(lane >= PSIDE, up[0], 0.0)
        v[1][i] = low[1] + jnp.where(lane >= PSIDE, up[1], up[0])
    return v


def pack_borders(v, q, send, corners):
    lane, sub = lanes(), sublanes()
    column, block = lane % PSIDE, lane // PSIDE
    group, slot = q // 4, q % 4
    for half in range(2):
        east = west = 0.0
        for j in range(4):
            at = 4 * slot + j
            east = east + jnp.where(column == at, roll(v[half][4 * j + 3], at - (PSIDE - 1)), 0.0)
            west = west + jnp.where(column == at, roll(v[half][4 * j], at), 0.0)
        send[0, group, half] += east
        send[1, group, half] += west
    north = south = 0.0
    for i in range(4):
        at = 4 * (slot % 2) + i
        north = north + jnp.where(
            block == at, roll(v[1][12 + i], PSIDE * at - (HALF - PSIDE)), 0.0
        )
        south = south + jnp.where(block == at, roll(v[0][i], PSIDE * at), 0.0)
    send[2, group, slot // 2] += north
    send[3, group, slot // 2] += south
    result = []
    for k, (node, half, where) in enumerate(CORNERS):
        value = jnp.broadcast_to(v[half][node][:, where : where + 1], (8, HALF))
        result.append(corners[k] + jnp.where(lane == 8 * q + sub, value, 0.0))
    return tuple(result)


def add_borders(v, q, lines, corners):
    lane, sub = lanes(), sublanes()
    column = lane % PSIDE
    group, slot = q // 4, q % 4
    for half in range(2):
        from_east, from_west = lines[0, group, half], lines[1, group, half]
        for j in range(4):
            at = 4 * slot + j
            v[half][4 * j + 3] += jnp.where(
                column == PSIDE - 1, roll(from_east, PSIDE - 1 - at), 0.0
            )
            v[half][4 * j] += jnp.where(column == 0, roll(from_west, -at), 0.0)
    from_north, from_south = lines[2, group, slot // 2], lines[3, group, slot // 2]
    for i in range(4):
        at = 4 * (slot % 2) + i
        v[1][12 + i] += jnp.where(
            lane >= HALF - PSIDE, roll(from_north, HALF - PSIDE - PSIDE * at), 0.0
        )
        v[0][i] += jnp.where(lane < PSIDE, roll(from_south, -PSIDE * at), 0.0)
    for k, (node, half, where) in enumerate(CORNERS):
        row = jnp.broadcast_to(corners[k], (8, HALF))
        value = jnp.sum(jnp.where(lane == 8 * q + sub, row, 0.0), axis=1, keepdims=True)
        v[half][node] += jnp.where(lane == where, value, 0.0)
    return v


def permuted(x, table):
    high = x.astype(jnp.bfloat16)
    rest = x - high.astype(jnp.float32)
    middle = rest.astype(jnp.bfloat16)
    low = (rest - middle.astype(jnp.float32)).astype(jnp.bfloat16)
    dot = functools.partial(jnp.dot, preferred_element_type=jnp.float32)
    return dot(high, table) + dot(middle, table) + dot(low, table)


def halves(x):
    return [x[:, :HALF], x[:, HALF:]]


def kernel(
    n_elem,
    n_lev,
    trc,
    thickness,
    winds,
    metric,
    beside,
    out,
    surf,
    near,
    raw,
    small_raw,
    small,
    tables,
    state,
    rate,
    coef,
    mixed_coef,
    mass,
    shared,
    scale,
    line_send,
    line_recv,
    corner_send,
    corner_recv,
    thick,
    last,
    inverse,
    column,
    columns,
    ratio,
    ratio_recv,
    last_ratio,
    last_recv,
    delta,
    result,
    last_rows,
    in_sem,
    small_sem,
    out_sem,
    line_ssem,
    line_rsem,
    column_ssem,
    column_rsem,
    ratio_ssem,
    ratio_rsem,
):
    place, level = lax.axis_index("elem"), lax.axis_index("lev")
    width = 2 * HALF
    offsets = (
        1,
        -1,
        ACROSS,
        -ACROSS,
        ACROSS + 1,
        ACROSS - 1,
        1 - ACROSS,
        -1 - ACROSS,
    )
    targets = [{"elem": lax.rem(place + offset + n_elem, n_elem)} for offset in offsets]
    peers = [{"lev": lax.rem(level + k, n_lev)} for k in range(1, n_lev)]

    barrier = pltpu.get_barrier_semaphore()
    for target in targets + peers:
        pl.semaphore_signal(barrier, inc=1, device_id=target, device_id_type=MESH)

    near_copy = pltpu.make_async_copy(beside, near, small_sem.at[0])
    near_copy.start()
    pieces = [
        (trc.at[pl.ds(768, 32)], 0, 32),
        (thickness, 32, 32),
        (winds, 64, 64),
        (metric, 128, 16),
    ]
    small_copies = []
    for k, (source, start, size) in enumerate(pieces):
        copy = pltpu.make_async_copy(
            source, small_raw.at[pl.ds(start, size)], small_sem.at[k + 1]
        )
        copy.start()
        small_copies.append(copy)
    in_copies = []
    for half in range(2):
        copy = pltpu.make_async_copy(
            trc.at[pl.ds(0, 768), pl.ds(HALF * half, HALF)], raw.at[half], in_sem.at[half]
        )
        copy.start()
        in_copies.append(copy)

    line_send[...] = jnp.zeros_like(line_send)

    @pl.when(level == 0)
    def _():
        ratio_recv[:, 1] = jnp.zeros_like(ratio_recv[:, 1])
        last_recv[1] = jnp.zeros_like(last_recv[1])

    @pl.when(level == n_lev - 1)
    def _():
        ratio_recv[:, 0] = jnp.zeros_like(ratio_recv[:, 0])
        last_recv[0] = jnp.zeros_like(last_recv[0])

    near_copy.wait()
    dot = functools.partial(jnp.dot, preferred_element_type=jnp.float32)
    element = lax.broadcasted_iota(jnp.int32, (width, width), 0)
    own = near[...] - place * width
    spots = []
    for side in (1, 3):
        step = jnp.where(own[side : side + 1, :] == element, 1.0, 0.0).astype(jnp.bfloat16)
        count = dot(jnp.ones((8, width), jnp.bfloat16), step)
        for doubling in range(4):
            count = count + dot(count.astype(jnp.bfloat16), step)
            if doubling < 3:
                step = dot(step, step).astype(jnp.bfloat16)
        spots.append(count)
    spot = (spots[0] + PSIDE * spots[1]).astype(jnp.int32)[0:1, :]
    to_drawn = jnp.where(spot == element, 1.0, 0.0)
    tables[1] = to_drawn.astype(jnp.bfloat16)
    tables[0] = jnp.transpose(to_drawn).astype(jnp.bfloat16)

    for copy in small_copies:
        copy.wait()
    small[...] = permuted(small_raw[...], tables[0])
    node = lax.broadcasted_iota(jnp.int32, (NODES, width), 0)
    point_i, point_j = node % 4, node // 4
    ends, inside = float(WEIGHTS[0]), float(WEIGHTS[1])
    weight_i = jnp.where((point_i == 0) | (point_i == 3), ends, inside)
    weight_j = jnp.where((point_j == 0) | (point_j == 3), ends, inside)
    area = small[pl.ds(128, NODES), :]
    mass[...] = weight_i * weight_j * area
    for l in range(2):
        coef[0, l] = -(weight_j * area) * small[pl.ds(64 + 16 * l, NODES), :]
        coef[1, l] = -(weight_i * area) * small[pl.ds(96 + 16 * l, NODES), :]

    for copy in in_copies:
        copy.wait()

    def take_in(q, carry):
        t, l = q // 2, q % 2
        x = jnp.concatenate(
            [
                jnp.concatenate(
                    [
                        raw[half, pl.ds(256 * t + 16 * l + n, 8, stride=32), :]
                        for n in range(NODES)
                    ],
                    axis=0,
                )
                for half in range(2)
            ],
            axis=1,
        )
        y = permuted(x, tables[0])
        for n in range(NODES):
            layer = small[pl.ds(32 + 16 * l + n, 1), :]
            state[q, n] = y[8 * n : 8 * n + 8] * layer
        return carry

    lax.fori_loop(0, 6, take_in, 0, unroll=True)
    wide_sub = lax.broadcasted_iota(jnp.int32, (8, width), 0)
    for n in range(NODES):
        tile = jnp.zeros((8, width), jnp.float32)
        for l in range(2):
            layer = small[pl.ds(32 + 16 * l + n, 1), :]
            tile = jnp.where(wide_sub == 2 * l, small[pl.ds(16 * l + n, 1), :] * layer, tile)
            tile = jnp.where(wide_sub == 2 * l + 1, layer, tile)
        state[6, n] = tile
        for k in range(2):
            mixed_coef[k, n] = jnp.where(
                wide_sub < 2, coef[k, 0, pl.ds(n, 1), :], coef[k, 1, pl.ds(n, 1), :]
            )

    def level_coef(l, half):
        at = pl.ds(HALF * half, HALF)
        return [[coef[k, l, pl.ds(n, 1), at] for n in range(NODES)] for k in range(2)]

    def both_coef(half):
        at = pl.ds(HALF * half, HALF)
        return [[mixed_coef[k, n, :, at] for n in range(NODES)] for k in range(2)]

    def load(ref, q):
        return [
            [ref[q, n, :, pl.ds(HALF * half, HALF)] for n in range(NODES)] for half in range(2)
        ]

    def save(ref, q, v):
        for half in range(2):
            for n in range(NODES):
                ref[q, n, :, pl.ds(HALF * half, HALF)] = v[half][n]

    def scaled(half):
        at = pl.ds(HALF * half, HALF)
        return [scale[pl.ds(n, 1), at] for n in range(NODES)]

    def tend(q, h, stage, corners, mixed):
        v = []
        for half in range(2):
            a, b = both_coef(half) if mixed else level_coef(q % 2, half)
            rates = weighted_tendency(h[half], a, b)
            if mixed:
                at = pl.ds(HALF * half, HALF)
                rates = [
                    jnp.where(sublanes() == 4, mass[pl.ds(n, 1), at], rates[n])
                    for n in range(NODES)
                ]
            v.append(rates)
        v = assembled_in_patch(v)
        save(rate, q, v)
        return pack_borders(v, q, line_send.at[stage], corners)

    def exchange(stage):
        copies = []
        for side, target in enumerate(targets):
            if side < 4:
                source = line_send.at[stage, side]
                landing = line_recv.at[stage, OPPOSITE[side]]
            else:
                source = corner_send.at[stage, side - 4]
                landing = corner_recv.at[stage, OPPOSITE[side] - 4]
            copy = pltpu.make_async_remote_copy(
                src_ref=source,
                dst_ref=landing,
                send_sem=line_ssem.at[stage, side],
                recv_sem=line_rsem.at[stage, OPPOSITE[side]],
                device_id=target,
                device_id_type=MESH,
            )
            copy.start()
            copies.append(copy)
        return copies

    def put_corners(stage, corners):
        for k in range(4):
            corner_send[stage, k] = jnp.sum(corners[k], axis=0, keepdims=True)

    def complete(q, stage):
        borders = [corner_recv[stage, k] for k in range(4)]
        return add_borders(load(rate, q), q, line_recv.at[stage], borders)

    no_corners = tuple(jnp.zeros((8, HALF), jnp.float32) for _ in range(4))

    corners = lax.fori_loop(
        0, 6, lambda q, c: tend(q, load(state, q), 0, c, False), no_corners, unroll=True
    )
    corners = tend(6, load(state, 6), 0, corners, True)
    put_corners(0, corners)
    pl.semaphore_wait(barrier, len(targets) + len(peers))
    sends = exchange(0)
    for copy in sends:
        copy.wait_recv()

    v = complete(6, 0)
    for half in range(2):
        for n in range(NODES):
            shared[pl.ds(n, 1), pl.ds(HALF * half, HALF)] = v[half][n][4:5, :]
    scale[...] = time_step / shared[...]

    def advance(q, v, corners, mixed):
        h = load(state, q)
        for half in range(2):
            c = scaled(half)
            for n in range(NODES):
                middle = h[half][n] + c[n] * v[half][n]
                state[q, n, :, pl.ds(HALF * half, HALF)] = h[half][n] + middle
                h[half][n] = middle
        return tend(q, h, 1, corners, mixed)

    corners = advance(6, v, no_corners, True)
    corners = lax.fori_loop(
        0, 6, lambda q, c: advance(q, complete(q, 0), c, False), corners, unroll=True
    )
    put_corners(1, corners)
    second_sends = exchange(1)
    for copy in second_sends:
        copy.wait_recv()

    def finish(q):
        v = complete(q, 1)
        h = load(state, q)
        for half in range(2):
            c = scaled(half)
            for n in range(NODES):
                h[half][n] = 0.5 * (h[half][n] + c[n] * v[half][n])
        return h

    h = finish(6)
    for half in range(2):
        at = pl.ds(HALF * half, HALF)
        for n in range(NODES):
            for l in range(2):
                last[l, pl.ds(n, 1), at] = h[half][n][2 * l : 2 * l + 1, :]
                thick[l, pl.ds(n, 1), at] = h[half][n][2 * l + 1 : 2 * l + 2, :]
    column[...] = thick[0] + thick[1]
    column_copies = []
    for k, peer in enumerate(peers):
        copy = pltpu.make_async_remote_copy(
            src_ref=column,
            dst_ref=columns.at[k],
            send_sem=column_ssem.at[k],
            recv_sem=column_rsem.at[k],
            device_id=peer,
            device_id_type=MESH,
        )
        copy.start()
        column_copies.append(copy)

    below = {"lev": lax.rem(level + n_lev - 1, n_lev)}
    above = {"lev": lax.rem(level + 1, n_lev)}

    def ratio_copy(t, l):
        return pltpu.make_async_remote_copy(
            src_ref=last_ratio.at[l] if t == 3 else ratio.at[t, l],
            dst_ref=last_recv.at[l] if t == 3 else ratio_recv.at[t, l],
            send_sem=ratio_ssem.at[t, l],
            recv_sem=ratio_rsem.at[t, l],
            device_id=below if l == 0 else above,
            device_id_type=MESH,
        )

    has_below, has_above = level > 0, level < n_lev - 1

    def send_ratios(t):
        pl.when(has_below)(lambda: ratio_copy(t, 0).start())
        pl.when(has_above)(lambda: ratio_copy(t, 1).start())

    for l in range(2):
        inverse[l] = 1.0 / thick[l]
        last_ratio[l] = last[l] * inverse[l]
    send_ratios(3)

    for t in range(3):

        def edge(l, carry, t=t):
            q = 2 * t + l
            h = finish(q)
            for half in range(2):
                at = pl.ds(HALF * half, HALF)
                for n in range(NODES):
                    state[q, n, :, at] = h[half][n]
                    ratio[t, l, n, :, at] = h[half][n] * inverse[l, pl.ds(n, 1), at]
            return carry

        lax.fori_loop(0, 2, edge, 0, unroll=True)
        send_ratios(t)

    for copy in column_copies:
        copy.wait_recv()
    own_column = column[...]
    total = own_column
    under = jnp.zeros_like(own_column)
    for k in range(1, n_lev):
        part = columns[k - 1]
        total = total + part
        under = under + jnp.where(k <= level, part, 0.0)
    surface_rows = total
    levels = 2 * n_lev

    def as_float(k):
        return k.astype(jnp.float32)

    for k in range(3):
        edge_level = as_float(2 * level + k)
        fraction = (edge_level + edge_level * (edge_level - 1.0) * (1.0 / (levels - 1))) * (
            0.5 / levels
        )
        if k > 0:
            under = under + thick[k - 1]
        delta[k] = under - surface_rows * fraction
    for l in range(2):
        share = (1.0 + 2.0 * as_float(2 * level + l) * (1.0 / (levels - 1))) * (0.5 / levels)
        delta[3 + l] = 1.0 / (surface_rows * share)

    def wait_ratios(t):
        pl.when(has_above)(lambda: ratio_copy(t, 0).wait_recv())
        pl.when(has_below)(lambda: ratio_copy(t, 1).wait_recv())

    def remapped(d, carried, own_ratio, ratio_above, ratio_below):
        low = d[0] * jnp.where(d[0] > 0.0, ratio_below, own_ratio[0])
        middle = d[1] * jnp.where(d[1] > 0.0, own_ratio[0], own_ratio[1])
        high = d[2] * jnp.where(d[2] > 0.0, own_ratio[1], ratio_above)
        return (carried[0] + low - middle) * d[3], (carried[1] + middle - high) * d[4]

    wait_ratios(3)
    d = [delta[k] for k in range(5)]
    first, second = remapped(
        d, [last[0], last[1]], [last_ratio[0], last_ratio[1]], last_recv[0], last_recv[1]
    )
    rows = permuted(jnp.concatenate([first, second, surface_rows], axis=0), tables[1])
    last_rows[...] = rows
    out_copies = [
        pltpu.make_async_copy(last_rows.at[pl.ds(32, 16)], surf, out_sem.at[3, 0]),
        pltpu.make_async_copy(
            last_rows.at[pl.ds(0, 32)], out.at[pl.ds(768, 32)], out_sem.at[3, 1]
        ),
    ]
    for copy in out_copies:
        copy.start()

    for t in range(3):
        wait_ratios(t)
        pairs = []
        for n in range(NODES):
            d = [delta[k, pl.ds(n, 1), :] for k in range(5)]
            pairs.append(
                remapped(
                    d,
                    [state[2 * t, n], state[2 * t + 1, n]],
                    [ratio[t, 0, n], ratio[t, 1, n]],
                    ratio_recv[t, 0, n],
                    ratio_recv[t, 1, n],
                )
            )
        for l in range(2):
            tiles = permuted(jnp.concatenate([pair[l] for pair in pairs], axis=0), tables[1])
            for n in range(NODES):
                for half in range(2):
                    result[half, pl.ds(256 * t + 16 * l + n, 8, stride=32), :] = tiles[
                        8 * n : 8 * n + 8, HALF * half : HALF * half + HALF
                    ]
        rows = pl.ds(256 * t, 256)
        for half in range(2):
            copy = pltpu.make_async_copy(
                result.at[half, rows],
                out.at[rows, pl.ds(HALF * half, HALF)],
                out_sem.at[t, half],
            )
            copy.start()
            out_copies.append(copy)

    for copy in out_copies:
        copy.wait()
    for copy in sends + second_sends + column_copies:
        copy.wait_send()
    for t in range(4):
        pl.when(has_below)(lambda t=t: ratio_copy(t, 0).wait_send())
        pl.when(has_above)(lambda t=t: ratio_copy(t, 1).wait_send())


def per_device(n_elem, n_lev, tracers, layer_mass, winds, metric, neighbours):
    width = metric.shape[-1]
    f32 = jnp.float32
    any_spec = pl.BlockSpec(memory_space=pl.ANY)
    tile = (NODES, 8, width)
    dma = pltpu.SemaphoreType.DMA
    scratch = [
        pltpu.VMEM((8, width), jnp.int32),
        pltpu.VMEM((2, 768, HALF), f32),
        pltpu.VMEM((144, width), f32),
        pltpu.VMEM((144, width), f32),
        pltpu.VMEM((2, width, width), jnp.bfloat16),
        pltpu.VMEM((7,) + tile, f32),
        pltpu.VMEM((7,) + tile, f32),
        pltpu.VMEM((2, 2, NODES, width), f32),
        pltpu.VMEM((2,) + tile, f32),
        pltpu.VMEM((NODES, width), f32),
        pltpu.VMEM((NODES, width), f32),
        pltpu.VMEM((NODES, width), f32),
        pltpu.VMEM((2, 4, 2, 2, 8, HALF), f32),
        pltpu.VMEM((2, 4, 2, 2, 8, HALF), f32),
        pltpu.VMEM((2, 4, 1, HALF), f32),
        pltpu.VMEM((2, 4, 1, HALF), f32),
        pltpu.VMEM((2, NODES, width), f32),
        pltpu.VMEM((2, NODES, width), f32),
        pltpu.VMEM((2, NODES, width), f32),
        pltpu.VMEM((NODES, width), f32),
        pltpu.VMEM((n_lev - 1, NODES, width), f32),
        pltpu.VMEM((3, 2) + tile, f32),
        pltpu.VMEM((3, 2) + tile, f32),
        pltpu.VMEM((2, NODES, width), f32),
        pltpu.VMEM((2, NODES, width), f32),
        pltpu.VMEM((5, NODES, width), f32),
        pltpu.VMEM((2, 768, HALF), f32),
        pltpu.VMEM((3 * NODES, width), f32),
        dma((2,)),
        dma((5,)),
        dma((4, 2)),
        dma((2, 8)),
        dma((2, 8)),
        dma((n_lev - 1,)),
        dma((n_lev - 1,)),
        dma((4, 2)),
        dma((4, 2)),
    ]
    out, surface = pl.pallas_call(
        functools.partial(kernel, n_elem, n_lev),
        out_shape=(
            jax.ShapeDtypeStruct((800, width), f32),
            jax.ShapeDtypeStruct((NODES, width), f32),
        ),
        in_specs=[any_spec] * 5,
        out_specs=(any_spec, any_spec),
        scratch_shapes=scratch,
        compiler_params=pltpu.CompilerParams(collective_id=0, has_side_effects=True),
        name="transport",
    )(
        tracers.reshape(-1, width),
        layer_mass.reshape(-1, width),
        winds.reshape(-1, width),
        metric,
        jnp.transpose(neighbours),
    )
    return out.reshape(tracers.shape), surface


def solution(mesh):
    placed = (
        P(None, "lev", None, ("members", "elem")),
        P("lev", None, ("members", "elem")),
        P(None, "lev", None, ("members", "elem")),
        P(None, "elem"),
        P("elem", None),
    )
    return jax.shard_map(
        functools.partial(per_device, mesh.shape["elem"], mesh.shape["lev"]),
        mesh=mesh,
        in_specs=placed,
        out_specs=(P(None, "lev", None, ("members", "elem")), P(None, ("members", "elem"))),
        check_vma=False,
    )
```

```python
import functools
import math

import jax
import jax.numpy as jnp
import numpy as np
from jax import lax
from jax.experimental import pallas as pl
from jax.experimental.pallas import tpu as pltpu
from jax.sharding import PartitionSpec as P

MESH = pl.DeviceIdType.MESH
PSIDE = 16
ACROSS = 8
NODES = 16
HALF = 128
time_step = 0.035

OPPOSITE = (1, 0, 3, 2, 7, 6, 5, 4)
CORNERS = ((15, 1, 127), (12, 1, 112), (3, 0, 15), (0, 0, 0))


def lagrange_scale(points, which):
    product = 1.0
    for other in range(4):
        if other != which:
            product = product * (points[which] - points[other])
    return product


def node_tables():
    points = np.array([-1.0, -1.0 / math.sqrt(5.0), 1.0 / math.sqrt(5.0), 1.0])
    weights = np.array([1.0, 5.0, 5.0, 1.0]) / 6.0
    derivative = np.zeros((4, 4))
    for target in range(4):
        for source in range(4):
            if target == source:
                derivative[target, source] = sum(
                    1.0 / (points[target] - points[other]) for other in range(4) if other != target
                )
            else:
                derivative[target, source] = lagrange_scale(points, target) / (
                    lagrange_scale(points, source) * (points[target] - points[source])
                )
    return weights, derivative


WEIGHTS, DERIVATIVE = node_tables()
STIFF = WEIGHTS[:, None] * DERIVATIVE


def weighted_difference(f):
    total, gap = f[0] + f[3], f[3] - f[0]
    inner, inner_gap = f[1] + f[2], f[2] - f[1]
    result = [None] * 4
    for i in range(2):
        q = 0.5 * STIFF[i]
        odd = float(q[3] - q[0]) * gap + float(q[2] - q[1]) * inner_gap
        even = float(q[0] + q[3]) * total + float(q[1] + q[2]) * inner
        result[i] = odd + even
        result[3 - i] = odd - even
    return result


def weighted_tendency(h, a, b):
    f = [a[n] * h[n] for n in range(NODES)]
    g = [b[n] * h[n] for n in range(NODES)]
    rows = [weighted_difference(f[4 * j : 4 * j + 4]) for j in range(4)]
    columns = [weighted_difference(g[i::4]) for i in range(4)]
    return [rows[n // 4][n % 4] + columns[n % 4][n // 4] for n in range(NODES)]


def lanes():
    return lax.broadcasted_iota(jnp.int32, (8, HALF), 1)


def sublanes():
    return lax.broadcasted_iota(jnp.int32, (8, HALF), 0)


def roll(x, shift):
    return pltpu.roll(x, (shift + 2 * HALF) % HALF, 1)


def assembled_in_patch(v):
    lane = lanes()
    column = lane % PSIDE
    for half in range(2):
        for j in range(4):
            left, right = v[half][4 * j], v[half][4 * j + 3]
            v[half][4 * j + 3] = right + jnp.where(column < PSIDE - 1, roll(left, -1), 0.0)
            v[half][4 * j] = left + jnp.where(column > 0, roll(right, 1), 0.0)
    edge = HALF - PSIDE
    for i in range(4):
        low = [v[0][i], v[1][i]]
        high = [v[0][12 + i], v[1][12 + i]]
        down = [roll(low[0], -PSIDE), roll(low[1], -PSIDE)]
        up = [roll(high[0], PSIDE), roll(high[1], PSIDE)]
        v[0][12 + i] = high[0] + jnp.where(lane < edge, down[0], down[1])
        v[1][12 + i] = high[1] + jnp.where(lane < edge, down[1], 0.0)
        v[0][i] = low[0] + jnp.where(lane >= PSIDE, up[0], 0.0)
        v[1][i] = low[1] + jnp.where(lane >= PSIDE, up[1], up[0])
    return v


def lines_of(v, slot):
    lane = lanes()
    column, block = lane % PSIDE, lane // PSIDE
    found = []
    for half in range(2):
        east = west = 0.0
        for j in range(4):
            at = 4 * slot + j
            east = east + jnp.where(column == at, roll(v[half][4 * j + 3], at - (PSIDE - 1)), 0.0)
            west = west + jnp.where(column == at, roll(v[half][4 * j], at), 0.0)
        found += [(0, half, east), (1, half, west)]
    north = south = 0.0
    for i in range(4):
        at = 4 * (slot % 2) + i
        north = north + jnp.where(
            block == at, roll(v[1][12 + i], PSIDE * at - (HALF - PSIDE)), 0.0
        )
        south = south + jnp.where(block == at, roll(v[0][i], PSIDE * at), 0.0)
    return found + [(2, slot // 2, north), (3, slot // 2, south)]


def corners_of(v, slot, corners):
    lane, sub = lanes(), sublanes()
    result = []
    for k, (node, half, where) in enumerate(CORNERS):
        value = jnp.broadcast_to(v[half][node][:, where : where + 1], (8, HALF))
        result.append(corners[k] + jnp.where(lane == 8 * slot + sub, value, 0.0))
    return tuple(result)


def placed_lines(slot, lines):
    lane = lanes()
    column = lane % PSIDE
    found = []
    for half in range(2):
        east, west = lines[0, half], lines[1, half]
        for j in range(4):
            at = 4 * slot + j
            found.append((half, 4 * j + 3, column == PSIDE - 1, roll(east, PSIDE - 1 - at)))
            found.append((half, 4 * j, column == 0, roll(west, -at)))
    north, south = lines[2, slot // 2], lines[3, slot // 2]
    for i in range(4):
        at = 4 * (slot % 2) + i
        found.append(
            (1, 12 + i, lane >= HALF - PSIDE, roll(north, HALF - PSIDE - PSIDE * at))
        )
        found.append((0, i, lane < PSIDE, roll(south, -PSIDE * at)))
    return found


def borders_of(slot, lines, corners):
    lane, sub = lanes(), sublanes()
    extra = [{}, {}]
    found = placed_lines(slot, lines)
    for k, (node, half, where) in enumerate(CORNERS):
        row = jnp.broadcast_to(corners[k], (8, HALF))
        value = jnp.sum(jnp.where(lane == 8 * slot + sub, row, 0.0), axis=1, keepdims=True)
        found.append((half, node, lane == where, value))
    for half, node, mask, value in found:
        part = jnp.where(mask, value, 0.0)
        extra[half][node] = extra[half][node] + part if node in extra[half] else part
    return extra


def permuted(x, table):
    high = x.astype(jnp.bfloat16)
    rest = x - high.astype(jnp.float32)
    middle = rest.astype(jnp.bfloat16)
    low = (rest - middle.astype(jnp.float32)).astype(jnp.bfloat16)
    dot = functools.partial(jnp.dot, preferred_element_type=jnp.float32)
    return dot(high, table) + dot(middle, table) + dot(low, table)


def halves(x):
    return [x[:, :HALF], x[:, HALF:]]


def kernel(
    n_elem,
    n_lev,
    trc,
    thickness,
    winds,
    metric,
    beside,
    out,
    surf,
    near,
    raw,
    small_raw,
    small,
    tables,
    state,
    rate,
    coef,
    mixed_coef,
    mass,
    shared,
    scale,
    line_send,
    line_recv,
    corner_send,
    corner_recv,
    thick,
    last,
    inverse,
    column,
    columns,
    ratio,
    ratio_recv,
    last_ratio,
    last_recv,
    edge_send,
    edge_recv,
    delta,
    result,
    last_rows,
    in_sem,
    small_sem,
    out_sem,
    line_ssem,
    line_rsem,
    column_ssem,
    column_rsem,
    ratio_ssem,
    ratio_rsem,
    edge_ssem,
    edge_rsem,
):
    place, level = lax.axis_index("elem"), lax.axis_index("lev")
    width = 2 * HALF
    offsets = (
        1,
        -1,
        ACROSS,
        -ACROSS,
        ACROSS + 1,
        ACROSS - 1,
        1 - ACROSS,
        -1 - ACROSS,
    )
    targets = [{"elem": lax.rem(place + offset + n_elem, n_elem)} for offset in offsets]
    peers = [{"lev": lax.rem(level + k, n_lev)} for k in range(1, n_lev)]

    barrier = pltpu.get_barrier_semaphore()
    for target in targets + peers:
        pl.semaphore_signal(barrier, inc=1, device_id=target, device_id_type=MESH)

    near_copy = pltpu.make_async_copy(beside, near, small_sem.at[0])
    near_copy.start()
    pieces = [
        (trc.at[pl.ds(768, 32)], 0, 32),
        (thickness, 32, 32),
        (winds, 64, 64),
        (metric, 128, 16),
    ]
    small_copies = []
    for k, (source, start, size) in enumerate(pieces):
        copy = pltpu.make_async_copy(
            source, small_raw.at[pl.ds(start, size)], small_sem.at[k + 1]
        )
        copy.start()
        small_copies.append(copy)
    in_copies = []
    for half in range(2):
        copy = pltpu.make_async_copy(
            trc.at[pl.ds(0, 768), pl.ds(HALF * half, HALF)], raw.at[half], in_sem.at[half]
        )
        copy.start()
        in_copies.append(copy)

    line_send[...] = jnp.zeros_like(line_send)
    edge_send[...] = jnp.zeros_like(edge_send)

    @pl.when(level == 0)
    def _():
        edge_recv[1] = jnp.zeros_like(edge_recv[1])
        ratio_recv[:, 1] = jnp.zeros_like(ratio_recv[:, 1])
        last_recv[1] = jnp.zeros_like(last_recv[1])

    @pl.when(level == n_lev - 1)
    def _():
        edge_recv[0] = jnp.zeros_like(edge_recv[0])
        ratio_recv[:, 0] = jnp.zeros_like(ratio_recv[:, 0])
        last_recv[0] = jnp.zeros_like(last_recv[0])

    near_copy.wait()
    dot = functools.partial(jnp.dot, preferred_element_type=jnp.float32)
    element = lax.broadcasted_iota(jnp.int32, (width, width), 0)
    own = near[...] - place * width
    spots = []
    for side in (1, 3):
        step = jnp.where(own[side : side + 1, :] == element, 1.0, 0.0).astype(jnp.bfloat16)
        count = dot(jnp.ones((8, width), jnp.bfloat16), step)
        for doubling in range(4):
            count = count + dot(count.astype(jnp.bfloat16), step)
            if doubling < 3:
                step = dot(step, step).astype(jnp.bfloat16)
        spots.append(count)
    spot = (spots[0] + PSIDE * spots[1]).astype(jnp.int32)[0:1, :]
    to_drawn = jnp.where(spot == element, 1.0, 0.0)
    tables[1] = to_drawn.astype(jnp.bfloat16)
    tables[0] = jnp.transpose(to_drawn).astype(jnp.bfloat16)

    for copy in small_copies:
        copy.wait()
    small[...] = permuted(small_raw[...], tables[0])
    node = lax.broadcasted_iota(jnp.int32, (NODES, width), 0)
    point_i, point_j = node % 4, node // 4
    ends, inside = float(WEIGHTS[0]), float(WEIGHTS[1])
    weight_i = jnp.where((point_i == 0) | (point_i == 3), ends, inside)
    weight_j = jnp.where((point_j == 0) | (point_j == 3), ends, inside)
    area = small[pl.ds(128, NODES), :]
    mass[...] = weight_i * weight_j * area
    for l in range(2):
        coef[0, l] = -(weight_j * area) * small[pl.ds(64 + 16 * l, NODES), :]
        coef[1, l] = -(weight_i * area) * small[pl.ds(96 + 16 * l, NODES), :]

    for copy in in_copies:
        copy.wait()

    def take_in(q, carry):
        t, l = (q - 1) // 2, (q - 1) % 2
        x = jnp.concatenate(
            [
                jnp.concatenate(
                    [
                        raw[half, pl.ds(256 * t + 16 * l + n, 8, stride=32), :]
                        for n in range(NODES)
                    ],
                    axis=0,
                )
                for half in range(2)
            ],
            axis=1,
        )
        y = permuted(x, tables[0])
        for n in range(NODES):
            layer = small[pl.ds(32 + 16 * l + n, 1), :]
            state[q, n] = y[8 * n : 8 * n + 8] * layer
        return carry

    lax.fori_loop(1, 7, take_in, 0, unroll=True)
    wide_sub = lax.broadcasted_iota(jnp.int32, (8, width), 0)
    for n in range(NODES):
        tile = jnp.zeros((8, width), jnp.float32)
        for l in range(2):
            layer = small[pl.ds(32 + 16 * l + n, 1), :]
            tile = jnp.where(wide_sub == 2 * l, small[pl.ds(16 * l + n, 1), :] * layer, tile)
            tile = jnp.where(wide_sub == 2 * l + 1, layer, tile)
        state[0, n] = tile
        for k in range(2):
            mixed_coef[k, n] = jnp.where(
                wide_sub < 2, coef[k, 0, pl.ds(n, 1), :], coef[k, 1, pl.ds(n, 1), :]
            )

    def level_coef(l, half):
        at = pl.ds(HALF * half, HALF)
        return [[coef[k, l, pl.ds(n, 1), at] for n in range(NODES)] for k in range(2)]

    def both_coef(half):
        at = pl.ds(HALF * half, HALF)
        return [[mixed_coef[k, n, :, at] for n in range(NODES)] for k in range(2)]

    def load(ref, q):
        return [
            [ref[q, n, :, pl.ds(HALF * half, HALF)] for n in range(NODES)] for half in range(2)
        ]

    def save(ref, q, v):
        for half in range(2):
            for n in range(NODES):
                ref[q, n, :, pl.ds(HALF * half, HALF)] = v[half][n]

    def scaled(half):
        at = pl.ds(HALF * half, HALF)
        return [scale[pl.ds(n, 1), at] for n in range(NODES)]

    def rates_of(q, h, mixed):
        v = []
        for half in range(2):
            a, b = both_coef(half) if mixed else level_coef((q - 1) % 2, half)
            rates = weighted_tendency(h[half], a, b)
            if mixed:
                at = pl.ds(HALF * half, HALF)
                rates = [
                    jnp.where(sublanes() == 4, mass[pl.ds(n, 1), at], rates[n])
                    for n in range(NODES)
                ]
            v.append(rates)
        return assembled_in_patch(v)

    def pack(v, q, stage, group, corners):
        slot = q - 4 * group
        for side, half, value in lines_of(v, slot):
            line_send[stage, group, side, half] += value
        return corners_of(v, slot, corners)

    def exchange(stage, group, corners):
        for k in range(4):
            corner_send[stage, group, k] = jnp.sum(corners[k], axis=0, keepdims=True)
        copies = []
        for side in (2, 3, 4, 5, 6, 7, 0, 1):
            if side < 4:
                source = line_send.at[stage, group, side]
                landing = line_recv.at[stage, group, OPPOSITE[side]]
            else:
                source = corner_send.at[stage, group, side - 4]
                landing = corner_recv.at[stage, group, OPPOSITE[side] - 4]
            copy = pltpu.make_async_remote_copy(
                src_ref=source,
                dst_ref=landing,
                send_sem=line_ssem.at[stage, group, side],
                recv_sem=line_rsem.at[stage, group, OPPOSITE[side]],
                device_id=targets[side],
                device_id_type=MESH,
            )
            copy.start()
            copies.append(copy)
        return copies

    def extra_of(q, stage, group):
        rows = [corner_recv[stage, group, k] for k in range(4)]
        return borders_of(q - 4 * group, line_recv.at[stage, group], rows)

    no_corners = tuple(jnp.zeros((8, HALF), jnp.float32) for _ in range(4))
    tiles_of = ((1, 4), (4, 7))

    def first(q, corners, group, mixed=False):
        v = rates_of(q, load(state, q), mixed)
        save(rate, q, v)
        return pack(v, q, 0, group, corners)

    first_sends, second_sends = [], []
    for group in range(2):
        corners = first(0, no_corners, 0, True) if group == 0 else no_corners
        corners = lax.fori_loop(
            *tiles_of[group], lambda q, c: first(q, c, group), corners, unroll=True
        )
        if group == 0:
            pl.semaphore_wait(barrier, len(targets) + len(peers))
        first_sends.append(exchange(0, group, corners))

    below = {"lev": lax.rem(level + n_lev - 1, n_lev)}
    above = {"lev": lax.rem(level + 1, n_lev)}
    has_below, has_above = level > 0, level < n_lev - 1

    def ratio_copy(t, l):
        return pltpu.make_async_remote_copy(
            src_ref=last_ratio.at[l] if t == 3 else ratio.at[t, l],
            dst_ref=last_recv.at[l] if t == 3 else ratio_recv.at[t, l],
            send_sem=ratio_ssem.at[t, l],
            recv_sem=ratio_rsem.at[t, l],
            device_id=below if l == 0 else above,
            device_id_type=MESH,
        )

    def send_ratios(t):
        pl.when(has_below)(lambda: ratio_copy(t, 0).start())
        pl.when(has_above)(lambda: ratio_copy(t, 1).start())

    def edge_copy(l):
        return pltpu.make_async_remote_copy(
            src_ref=edge_send.at[l],
            dst_ref=edge_recv.at[l],
            send_sem=edge_ssem.at[l],
            recv_sem=edge_rsem.at[l],
            device_id=below if l == 0 else above,
            device_id_type=MESH,
        )

    def second(q, corners, group, mixed=False):
        v = load(rate, q)
        extra = extra_of(q, 0, group)
        for half in range(2):
            for n in extra[half]:
                v[half][n] = v[half][n] + extra[half][n]
        if mixed:
            for half in range(2):
                for n in range(NODES):
                    shared[pl.ds(n, 1), pl.ds(HALF * half, HALF)] = v[half][n][4:5, :]
            scale[...] = time_step / shared[...]
        h = load(state, q)
        for half in range(2):
            c = scaled(half)
            for n in range(NODES):
                middle = h[half][n] + c[n] * v[half][n]
                state[q, n, :, pl.ds(HALF * half, HALF)] = h[half][n] + middle
                h[half][n] = middle
        v = rates_of(q, h, mixed)
        h = load(state, q)
        for half in range(2):
            c = scaled(half)
            for n in range(NODES):
                h[half][n] = 0.5 * (h[half][n] + c[n] * v[half][n])
        save(state, q, h)
        if mixed:
            split_mixed(h)
            for l in range(2):
                last_ratio[l] = last[l] * inverse[l]
        else:
            t, l = (q - 1) // 2, (q - 1) % 2
            for half in range(2):
                at = pl.ds(HALF * half, HALF)
                for n in range(NODES):
                    ratio[t, l, n, :, at] = h[half][n] * inverse[l, pl.ds(n, 1), at]
        return pack(v, q, 1, group, corners)

    def split_mixed(h):
        for half in range(2):
            at = pl.ds(HALF * half, HALF)
            for n in range(NODES):
                for l in range(2):
                    last[l, pl.ds(n, 1), at] = h[half][n][2 * l : 2 * l + 1, :]
                    thick[l, pl.ds(n, 1), at] = h[half][n][2 * l + 1 : 2 * l + 2, :]
        for l in range(2):
            inverse[l] = 1.0 / thick[l]

    for group in range(2):
        for copy in first_sends[group]:
            copy.wait_recv()
        corners = second(0, no_corners, 0, True) if group == 0 else no_corners
        corners = lax.fori_loop(
            *tiles_of[group], lambda q, c: second(q, c, group), corners, unroll=True
        )
        second_sends.append(exchange(1, group, corners))
        for t in ((3, 0), (1, 2))[group]:
            send_ratios(t)

    def finish(q, group, mixed=False):
        extra = extra_of(q, 1, group)
        h = load(state, q)
        for half in range(2):
            c = scaled(half)
            at = pl.ds(HALF * half, HALF)
            for n in extra[half]:
                h[half][n] = h[half][n] + 0.5 * (c[n] * extra[half][n])
                state[q, n, :, at] = h[half][n]
        return h

    def send_outline(q, h, l, slot, factor):
        r = [[h[half][n] * factor(half, n) for n in range(NODES)] for half in range(2)]
        for side, half, value in lines_of(r, slot):
            edge_send[l, side, half] += value

    def finish_levels(q, carry, group):
        t, l = (q - 1) // 2, (q - 1) % 2
        h = finish(q, group)
        send_outline(
            q, h, l, t, lambda half, n: inverse[l, pl.ds(n, 1), pl.ds(HALF * half, HALF)]
        )
        return carry

    column_copies = []
    for group in range(2):
        for copy in second_sends[group]:
            copy.wait_recv()
        if group == 0:
            h = finish(0, 0)
            split_mixed(h)
            column[...] = thick[0] + thick[1]
            for k, peer in enumerate(peers):
                copy = pltpu.make_async_remote_copy(
                    src_ref=column,
                    dst_ref=columns.at[k],
                    send_sem=column_ssem.at[k],
                    recv_sem=column_rsem.at[k],
                    device_id=peer,
                    device_id_type=MESH,
                )
                copy.start()
                column_copies.append(copy)
            for l in range(2):
                send_outline(
                    0,
                    h,
                    l,
                    3,
                    lambda half, n: inverse[l, pl.ds(n, 1), pl.ds(HALF * half, HALF)],
                )
        lax.fori_loop(
            *tiles_of[group], lambda q, c: finish_levels(q, c, group), 0, unroll=True
        )
    pl.when(has_below)(lambda: edge_copy(0).start())
    pl.when(has_above)(lambda: edge_copy(1).start())

    for copy in column_copies:
        copy.wait_recv()
    own_column = column[...]
    total = own_column
    under = jnp.zeros_like(own_column)
    for k in range(1, n_lev):
        part = columns[k - 1]
        total = total + part
        under = under + jnp.where(k <= level, part, 0.0)
    surface_rows = total
    levels = 2 * n_lev

    def as_float(k):
        return k.astype(jnp.float32)

    for k in range(3):
        edge_level = as_float(2 * level + k)
        fraction = (edge_level + edge_level * (edge_level - 1.0) * (1.0 / (levels - 1))) * (
            0.5 / levels
        )
        if k > 0:
            under = under + thick[k - 1]
        delta[k] = under - surface_rows * fraction
    for l in range(2):
        share = (1.0 + 2.0 * as_float(2 * level + l) * (1.0 / (levels - 1))) * (0.5 / levels)
        delta[3 + l] = 1.0 / (surface_rows * share)

    def wait_ratios(t):
        pl.when(has_above)(lambda: ratio_copy(t, 0).wait_recv())
        pl.when(has_below)(lambda: ratio_copy(t, 1).wait_recv())

    def remapped(d, carried, own_ratio, ratio_above, ratio_below):
        low = d[0] * jnp.where(d[0] > 0.0, ratio_below, own_ratio[0])
        middle = d[1] * jnp.where(d[1] > 0.0, own_ratio[0], own_ratio[1])
        high = d[2] * jnp.where(d[2] > 0.0, own_ratio[1], ratio_above)
        return (carried[0] + low - middle) * d[3], (carried[1] + middle - high) * d[4]

    pl.when(has_above)(lambda: edge_copy(0).wait_recv())
    pl.when(has_below)(lambda: edge_copy(1).wait_recv())
    wait_ratios(3)
    for l in range(2):
        for half, n, mask, value in placed_lines(3, edge_recv.at[l]):
            row, at = pl.ds(n, 1), pl.ds(HALF * half, HALF)
            last_recv[l, row, at] = jnp.where(
                mask[0:1], value[2 * l : 2 * l + 1], last_recv[l, row, at]
            )
    d = [delta[k] for k in range(5)]
    first, second = remapped(
        d,
        [last[0], last[1]],
        [last[0] * inverse[0], last[1] * inverse[1]],
        last_recv[0],
        last_recv[1],
    )
    rows = permuted(jnp.concatenate([first, second, surface_rows], axis=0), tables[1])
    last_rows[...] = rows
    out_copies = [
        pltpu.make_async_copy(last_rows.at[pl.ds(32, 16)], surf, out_sem.at[3, 0]),
        pltpu.make_async_copy(
            last_rows.at[pl.ds(0, 32)], out.at[pl.ds(768, 32)], out_sem.at[3, 1]
        ),
    ]
    for copy in out_copies:
        copy.start()

    for t in range(3):
        wait_ratios(t)
        beside_block = []
        for l in range(2):
            r = load(ratio_recv.at[t], l)
            for half, n, mask, value in placed_lines(t, edge_recv.at[l]):
                r[half][n] = jnp.where(mask, value, r[half][n])
            beside_block.append(r)
        pairs = []
        for n in range(NODES):
            parts = []
            for half in range(2):
                at = pl.ds(HALF * half, HALF)
                d = [delta[k, pl.ds(n, 1), at] for k in range(5)]
                carried = [state[2 * t + 1 + l, n, :, at] for l in range(2)]
                own_ratio = [carried[l] * inverse[l, pl.ds(n, 1), at] for l in range(2)]
                parts.append(
                    remapped(d, carried, own_ratio, beside_block[0][half][n], beside_block[1][half][n])
                )
            pairs.append(
                [jnp.concatenate([parts[0][l], parts[1][l]], axis=1) for l in range(2)]
            )
        for l in range(2):
            tiles = permuted(jnp.concatenate([pair[l] for pair in pairs], axis=0), tables[1])
            for n in range(NODES):
                for half in range(2):
                    result[half, pl.ds(256 * t + 16 * l + n, 8, stride=32), :] = tiles[
                        8 * n : 8 * n + 8, HALF * half : HALF * half + HALF
                    ]
        rows = pl.ds(256 * t, 256)
        for half in range(2):
            copy = pltpu.make_async_copy(
                result.at[half, rows],
                out.at[rows, pl.ds(HALF * half, HALF)],
                out_sem.at[t, half],
            )
            copy.start()
            out_copies.append(copy)

    for copy in out_copies:
        copy.wait()
    for copy in sum(first_sends + second_sends, column_copies):
        copy.wait_send()
    for t in range(4):
        pl.when(has_below)(lambda t=t: ratio_copy(t, 0).wait_send())
        pl.when(has_above)(lambda t=t: ratio_copy(t, 1).wait_send())
    pl.when(has_below)(lambda: edge_copy(0).wait_send())
    pl.when(has_above)(lambda: edge_copy(1).wait_send())


def per_device(n_elem, n_lev, tracers, layer_mass, winds, metric, neighbours):
    width = metric.shape[-1]
    f32 = jnp.float32
    any_spec = pl.BlockSpec(memory_space=pl.ANY)
    tile = (NODES, 8, width)
    dma = pltpu.SemaphoreType.DMA
    scratch = [
        pltpu.VMEM((8, width), jnp.int32),
        pltpu.VMEM((2, 768, HALF), f32),
        pltpu.VMEM((144, width), f32),
        pltpu.VMEM((144, width), f32),
        pltpu.VMEM((2, width, width), jnp.bfloat16),
        pltpu.VMEM((7,) + tile, f32),
        pltpu.VMEM((7,) + tile, f32),
        pltpu.VMEM((2, 2, NODES, width), f32),
        pltpu.VMEM((2,) + tile, f32),
        pltpu.VMEM((NODES, width), f32),
        pltpu.VMEM((NODES, width), f32),
        pltpu.VMEM((NODES, width), f32),
        pltpu.VMEM((2, 2, 4, 2, 8, HALF), f32),
        pltpu.VMEM((2, 2, 4, 2, 8, HALF), f32),
        pltpu.VMEM((2, 2, 4, 1, HALF), f32),
        pltpu.VMEM((2, 2, 4, 1, HALF), f32),
        pltpu.VMEM((2, NODES, width), f32),
        pltpu.VMEM((2, NODES, width), f32),
        pltpu.VMEM((2, NODES, width), f32),
        pltpu.VMEM((NODES, width), f32),
        pltpu.VMEM((n_lev - 1, NODES, width), f32),
        pltpu.VMEM((3, 2) + tile, f32),
        pltpu.VMEM((3, 2) + tile, f32),
        pltpu.VMEM((2, NODES, width), f32),
        pltpu.VMEM((2, NODES, width), f32),
        pltpu.VMEM((2, 4, 2, 8, HALF), f32),
        pltpu.VMEM((2, 4, 2, 8, HALF), f32),
        pltpu.VMEM((5, NODES, width), f32),
        pltpu.VMEM((2, 768, HALF), f32),
        pltpu.VMEM((3 * NODES, width), f32),
        dma((2,)),
        dma((5,)),
        dma((4, 2)),
        dma((2, 2, 8)),
        dma((2, 2, 8)),
        dma((n_lev - 1,)),
        dma((n_lev - 1,)),
        dma((4, 2)),
        dma((4, 2)),
        dma((2,)),
        dma((2,)),
    ]
    out, surface = pl.pallas_call(
        functools.partial(kernel, n_elem, n_lev),
        out_shape=(
            jax.ShapeDtypeStruct((800, width), f32),
            jax.ShapeDtypeStruct((NODES, width), f32),
        ),
        in_specs=[any_spec] * 5,
        out_specs=(any_spec, any_spec),
        scratch_shapes=scratch,
        compiler_params=pltpu.CompilerParams(collective_id=0, has_side_effects=True),
        name="transport",
    )(
        tracers.reshape(-1, width),
        layer_mass.reshape(-1, width),
        winds.reshape(-1, width),
        metric,
        jnp.transpose(neighbours),
    )
    return out.reshape(tracers.shape), surface


def solution(mesh):
    placed = (
        P(None, "lev", None, ("members", "elem")),
        P("lev", None, ("members", "elem")),
        P(None, "lev", None, ("members", "elem")),
        P(None, "elem"),
        P("elem", None),
    )
    return jax.shard_map(
        functools.partial(per_device, mesh.shape["elem"], mesh.shape["lev"]),
        mesh=mesh,
        in_specs=placed,
        out_specs=(P(None, "lev", None, ("members", "elem")), P(None, ("members", "elem"))),
        check_vma=False,
    )
```

```python
import functools
import math

import jax
import jax.numpy as jnp
import numpy as np
from jax import lax
from jax.experimental import pallas as pl
from jax.experimental.pallas import tpu as pltpu
from jax.sharding import PartitionSpec as P

MESH = pl.DeviceIdType.MESH
PSIDE = 16
ACROSS = 8
NODES = 16
HALF = 128
time_step = 0.035

OPPOSITE = (1, 0, 3, 2, 7, 6, 5, 4)
CORNERS = ((15, 1, 127), (12, 1, 112), (3, 0, 15), (0, 0, 0))


def lagrange_scale(points, which):
    product = 1.0
    for other in range(4):
        if other != which:
            product = product * (points[which] - points[other])
    return product


def node_tables():
    points = np.array([-1.0, -1.0 / math.sqrt(5.0), 1.0 / math.sqrt(5.0), 1.0])
    weights = np.array([1.0, 5.0, 5.0, 1.0]) / 6.0
    derivative = np.zeros((4, 4))
    for target in range(4):
        for source in range(4):
            if target == source:
                derivative[target, source] = sum(
                    1.0 / (points[target] - points[other]) for other in range(4) if other != target
                )
            else:
                derivative[target, source] = lagrange_scale(points, target) / (
                    lagrange_scale(points, source) * (points[target] - points[source])
                )
    return weights, derivative


WEIGHTS, DERIVATIVE = node_tables()
STIFF = WEIGHTS[:, None] * DERIVATIVE


def weighted_difference(f):
    total, gap = f[0] + f[3], f[3] - f[0]
    inner, inner_gap = f[1] + f[2], f[2] - f[1]
    result = [None] * 4
    for i in range(2):
        q = 0.5 * STIFF[i]
        odd = float(q[3] - q[0]) * gap + float(q[2] - q[1]) * inner_gap
        even = float(q[0] + q[3]) * total + float(q[1] + q[2]) * inner
        result[i] = odd + even
        result[3 - i] = odd - even
    return result


def weighted_tendency(h, a, b):
    f = [a[n] * h[n] for n in range(NODES)]
    g = [b[n] * h[n] for n in range(NODES)]
    rows = [weighted_difference(f[4 * j : 4 * j + 4]) for j in range(4)]
    columns = [weighted_difference(g[i::4]) for i in range(4)]
    return [rows[n // 4][n % 4] + columns[n % 4][n // 4] for n in range(NODES)]


def lanes():
    return lax.broadcasted_iota(jnp.int32, (8, HALF), 1)


def sublanes():
    return lax.broadcasted_iota(jnp.int32, (8, HALF), 0)


def roll(x, shift):
    return pltpu.roll(x, (shift + 2 * HALF) % HALF, 1)


def assembled_in_patch(v):
    lane = lanes()
    column = lane % PSIDE
    for half in range(2):
        for j in range(4):
            left, right = v[half][4 * j], v[half][4 * j + 3]
            v[half][4 * j + 3] = right + jnp.where(column < PSIDE - 1, roll(left, -1), 0.0)
            v[half][4 * j] = left + jnp.where(column > 0, roll(right, 1), 0.0)
    edge = HALF - PSIDE
    for i in range(4):
        low = [v[0][i], v[1][i]]
        high = [v[0][12 + i], v[1][12 + i]]
        down = [roll(low[0], -PSIDE), roll(low[1], -PSIDE)]
        up = [roll(high[0], PSIDE), roll(high[1], PSIDE)]
        v[0][12 + i] = high[0] + jnp.where(lane < edge, down[0], down[1])
        v[1][12 + i] = high[1] + jnp.where(lane < edge, down[1], 0.0)
        v[0][i] = low[0] + jnp.where(lane >= PSIDE, up[0], 0.0)
        v[1][i] = low[1] + jnp.where(lane >= PSIDE, up[1], up[0])
    return v


def lines_of(v, slot):
    lane = lanes()
    column, block = lane % PSIDE, lane // PSIDE
    found = []
    for half in range(2):
        east = west = 0.0
        for j in range(4):
            at = 4 * slot + j
            east = east + jnp.where(column == at, roll(v[half][4 * j + 3], at - (PSIDE - 1)), 0.0)
            west = west + jnp.where(column == at, roll(v[half][4 * j], at), 0.0)
        found += [(0, half, east), (1, half, west)]
    north = south = 0.0
    for i in range(4):
        at = 4 * (slot % 2) + i
        north = north + jnp.where(
            block == at, roll(v[1][12 + i], PSIDE * at - (HALF - PSIDE)), 0.0
        )
        south = south + jnp.where(block == at, roll(v[0][i], PSIDE * at), 0.0)
    return found + [(2, slot // 2, north), (3, slot // 2, south)]


def corners_of(v, slot, corners):
    lane, sub = lanes(), sublanes()
    result = []
    for k, (node, half, where) in enumerate(CORNERS):
        value = jnp.broadcast_to(v[half][node][:, where : where + 1], (8, HALF))
        result.append(corners[k] + jnp.where(lane == 8 * slot + sub, value, 0.0))
    return tuple(result)


def placed_lines(slot, lines):
    lane = lanes()
    column = lane % PSIDE
    found = []
    for half in range(2):
        east, west = lines[0, half], lines[1, half]
        for j in range(4):
            at = 4 * slot + j
            found.append((half, 4 * j + 3, column == PSIDE - 1, roll(east, PSIDE - 1 - at)))
            found.append((half, 4 * j, column == 0, roll(west, -at)))
    north, south = lines[2, slot // 2], lines[3, slot // 2]
    for i in range(4):
        at = 4 * (slot % 2) + i
        found.append(
            (1, 12 + i, lane >= HALF - PSIDE, roll(north, HALF - PSIDE - PSIDE * at))
        )
        found.append((0, i, lane < PSIDE, roll(south, -PSIDE * at)))
    return found


def borders_of(slot, lines, corners):
    lane, sub = lanes(), sublanes()
    extra = [{}, {}]
    found = placed_lines(slot, lines)
    for k, (node, half, where) in enumerate(CORNERS):
        row = jnp.broadcast_to(corners[k], (8, HALF))
        value = jnp.sum(jnp.where(lane == 8 * slot + sub, row, 0.0), axis=1, keepdims=True)
        found.append((half, node, lane == where, value))
    for half, node, mask, value in found:
        part = jnp.where(mask, value, 0.0)
        extra[half][node] = extra[half][node] + part if node in extra[half] else part
    return extra


def permuted(x, table):
    high = x.astype(jnp.bfloat16)
    rest = x - high.astype(jnp.float32)
    middle = rest.astype(jnp.bfloat16)
    low = (rest - middle.astype(jnp.float32)).astype(jnp.bfloat16)
    dot = functools.partial(jnp.dot, preferred_element_type=jnp.float32)
    return dot(high, table) + dot(middle, table) + dot(low, table)


def halves(x):
    return [x[:, :HALF], x[:, HALF:]]


def kernel(
    n_elem,
    n_lev,
    trc,
    thickness,
    winds,
    metric,
    beside,
    out,
    sums,
    near,
    raw,
    small_raw,
    small,
    tables,
    state,
    rate,
    coef,
    mixed_coef,
    mass,
    shared,
    scale,
    line_send,
    line_recv,
    corner_send,
    corner_recv,
    thick,
    last,
    inverse,
    column,
    columns,
    ratio,
    ratio_recv,
    last_ratio,
    last_recv,
    edge_send,
    edge_recv,
    delta,
    result,
    in_sem,
    small_sem,
    line_ssem,
    line_rsem,
    column_ssem,
    column_rsem,
    ratio_ssem,
    ratio_rsem,
    edge_ssem,
    edge_rsem,
):
    place, level = lax.axis_index("elem"), lax.axis_index("lev")
    width = 2 * HALF
    offsets = (
        1,
        -1,
        ACROSS,
        -ACROSS,
        ACROSS + 1,
        ACROSS - 1,
        1 - ACROSS,
        -1 - ACROSS,
    )
    targets = [{"elem": lax.rem(place + offset + n_elem, n_elem)} for offset in offsets]
    peers = [{"lev": lax.rem(level + k, n_lev)} for k in range(1, n_lev)]

    barrier = pltpu.get_barrier_semaphore()
    for target in targets + peers:
        pl.semaphore_signal(barrier, inc=1, device_id=target, device_id_type=MESH)

    near_copy = pltpu.make_async_copy(beside, near, small_sem.at[0])
    near_copy.start()
    pieces = [
        (trc.at[pl.ds(768, 32)], 0, 32),
        (thickness, 32, 32),
        (winds, 64, 64),
        (metric, 128, 16),
    ]
    small_copies = []
    for k, (source, start, size) in enumerate(pieces):
        copy = pltpu.make_async_copy(
            source, small_raw.at[pl.ds(start, size)], small_sem.at[k + 1]
        )
        copy.start()
        small_copies.append(copy)
    in_copies = []
    for half in range(2):
        copy = pltpu.make_async_copy(
            trc.at[pl.ds(0, 768), pl.ds(HALF * half, HALF)], raw.at[half], in_sem.at[half]
        )
        copy.start()
        in_copies.append(copy)

    line_send[...] = jnp.zeros_like(line_send)
    edge_send[...] = jnp.zeros_like(edge_send)

    @pl.when(level == 0)
    def _():
        edge_recv[1] = jnp.zeros_like(edge_recv[1])
        ratio_recv[:, 1] = jnp.zeros_like(ratio_recv[:, 1])
        last_recv[1] = jnp.zeros_like(last_recv[1])

    @pl.when(level == n_lev - 1)
    def _():
        edge_recv[0] = jnp.zeros_like(edge_recv[0])
        ratio_recv[:, 0] = jnp.zeros_like(ratio_recv[:, 0])
        last_recv[0] = jnp.zeros_like(last_recv[0])

    near_copy.wait()
    dot = functools.partial(jnp.dot, preferred_element_type=jnp.float32)
    element = lax.broadcasted_iota(jnp.int32, (width, width), 0)
    own = near[...] - place * width
    spots = []
    for side in (1, 3):
        step = jnp.where(own[side : side + 1, :] == element, 1.0, 0.0).astype(jnp.bfloat16)
        count = dot(jnp.ones((8, width), jnp.bfloat16), step)
        for doubling in range(4):
            count = count + dot(count.astype(jnp.bfloat16), step)
            if doubling < 3:
                step = dot(step, step).astype(jnp.bfloat16)
        spots.append(count)
    spot = (spots[0] + PSIDE * spots[1]).astype(jnp.int32)[0:1, :]
    to_drawn = jnp.where(spot == element, 1.0, 0.0)
    tables[1] = to_drawn.astype(jnp.bfloat16)
    tables[0] = jnp.transpose(to_drawn).astype(jnp.bfloat16)

    for copy in small_copies:
        copy.wait()
    small[...] = permuted(small_raw[...], tables[0])
    node = lax.broadcasted_iota(jnp.int32, (NODES, width), 0)
    point_i, point_j = node % 4, node // 4
    ends, inside = float(WEIGHTS[0]), float(WEIGHTS[1])
    weight_i = jnp.where((point_i == 0) | (point_i == 3), ends, inside)
    weight_j = jnp.where((point_j == 0) | (point_j == 3), ends, inside)
    area = small[pl.ds(128, NODES), :]
    mass[...] = weight_i * weight_j * area
    for l in range(2):
        coef[0, l] = -(weight_j * area) * small[pl.ds(64 + 16 * l, NODES), :]
        coef[1, l] = -(weight_i * area) * small[pl.ds(96 + 16 * l, NODES), :]

    for copy in in_copies:
        copy.wait()

    def take_in(q, carry):
        t, l = (q - 1) // 2, (q - 1) % 2
        x = jnp.concatenate(
            [
                jnp.concatenate(
                    [
                        raw[half, pl.ds(256 * t + 16 * l + n, 8, stride=32), :]
                        for n in range(NODES)
                    ],
                    axis=0,
                )
                for half in range(2)
            ],
            axis=1,
        )
        y = permuted(x, tables[0])
        for n in range(NODES):
            layer = small[pl.ds(32 + 16 * l + n, 1), :]
            state[q, n] = y[8 * n : 8 * n + 8] * layer
        return carry

    lax.fori_loop(1, 7, take_in, 0, unroll=True)
    wide_sub = lax.broadcasted_iota(jnp.int32, (8, width), 0)
    for n in range(NODES):
        tile = jnp.zeros((8, width), jnp.float32)
        for l in range(2):
            layer = small[pl.ds(32 + 16 * l + n, 1), :]
            tile = jnp.where(wide_sub == 2 * l, small[pl.ds(16 * l + n, 1), :] * layer, tile)
            tile = jnp.where(wide_sub == 2 * l + 1, layer, tile)
        state[0, n] = tile
        for k in range(2):
            mixed_coef[k, n] = jnp.where(
                wide_sub < 2, coef[k, 0, pl.ds(n, 1), :], coef[k, 1, pl.ds(n, 1), :]
            )

    def level_coef(l, half):
        at = pl.ds(HALF * half, HALF)
        return [[coef[k, l, pl.ds(n, 1), at] for n in range(NODES)] for k in range(2)]

    def both_coef(half):
        at = pl.ds(HALF * half, HALF)
        return [[mixed_coef[k, n, :, at] for n in range(NODES)] for k in range(2)]

    def load(ref, q):
        return [
            [ref[q, n, :, pl.ds(HALF * half, HALF)] for n in range(NODES)] for half in range(2)
        ]

    def save(ref, q, v):
        for half in range(2):
            for n in range(NODES):
                ref[q, n, :, pl.ds(HALF * half, HALF)] = v[half][n]

    def scaled(half):
        at = pl.ds(HALF * half, HALF)
        return [scale[pl.ds(n, 1), at] for n in range(NODES)]

    def rates_of(q, h, mixed):
        v = []
        for half in range(2):
            a, b = both_coef(half) if mixed else level_coef((q - 1) % 2, half)
            rates = weighted_tendency(h[half], a, b)
            if mixed:
                at = pl.ds(HALF * half, HALF)
                rates = [
                    jnp.where(sublanes() == 4, mass[pl.ds(n, 1), at], rates[n])
                    for n in range(NODES)
                ]
            v.append(rates)
        return assembled_in_patch(v)

    def pack(v, q, stage, group, corners):
        slot = q - 4 * group
        for side, half, value in lines_of(v, slot):
            line_send[stage, group, side, half] += value
        return corners_of(v, slot, corners)

    def exchange(stage, group, corners):
        for k in range(4):
            corner_send[stage, group, k] = jnp.sum(corners[k], axis=0, keepdims=True)
        copies = []
        for side in (2, 3, 4, 5, 6, 7, 0, 1):
            if side < 4:
                source = line_send.at[stage, group, side]
                landing = line_recv.at[stage, group, OPPOSITE[side]]
            else:
                source = corner_send.at[stage, group, side - 4]
                landing = corner_recv.at[stage, group, OPPOSITE[side] - 4]
            copy = pltpu.make_async_remote_copy(
                src_ref=source,
                dst_ref=landing,
                send_sem=line_ssem.at[stage, group, side],
                recv_sem=line_rsem.at[stage, group, OPPOSITE[side]],
                device_id=targets[side],
                device_id_type=MESH,
            )
            copy.start()
            copies.append(copy)
        return copies

    def extra_of(q, stage, group):
        rows = [corner_recv[stage, group, k] for k in range(4)]
        return borders_of(q - 4 * group, line_recv.at[stage, group], rows)

    no_corners = tuple(jnp.zeros((8, HALF), jnp.float32) for _ in range(4))
    tiles_of = ((1, 4), (4, 7))

    def first(q, corners, group, mixed=False):
        v = rates_of(q, load(state, q), mixed)
        save(rate, q, v)
        return pack(v, q, 0, group, corners)

    first_sends, second_sends = [], []
    for group in range(2):
        corners = first(0, no_corners, 0, True) if group == 0 else no_corners
        corners = lax.fori_loop(
            *tiles_of[group], lambda q, c: first(q, c, group), corners, unroll=True
        )
        if group == 0:
            pl.semaphore_wait(barrier, len(targets) + len(peers))
        first_sends.append(exchange(0, group, corners))

    below = {"lev": lax.rem(level + n_lev - 1, n_lev)}
    above = {"lev": lax.rem(level + 1, n_lev)}
    has_below, has_above = level > 0, level < n_lev - 1

    def ratio_copy(t, l):
        return pltpu.make_async_remote_copy(
            src_ref=last_ratio.at[l] if t == 3 else ratio.at[t, l],
            dst_ref=last_recv.at[l] if t == 3 else ratio_recv.at[t, l],
            send_sem=ratio_ssem.at[t, l],
            recv_sem=ratio_rsem.at[t, l],
            device_id=below if l == 0 else above,
            device_id_type=MESH,
        )

    def send_ratios(t):
        pl.when(has_below)(lambda: ratio_copy(t, 0).start())
        pl.when(has_above)(lambda: ratio_copy(t, 1).start())

    def edge_copy(l):
        return pltpu.make_async_remote_copy(
            src_ref=edge_send.at[l],
            dst_ref=edge_recv.at[l],
            send_sem=edge_ssem.at[l],
            recv_sem=edge_rsem.at[l],
            device_id=below if l == 0 else above,
            device_id_type=MESH,
        )

    def second(q, corners, group, mixed=False):
        v = load(rate, q)
        extra = extra_of(q, 0, group)
        for half in range(2):
            for n in extra[half]:
                v[half][n] = v[half][n] + extra[half][n]
        if mixed:
            for half in range(2):
                for n in range(NODES):
                    shared[pl.ds(n, 1), pl.ds(HALF * half, HALF)] = v[half][n][4:5, :]
            scale[...] = time_step / shared[...]
        h = load(state, q)
        for half in range(2):
            c = scaled(half)
            for n in range(NODES):
                middle = h[half][n] + c[n] * v[half][n]
                state[q, n, :, pl.ds(HALF * half, HALF)] = h[half][n] + middle
                h[half][n] = middle
        v = rates_of(q, h, mixed)
        h = load(state, q)
        for half in range(2):
            c = scaled(half)
            for n in range(NODES):
                h[half][n] = 0.5 * (h[half][n] + c[n] * v[half][n])
        save(state, q, h)
        if mixed:
            split_mixed(h)
            for l in range(2):
                last_ratio[l] = last[l] * inverse[l]
        else:
            t, l = (q - 1) // 2, (q - 1) % 2
            for half in range(2):
                at = pl.ds(HALF * half, HALF)
                for n in range(NODES):
                    ratio[t, l, n, :, at] = h[half][n] * inverse[l, pl.ds(n, 1), at]
        return pack(v, q, 1, group, corners)

    def split_mixed(h):
        for half in range(2):
            at = pl.ds(HALF * half, HALF)
            for n in range(NODES):
                for l in range(2):
                    last[l, pl.ds(n, 1), at] = h[half][n][2 * l : 2 * l + 1, :]
                    thick[l, pl.ds(n, 1), at] = h[half][n][2 * l + 1 : 2 * l + 2, :]
        for l in range(2):
            inverse[l] = 1.0 / thick[l]

    for group in range(2):
        for copy in first_sends[group]:
            copy.wait_recv()
        corners = second(0, no_corners, 0, True) if group == 0 else no_corners
        corners = lax.fori_loop(
            *tiles_of[group], lambda q, c: second(q, c, group), corners, unroll=True
        )
        second_sends.append(exchange(1, group, corners))
        for t in ((3, 0), (1, 2))[group]:
            send_ratios(t)

    def finish(q, group, mixed=False):
        extra = extra_of(q, 1, group)
        h = load(state, q)
        for half in range(2):
            c = scaled(half)
            at = pl.ds(HALF * half, HALF)
            for n in extra[half]:
                h[half][n] = h[half][n] + 0.5 * (c[n] * extra[half][n])
                state[q, n, :, at] = h[half][n]
        return h

    def send_outline(q, h, l, slot, factor):
        r = [[h[half][n] * factor(half, n) for n in range(NODES)] for half in range(2)]
        for side, half, value in lines_of(r, slot):
            edge_send[l, side, half] += value

    def finish_levels(q, carry, group):
        t, l = (q - 1) // 2, (q - 1) % 2
        h = finish(q, group)
        send_outline(
            q, h, l, t, lambda half, n: inverse[l, pl.ds(n, 1), pl.ds(HALF * half, HALF)]
        )
        return carry

    column_copies = []
    for group in range(2):
        for copy in second_sends[group]:
            copy.wait_recv()
        if group == 0:
            h = finish(0, 0)
            split_mixed(h)
            column[...] = thick[0] + thick[1]
            for k, peer in enumerate(peers):
                copy = pltpu.make_async_remote_copy(
                    src_ref=column,
                    dst_ref=columns.at[k],
                    send_sem=column_ssem.at[k],
                    recv_sem=column_rsem.at[k],
                    device_id=peer,
                    device_id_type=MESH,
                )
                copy.start()
                column_copies.append(copy)
            for l in range(2):
                send_outline(
                    0,
                    h,
                    l,
                    3,
                    lambda half, n: inverse[l, pl.ds(n, 1), pl.ds(HALF * half, HALF)],
                )
        lax.fori_loop(
            *tiles_of[group], lambda q, c: finish_levels(q, c, group), 0, unroll=True
        )
    pl.when(has_below)(lambda: edge_copy(0).start())
    pl.when(has_above)(lambda: edge_copy(1).start())

    for copy in column_copies:
        copy.wait_recv()
    own_column = column[...]
    others = jnp.zeros_like(own_column)
    under = jnp.zeros_like(own_column)
    for k in range(1, n_lev):
        part = columns[k - 1]
        others = others + part
        under = under + jnp.where(k <= level, part, 0.0)
    surface_rows = own_column + others
    levels = 2 * n_lev

    def as_float(k):
        return k.astype(jnp.float32)

    for k in range(3):
        edge_level = as_float(2 * level + k)
        fraction = (edge_level + edge_level * (edge_level - 1.0) * (1.0 / (levels - 1))) * (
            0.5 / levels
        )
        if k > 0:
            under = under + thick[k - 1]
        delta[k] = under - surface_rows * fraction
    def wait_ratios(t):
        pl.when(has_above)(lambda: ratio_copy(t, 0).wait_recv())
        pl.when(has_below)(lambda: ratio_copy(t, 1).wait_recv())

    def remapped(d, carried, own_ratio, ratio_above, ratio_below):
        low = d[0] * jnp.where(d[0] > 0.0, ratio_below, own_ratio[0])
        middle = d[1] * jnp.where(d[1] > 0.0, own_ratio[0], own_ratio[1])
        high = d[2] * jnp.where(d[2] > 0.0, own_ratio[1], ratio_above)
        return carried[0] + low - middle, carried[1] + middle - high

    pl.when(has_above)(lambda: edge_copy(0).wait_recv())
    pl.when(has_below)(lambda: edge_copy(1).wait_recv())
    wait_ratios(3)
    for l in range(2):
        for half, n, mask, value in placed_lines(3, edge_recv.at[l]):
            row, at = pl.ds(n, 1), pl.ds(HALF * half, HALF)
            last_recv[l, row, at] = jnp.where(
                mask[0:1], value[2 * l : 2 * l + 1], last_recv[l, row, at]
            )
    d = [delta[k] for k in range(3)]
    first, second = remapped(
        d,
        [last[0], last[1]],
        [last[0] * inverse[0], last[1] * inverse[1]],
        last_recv[0],
        last_recv[1],
    )
    shares = [
        surface_rows
        * ((1.0 + 2.0 * as_float(2 * level + l) * (1.0 / (levels - 1))) * (0.5 / levels))
        for l in range(2)
    ]
    rows = permuted(
        jnp.concatenate([first, second, own_column, others] + shares, axis=0), tables[1]
    )
    out[pl.ds(768, 32), :] = rows[0:32]
    sums[...] = rows[32:96]
    for t in range(3):
        wait_ratios(t)
        beside_block = []
        for l in range(2):
            r = load(ratio_recv.at[t], l)
            for half, n, mask, value in placed_lines(t, edge_recv.at[l]):
                r[half][n] = jnp.where(mask, value, r[half][n])
            beside_block.append(r)
        pairs = []
        for n in range(NODES):
            parts = []
            for half in range(2):
                at = pl.ds(HALF * half, HALF)
                d = [delta[k, pl.ds(n, 1), at] for k in range(3)]
                carried = [state[2 * t + 1 + l, n, :, at] for l in range(2)]
                own_ratio = [carried[l] * inverse[l, pl.ds(n, 1), at] for l in range(2)]
                parts.append(
                    remapped(d, carried, own_ratio, beside_block[0][half][n], beside_block[1][half][n])
                )
            pairs.append(
                [jnp.concatenate([parts[0][l], parts[1][l]], axis=1) for l in range(2)]
            )
        for l in range(2):
            tiles = permuted(jnp.concatenate([pair[l] for pair in pairs], axis=0), tables[1])
            for n in range(NODES):
                for half in range(2):
                    result[half, pl.ds(256 * t + 16 * l + n, 8, stride=32), :] = tiles[
                        8 * n : 8 * n + 8, HALF * half : HALF * half + HALF
                    ]
        rows = pl.ds(256 * t, 256)
        for half in range(2):
            out[rows, pl.ds(HALF * half, HALF)] = result[half, rows, :]
    for copy in sum(first_sends + second_sends, column_copies):
        copy.wait_send()
    for t in range(4):
        pl.when(has_below)(lambda t=t: ratio_copy(t, 0).wait_send())
        pl.when(has_above)(lambda t=t: ratio_copy(t, 1).wait_send())
    pl.when(has_below)(lambda: edge_copy(0).wait_send())
    pl.when(has_above)(lambda: edge_copy(1).wait_send())


def per_device(n_elem, n_lev, tracers, layer_mass, winds, metric, neighbours):
    width = metric.shape[-1]
    f32 = jnp.float32
    tile = (NODES, 8, width)
    dma = pltpu.SemaphoreType.DMA
    scratch = [
        pltpu.VMEM((8, width), jnp.int32),
        pltpu.VMEM((2, 768, HALF), f32),
        pltpu.VMEM((144, width), f32),
        pltpu.VMEM((144, width), f32),
        pltpu.VMEM((2, width, width), jnp.bfloat16),
        pltpu.VMEM((7,) + tile, f32),
        pltpu.VMEM((7,) + tile, f32),
        pltpu.VMEM((2, 2, NODES, width), f32),
        pltpu.VMEM((2,) + tile, f32),
        pltpu.VMEM((NODES, width), f32),
        pltpu.VMEM((NODES, width), f32),
        pltpu.VMEM((NODES, width), f32),
        pltpu.VMEM((2, 2, 4, 2, 8, HALF), f32),
        pltpu.VMEM((2, 2, 4, 2, 8, HALF), f32),
        pltpu.VMEM((2, 2, 4, 1, HALF), f32),
        pltpu.VMEM((2, 2, 4, 1, HALF), f32),
        pltpu.VMEM((2, NODES, width), f32),
        pltpu.VMEM((2, NODES, width), f32),
        pltpu.VMEM((2, NODES, width), f32),
        pltpu.VMEM((NODES, width), f32),
        pltpu.VMEM((n_lev - 1, NODES, width), f32),
        pltpu.VMEM((3, 2) + tile, f32),
        pltpu.VMEM((3, 2) + tile, f32),
        pltpu.VMEM((2, NODES, width), f32),
        pltpu.VMEM((2, NODES, width), f32),
        pltpu.VMEM((2, 4, 2, 8, HALF), f32),
        pltpu.VMEM((2, 4, 2, 8, HALF), f32),
        pltpu.VMEM((3, NODES, width), f32),
        pltpu.VMEM((2, 768, HALF), f32),
        dma((2,)),
        dma((5,)),
        dma((2, 2, 8)),
        dma((2, 2, 8)),
        dma((n_lev - 1,)),
        dma((n_lev - 1,)),
        dma((4, 2)),
        dma((4, 2)),
        dma((2,)),
        dma((2,)),
    ]
    result, sums = pl.pallas_call(
        functools.partial(kernel, n_elem, n_lev),
        out_shape=(
            jax.ShapeDtypeStruct((800, width), f32),
            jax.ShapeDtypeStruct((4 * NODES, width), f32),
        ),
        in_specs=[pl.BlockSpec(memory_space=pltpu.HBM)] * 5,
        out_specs=(
            pl.BlockSpec(memory_space=pltpu.VMEM),
            pl.BlockSpec(memory_space=pltpu.VMEM),
        ),
        scratch_shapes=scratch,
        compiler_params=pltpu.CompilerParams(
            collective_id=0, has_side_effects=True, vmem_limit_bytes=24 * 1024 * 1024
        ),
        name="transport",
    )(
        *[
            pltpu.with_memory_space_constraint(x, pltpu.HBM)
            for x in (
                tracers.reshape(-1, width),
                layer_mass.reshape(-1, width),
                winds.reshape(-1, width),
                metric,
                jnp.transpose(neighbours),
            )
        ]
    )
    surface = sums[:NODES] + sums[NODES : 2 * NODES]
    shares = sums[2 * NODES :].reshape(layer_mass.shape)
    return result.reshape(tracers.shape) / shares, surface


def solution(mesh):
    placed = (
        P(None, "lev", None, ("members", "elem")),
        P("lev", None, ("members", "elem")),
        P(None, "lev", None, ("members", "elem")),
        P(None, "elem"),
        P("elem", None),
    )
    return jax.shard_map(
        functools.partial(per_device, mesh.shape["elem"], mesh.shape["lev"]),
        mesh=mesh,
        in_specs=placed,
        out_specs=(P(None, "lev", None, ("members", "elem")), P(None, ("members", "elem"))),
        check_vma=False,
    )
```

```python
import functools
import math

import jax
import jax.numpy as jnp
import numpy as np
from jax import lax
from jax.experimental import pallas as pl
from jax.experimental.pallas import tpu as pltpu
from jax.sharding import PartitionSpec as P

MESH = pl.DeviceIdType.MESH
PSIDE = 16
ACROSS = 8
NODES = 16
HALF = 128
time_step = 0.035

OPPOSITE = (1, 0, 3, 2, 7, 6, 5, 4)
CORNERS = ((15, 1, 127), (12, 1, 112), (3, 0, 15), (0, 0, 0))


def lagrange_scale(points, which):
    product = 1.0
    for other in range(4):
        if other != which:
            product = product * (points[which] - points[other])
    return product


def node_tables():
    points = np.array([-1.0, -1.0 / math.sqrt(5.0), 1.0 / math.sqrt(5.0), 1.0])
    weights = np.array([1.0, 5.0, 5.0, 1.0]) / 6.0
    derivative = np.zeros((4, 4))
    for target in range(4):
        for source in range(4):
            if target == source:
                derivative[target, source] = sum(
                    1.0 / (points[target] - points[other]) for other in range(4) if other != target
                )
            else:
                derivative[target, source] = lagrange_scale(points, target) / (
                    lagrange_scale(points, source) * (points[target] - points[source])
                )
    return weights, derivative


WEIGHTS, DERIVATIVE = node_tables()
STIFF = WEIGHTS[:, None] * DERIVATIVE


def weighted_difference(f):
    total, gap = f[0] + f[3], f[3] - f[0]
    inner, inner_gap = f[1] + f[2], f[2] - f[1]
    result = [None] * 4
    for i in range(2):
        q = 0.5 * STIFF[i]
        odd = float(q[3] - q[0]) * gap + float(q[2] - q[1]) * inner_gap
        even = float(q[0] + q[3]) * total + float(q[1] + q[2]) * inner
        result[i] = odd + even
        result[3 - i] = odd - even
    return result


def weighted_tendency(h, a, b):
    f = [a[n] * h[n] for n in range(NODES)]
    g = [b[n] * h[n] for n in range(NODES)]
    rows = [weighted_difference(f[4 * j : 4 * j + 4]) for j in range(4)]
    columns = [weighted_difference(g[i::4]) for i in range(4)]
    return [rows[n // 4][n % 4] + columns[n % 4][n // 4] for n in range(NODES)]


def lanes():
    return lax.broadcasted_iota(jnp.int32, (8, HALF), 1)


def sublanes():
    return lax.broadcasted_iota(jnp.int32, (8, HALF), 0)


def roll(x, shift):
    return pltpu.roll(x, (shift + 2 * HALF) % HALF, 1)


def assembled_in_patch(v):
    lane = lanes()
    column = lane % PSIDE
    for half in range(2):
        for j in range(4):
            left, right = v[half][4 * j], v[half][4 * j + 3]
            v[half][4 * j + 3] = right + jnp.where(column < PSIDE - 1, roll(left, -1), 0.0)
            v[half][4 * j] = left + jnp.where(column > 0, roll(right, 1), 0.0)
    edge = HALF - PSIDE
    for i in range(4):
        low = [v[0][i], v[1][i]]
        high = [v[0][12 + i], v[1][12 + i]]
        down = [roll(low[0], -PSIDE), roll(low[1], -PSIDE)]
        up = [roll(high[0], PSIDE), roll(high[1], PSIDE)]
        v[0][12 + i] = high[0] + jnp.where(lane < edge, down[0], down[1])
        v[1][12 + i] = high[1] + jnp.where(lane < edge, down[1], 0.0)
        v[0][i] = low[0] + jnp.where(lane >= PSIDE, up[0], 0.0)
        v[1][i] = low[1] + jnp.where(lane >= PSIDE, up[1], up[0])
    return v


def lines_of(v, slot):
    lane = lanes()
    column, block = lane % PSIDE, lane // PSIDE
    found = []
    for half in range(2):
        east = west = 0.0
        for j in range(4):
            at = 4 * slot + j
            east = east + jnp.where(column == at, roll(v[half][4 * j + 3], at - (PSIDE - 1)), 0.0)
            west = west + jnp.where(column == at, roll(v[half][4 * j], at), 0.0)
        found += [(0, half, east), (1, half, west)]
    north = south = 0.0
    for i in range(4):
        at = 4 * (slot % 2) + i
        north = north + jnp.where(
            block == at, roll(v[1][12 + i], PSIDE * at - (HALF - PSIDE)), 0.0
        )
        south = south + jnp.where(block == at, roll(v[0][i], PSIDE * at), 0.0)
    return found + [(2, slot // 2, north), (3, slot // 2, south)]


def corners_of(v, slot, corners):
    lane, sub = lanes(), sublanes()
    result = []
    for k, (node, half, where) in enumerate(CORNERS):
        value = jnp.broadcast_to(v[half][node][:, where : where + 1], (8, HALF))
        result.append(corners[k] + jnp.where(lane == 8 * slot + sub, value, 0.0))
    return tuple(result)


def placed_lines(slot, lines):
    lane = lanes()
    column = lane % PSIDE
    found = []
    for half in range(2):
        east, west = lines[0, half], lines[1, half]
        for j in range(4):
            at = 4 * slot + j
            found.append((half, 4 * j + 3, column == PSIDE - 1, roll(east, PSIDE - 1 - at)))
            found.append((half, 4 * j, column == 0, roll(west, -at)))
    north, south = lines[2, slot // 2], lines[3, slot // 2]
    for i in range(4):
        at = 4 * (slot % 2) + i
        found.append(
            (1, 12 + i, lane >= HALF - PSIDE, roll(north, HALF - PSIDE - PSIDE * at))
        )
        found.append((0, i, lane < PSIDE, roll(south, -PSIDE * at)))
    return found


def borders_of(slot, lines, corners):
    lane, sub = lanes(), sublanes()
    extra = [{}, {}]
    found = placed_lines(slot, lines)
    for k, (node, half, where) in enumerate(CORNERS):
        row = jnp.broadcast_to(corners[k], (8, HALF))
        value = jnp.sum(jnp.where(lane == 8 * slot + sub, row, 0.0), axis=1, keepdims=True)
        found.append((half, node, lane == where, value))
    for half, node, mask, value in found:
        part = jnp.where(mask, value, 0.0)
        extra[half][node] = extra[half][node] + part if node in extra[half] else part
    return extra


def permuted(x, table):
    high = x.astype(jnp.bfloat16)
    rest = x - high.astype(jnp.float32)
    middle = rest.astype(jnp.bfloat16)
    low = (rest - middle.astype(jnp.float32)).astype(jnp.bfloat16)
    dot = functools.partial(jnp.dot, preferred_element_type=jnp.float32)
    return dot(high, table) + dot(middle, table) + dot(low, table)


def halves(x):
    return [x[:, :HALF], x[:, HALF:]]


def kernel(
    n_elem,
    n_lev,
    trc,
    thickness,
    winds,
    metric,
    beside,
    out,
    surface,
    near,
    raw,
    small_raw,
    small,
    tables,
    state,
    rate,
    coef,
    mixed_coef,
    mass,
    shared,
    scale,
    line_send,
    line_recv,
    corner_send,
    corner_recv,
    thick,
    last,
    inverse,
    column,
    columns,
    ratio,
    ratio_recv,
    last_ratio,
    last_recv,
    edge_send,
    edge_recv,
    delta,
    result,
    in_sem,
    small_sem,
    line_ssem,
    line_rsem,
    column_ssem,
    column_rsem,
    ratio_ssem,
    ratio_rsem,
    edge_ssem,
    edge_rsem,
):
    place, level = lax.axis_index("elem"), lax.axis_index("lev")
    width = 2 * HALF
    offsets = (
        1,
        -1,
        ACROSS,
        -ACROSS,
        ACROSS + 1,
        ACROSS - 1,
        1 - ACROSS,
        -1 - ACROSS,
    )
    targets = [{"elem": lax.rem(place + offset + n_elem, n_elem)} for offset in offsets]
    peers = [{"lev": lax.rem(level + k, n_lev)} for k in range(1, n_lev)]

    barrier = pltpu.get_barrier_semaphore()
    for target in targets + peers:
        pl.semaphore_signal(barrier, inc=1, device_id=target, device_id_type=MESH)

    near_copy = pltpu.make_async_copy(beside, near, small_sem.at[0])
    near_copy.start()
    pieces = [
        (trc.at[pl.ds(768, 32)], 0, 32),
        (thickness, 32, 32),
        (winds, 64, 64),
        (metric, 128, 16),
    ]
    small_copies = []
    for k, (source, start, size) in enumerate(pieces):
        copy = pltpu.make_async_copy(
            source, small_raw.at[pl.ds(start, size)], small_sem.at[k + 1]
        )
        copy.start()
        small_copies.append(copy)
    in_copies = []
    for half in range(2):
        copy = pltpu.make_async_copy(
            trc.at[pl.ds(0, 768), pl.ds(HALF * half, HALF)], raw.at[half], in_sem.at[half]
        )
        copy.start()
        in_copies.append(copy)

    line_send[...] = jnp.zeros_like(line_send)
    edge_send[...] = jnp.zeros_like(edge_send)

    @pl.when(level == 0)
    def _():
        edge_recv[1] = jnp.zeros_like(edge_recv[1])
        ratio_recv[:, 1] = jnp.zeros_like(ratio_recv[:, 1])
        last_recv[1] = jnp.zeros_like(last_recv[1])

    @pl.when(level == n_lev - 1)
    def _():
        edge_recv[0] = jnp.zeros_like(edge_recv[0])
        ratio_recv[:, 0] = jnp.zeros_like(ratio_recv[:, 0])
        last_recv[0] = jnp.zeros_like(last_recv[0])

    near_copy.wait()
    dot = functools.partial(jnp.dot, preferred_element_type=jnp.float32)
    element = lax.broadcasted_iota(jnp.int32, (width, width), 0)
    own = near[...] - place * width
    spots = []
    for side in (1, 3):
        step = jnp.where(own[side : side + 1, :] == element, 1.0, 0.0).astype(jnp.bfloat16)
        count = dot(jnp.ones((8, width), jnp.bfloat16), step)
        for doubling in range(4):
            count = count + dot(count.astype(jnp.bfloat16), step)
            if doubling < 3:
                step = dot(step, step).astype(jnp.bfloat16)
        spots.append(count)
    spot = (spots[0] + PSIDE * spots[1]).astype(jnp.int32)[0:1, :]
    to_drawn = jnp.where(spot == element, 1.0, 0.0)
    tables[1] = to_drawn.astype(jnp.bfloat16)
    tables[0] = jnp.transpose(to_drawn).astype(jnp.bfloat16)

    for copy in small_copies:
        copy.wait()
    small[...] = permuted(small_raw[...], tables[0])
    node = lax.broadcasted_iota(jnp.int32, (NODES, width), 0)
    point_i, point_j = node % 4, node // 4
    ends, inside = float(WEIGHTS[0]), float(WEIGHTS[1])
    weight_i = jnp.where((point_i == 0) | (point_i == 3), ends, inside)
    weight_j = jnp.where((point_j == 0) | (point_j == 3), ends, inside)
    area = small[pl.ds(128, NODES), :]
    mass[...] = weight_i * weight_j * area
    for l in range(2):
        coef[0, l] = -(weight_j * area) * small[pl.ds(64 + 16 * l, NODES), :]
        coef[1, l] = -(weight_i * area) * small[pl.ds(96 + 16 * l, NODES), :]

    for copy in in_copies:
        copy.wait()

    def take_in(q, carry):
        t, l = (q - 1) // 2, (q - 1) % 2
        x = jnp.concatenate(
            [
                jnp.concatenate(
                    [
                        raw[half, pl.ds(256 * t + 16 * l + n, 8, stride=32), :]
                        for n in range(NODES)
                    ],
                    axis=0,
                )
                for half in range(2)
            ],
            axis=1,
        )
        y = permuted(x, tables[0])
        for n in range(NODES):
            layer = small[pl.ds(32 + 16 * l + n, 1), :]
            state[q, n] = y[8 * n : 8 * n + 8] * layer
        return carry

    lax.fori_loop(1, 7, take_in, 0, unroll=True)
    wide_sub = lax.broadcasted_iota(jnp.int32, (8, width), 0)
    for n in range(NODES):
        tile = jnp.zeros((8, width), jnp.float32)
        for l in range(2):
            layer = small[pl.ds(32 + 16 * l + n, 1), :]
            tile = jnp.where(wide_sub == 2 * l, small[pl.ds(16 * l + n, 1), :] * layer, tile)
            tile = jnp.where(wide_sub == 2 * l + 1, layer, tile)
        state[0, n] = tile
        for k in range(2):
            mixed_coef[k, n] = jnp.where(
                wide_sub < 2, coef[k, 0, pl.ds(n, 1), :], coef[k, 1, pl.ds(n, 1), :]
            )

    def level_coef(l, half):
        at = pl.ds(HALF * half, HALF)
        return [[coef[k, l, pl.ds(n, 1), at] for n in range(NODES)] for k in range(2)]

    def both_coef(half):
        at = pl.ds(HALF * half, HALF)
        return [[mixed_coef[k, n, :, at] for n in range(NODES)] for k in range(2)]

    def load(ref, q):
        return [
            [ref[q, n, :, pl.ds(HALF * half, HALF)] for n in range(NODES)] for half in range(2)
        ]

    def save(ref, q, v):
        for half in range(2):
            for n in range(NODES):
                ref[q, n, :, pl.ds(HALF * half, HALF)] = v[half][n]

    def scaled(half):
        at = pl.ds(HALF * half, HALF)
        return [scale[pl.ds(n, 1), at] for n in range(NODES)]

    def rates_of(q, h, mixed):
        v = []
        for half in range(2):
            a, b = both_coef(half) if mixed else level_coef((q - 1) % 2, half)
            rates = weighted_tendency(h[half], a, b)
            if mixed:
                at = pl.ds(HALF * half, HALF)
                rates = [
                    jnp.where(sublanes() == 4, mass[pl.ds(n, 1), at], rates[n])
                    for n in range(NODES)
                ]
            v.append(rates)
        return assembled_in_patch(v)

    def pack(v, q, stage, group, corners):
        slot = q - slot_base[group]
        for side, half, value in lines_of(v, slot):
            line_send[stage, group, side, half] += value
        return corners_of(v, slot, corners)

    def exchange(stage, group, corners):
        for k in range(4):
            corner_send[stage, group, k] = jnp.sum(corners[k], axis=0, keepdims=True)
        copies = []
        for side in (2, 3, 4, 5, 6, 7, 0, 1):
            if side < 4:
                source = line_send.at[stage, group, side]
                landing = line_recv.at[stage, group, OPPOSITE[side]]
            else:
                source = corner_send.at[stage, group, side - 4]
                landing = corner_recv.at[stage, group, OPPOSITE[side] - 4]
            copy = pltpu.make_async_remote_copy(
                src_ref=source,
                dst_ref=landing,
                send_sem=line_ssem.at[stage, group, side],
                recv_sem=line_rsem.at[stage, group, OPPOSITE[side]],
                device_id=targets[side],
                device_id_type=MESH,
            )
            copy.start()
            copies.append(copy)
        return copies

    def extra_of(q, stage, group):
        rows = [corner_recv[stage, group, k] for k in range(4)]
        return borders_of(q - slot_base[group], line_recv.at[stage, group], rows)

    no_corners = tuple(jnp.zeros((8, HALF), jnp.float32) for _ in range(4))
    tiles_of = ((1, 3), (3, 7))
    slot_base = (0, 3)

    def first(q, corners, group, mixed=False):
        v = rates_of(q, load(state, q), mixed)
        save(rate, q, v)
        return pack(v, q, 0, group, corners)

    first_sends, second_sends = [], []
    for group in range(2):
        corners = first(0, no_corners, 0, True) if group == 0 else no_corners
        corners = lax.fori_loop(
            *tiles_of[group], lambda q, c: first(q, c, group), corners, unroll=True
        )
        if group == 0:
            pl.semaphore_wait(barrier, len(targets) + len(peers))
        first_sends.append(exchange(0, group, corners))

    below = {"lev": lax.rem(level + n_lev - 1, n_lev)}
    above = {"lev": lax.rem(level + 1, n_lev)}
    has_below, has_above = level > 0, level < n_lev - 1

    def ratio_copy(t, l):
        return pltpu.make_async_remote_copy(
            src_ref=last_ratio.at[l] if t == 3 else ratio.at[t, l],
            dst_ref=last_recv.at[l] if t == 3 else ratio_recv.at[t, l],
            send_sem=ratio_ssem.at[t, l],
            recv_sem=ratio_rsem.at[t, l],
            device_id=below if l == 0 else above,
            device_id_type=MESH,
        )

    def send_ratios(t):
        pl.when(has_below)(lambda: ratio_copy(t, 0).start())
        pl.when(has_above)(lambda: ratio_copy(t, 1).start())

    def edge_copy(l):
        return pltpu.make_async_remote_copy(
            src_ref=edge_send.at[l],
            dst_ref=edge_recv.at[l],
            send_sem=edge_ssem.at[l],
            recv_sem=edge_rsem.at[l],
            device_id=below if l == 0 else above,
            device_id_type=MESH,
        )

    def second(q, corners, group, mixed=False):
        v = load(rate, q)
        extra = extra_of(q, 0, group)
        for half in range(2):
            for n in extra[half]:
                v[half][n] = v[half][n] + extra[half][n]
        if mixed:
            for half in range(2):
                for n in range(NODES):
                    shared[pl.ds(n, 1), pl.ds(HALF * half, HALF)] = v[half][n][4:5, :]
            scale[...] = time_step / shared[...]
        h = load(state, q)
        for half in range(2):
            c = scaled(half)
            for n in range(NODES):
                middle = h[half][n] + c[n] * v[half][n]
                state[q, n, :, pl.ds(HALF * half, HALF)] = h[half][n] + middle
                h[half][n] = middle
        v = rates_of(q, h, mixed)
        h = load(state, q)
        for half in range(2):
            c = scaled(half)
            for n in range(NODES):
                h[half][n] = 0.5 * (h[half][n] + c[n] * v[half][n])
        save(state, q, h)
        if mixed:
            split_mixed(h)
            for l in range(2):
                last_ratio[l] = last[l] * inverse[l]
        else:
            t, l = (q - 1) // 2, (q - 1) % 2
            for half in range(2):
                at = pl.ds(HALF * half, HALF)
                for n in range(NODES):
                    ratio[t, l, n, :, at] = h[half][n] * inverse[l, pl.ds(n, 1), at]
        return pack(v, q, 1, group, corners)

    def split_mixed(h):
        for half in range(2):
            at = pl.ds(HALF * half, HALF)
            for n in range(NODES):
                for l in range(2):
                    last[l, pl.ds(n, 1), at] = h[half][n][2 * l : 2 * l + 1, :]
                    thick[l, pl.ds(n, 1), at] = h[half][n][2 * l + 1 : 2 * l + 2, :]
        for l in range(2):
            inverse[l] = 1.0 / thick[l]

    for group in range(2):
        for copy in first_sends[group]:
            copy.wait_recv()
        corners = second(0, no_corners, 0, True) if group == 0 else no_corners
        for t in ((0,), (1, 2))[group]:
            corners = lax.fori_loop(
                2 * t + 1, 2 * t + 3, lambda q, c: second(q, c, group), corners, unroll=True
            )
            if t == 0:
                send_ratios(3)
            if t < 2:
                send_ratios(t)
        second_sends.append(exchange(1, group, corners))

    def finish(q, group, mixed=False):
        extra = extra_of(q, 1, group)
        h = load(state, q)
        for half in range(2):
            c = scaled(half)
            at = pl.ds(HALF * half, HALF)
            for n in extra[half]:
                h[half][n] = h[half][n] + 0.5 * (c[n] * extra[half][n])
                state[q, n, :, at] = h[half][n]
        return h

    def send_outline(q, h, l, slot, factor):
        r = [[h[half][n] * factor(half, n) for n in range(NODES)] for half in range(2)]
        for side, half, value in lines_of(r, slot):
            edge_send[l, side, half] += value

    def finish_levels(q, carry, group):
        t, l = (q - 1) // 2, (q - 1) % 2
        h = finish(q, group)
        send_outline(
            q, h, l, t, lambda half, n: inverse[l, pl.ds(n, 1), pl.ds(HALF * half, HALF)]
        )
        return carry

    column_copies = []
    for group in range(2):
        for copy in second_sends[group]:
            copy.wait_recv()
        if group == 0:
            h = finish(0, 0)
            split_mixed(h)
            column[...] = thick[0] + thick[1]
            for k, peer in enumerate(peers):
                copy = pltpu.make_async_remote_copy(
                    src_ref=column,
                    dst_ref=columns.at[k],
                    send_sem=column_ssem.at[k],
                    recv_sem=column_rsem.at[k],
                    device_id=peer,
                    device_id_type=MESH,
                )
                copy.start()
                column_copies.append(copy)
            for l in range(2):
                send_outline(
                    0,
                    h,
                    l,
                    3,
                    lambda half, n: inverse[l, pl.ds(n, 1), pl.ds(HALF * half, HALF)],
                )
        lax.fori_loop(
            *tiles_of[group], lambda q, c: finish_levels(q, c, group), 0, unroll=True
        )
    pl.when(has_below)(lambda: edge_copy(0).start())
    pl.when(has_above)(lambda: edge_copy(1).start())
    send_ratios(2)

    for copy in column_copies:
        copy.wait_recv()
    own_column = column[...]
    others = jnp.zeros_like(own_column)
    under = jnp.zeros_like(own_column)
    for k in range(1, n_lev):
        part = columns[k - 1]
        others = others + part
        under = under + jnp.where(k <= level, part, 0.0)
    surface_rows = own_column + others
    levels = 2 * n_lev

    def as_float(k):
        return k.astype(jnp.float32)

    for k in range(3):
        edge_level = as_float(2 * level + k)
        fraction = (edge_level + edge_level * (edge_level - 1.0) * (1.0 / (levels - 1))) * (
            0.5 / levels
        )
        if k > 0:
            under = under + thick[k - 1]
        delta[k] = under - surface_rows * fraction
    for l in range(2):
        share = (1.0 + 2.0 * as_float(2 * level + l) * (1.0 / (levels - 1))) * (0.5 / levels)
        delta[3 + l] = 1.0 / (surface_rows * share)

    def wait_ratios(t):
        pl.when(has_above)(lambda: ratio_copy(t, 0).wait_recv())
        pl.when(has_below)(lambda: ratio_copy(t, 1).wait_recv())

    def remapped(d, carried, own_ratio, ratio_above, ratio_below):
        low = d[0] * jnp.where(d[0] > 0.0, ratio_below, own_ratio[0])
        middle = d[1] * jnp.where(d[1] > 0.0, own_ratio[0], own_ratio[1])
        high = d[2] * jnp.where(d[2] > 0.0, own_ratio[1], ratio_above)
        return (carried[0] + low - middle) * d[3], (carried[1] + middle - high) * d[4]

    pl.when(has_above)(lambda: edge_copy(0).wait_recv())
    pl.when(has_below)(lambda: edge_copy(1).wait_recv())
    wait_ratios(3)
    for l in range(2):
        for half, n, mask, value in placed_lines(3, edge_recv.at[l]):
            row, at = pl.ds(n, 1), pl.ds(HALF * half, HALF)
            last_recv[l, row, at] = jnp.where(
                mask[0:1], value[2 * l : 2 * l + 1], last_recv[l, row, at]
            )
    d = [delta[k] for k in range(5)]
    first, second = remapped(
        d,
        [last[0], last[1]],
        [last[0] * inverse[0], last[1] * inverse[1]],
        last_recv[0],
        last_recv[1],
    )
    rows = permuted(jnp.concatenate([first, second, surface_rows], axis=0), tables[1])
    out[pl.ds(768, 32), :] = rows[0:32]
    surface[...] = rows[32:48]
    for t in range(3):
        wait_ratios(t)
        beside_block = []
        for l in range(2):
            r = load(ratio_recv.at[t], l)
            for half, n, mask, value in placed_lines(t, edge_recv.at[l]):
                r[half][n] = jnp.where(mask, value, r[half][n])
            beside_block.append(r)
        pairs = []
        for n in range(NODES):
            parts = []
            for half in range(2):
                at = pl.ds(HALF * half, HALF)
                d = [delta[k, pl.ds(n, 1), at] for k in range(5)]
                carried = [state[2 * t + 1 + l, n, :, at] for l in range(2)]
                own_ratio = [carried[l] * inverse[l, pl.ds(n, 1), at] for l in range(2)]
                parts.append(
                    remapped(d, carried, own_ratio, beside_block[0][half][n], beside_block[1][half][n])
                )
            pairs.append(
                [jnp.concatenate([parts[0][l], parts[1][l]], axis=1) for l in range(2)]
            )
        for l in range(2):
            tiles = permuted(jnp.concatenate([pair[l] for pair in pairs], axis=0), tables[1])
            for n in range(NODES):
                for half in range(2):
                    result[half, pl.ds(256 * t + 16 * l + n, 8, stride=32), :] = tiles[
                        8 * n : 8 * n + 8, HALF * half : HALF * half + HALF
                    ]
        rows = pl.ds(256 * t, 256)
        for half in range(2):
            out[rows, pl.ds(HALF * half, HALF)] = result[half, rows, :]
    for copy in sum(first_sends + second_sends, column_copies):
        copy.wait_send()
    for t in range(4):
        pl.when(has_below)(lambda t=t: ratio_copy(t, 0).wait_send())
        pl.when(has_above)(lambda t=t: ratio_copy(t, 1).wait_send())
    pl.when(has_below)(lambda: edge_copy(0).wait_send())
    pl.when(has_above)(lambda: edge_copy(1).wait_send())


def store(result, surface, out, surf, sem):
    copies = [pltpu.make_async_copy(surface, surf, sem.at[4])]
    for k in range(4):
        rows = pl.ds(200 * k, 200)
        copies.append(pltpu.make_async_copy(result.at[rows], out.at[rows], sem.at[k]))
    for copy in copies:
        copy.start()
    for copy in copies:
        copy.wait()


def per_device(n_elem, n_lev, tracers, layer_mass, winds, metric, neighbours):
    width = metric.shape[-1]
    f32 = jnp.float32
    tile = (NODES, 8, width)
    dma = pltpu.SemaphoreType.DMA
    scratch = [
        pltpu.VMEM((8, width), jnp.int32),
        pltpu.VMEM((2, 768, HALF), f32),
        pltpu.VMEM((144, width), f32),
        pltpu.VMEM((144, width), f32),
        pltpu.VMEM((2, width, width), jnp.bfloat16),
        pltpu.VMEM((7,) + tile, f32),
        pltpu.VMEM((7,) + tile, f32),
        pltpu.VMEM((2, 2, NODES, width), f32),
        pltpu.VMEM((2,) + tile, f32),
        pltpu.VMEM((NODES, width), f32),
        pltpu.VMEM((NODES, width), f32),
        pltpu.VMEM((NODES, width), f32),
        pltpu.VMEM((2, 2, 4, 2, 8, HALF), f32),
        pltpu.VMEM((2, 2, 4, 2, 8, HALF), f32),
        pltpu.VMEM((2, 2, 4, 1, HALF), f32),
        pltpu.VMEM((2, 2, 4, 1, HALF), f32),
        pltpu.VMEM((2, NODES, width), f32),
        pltpu.VMEM((2, NODES, width), f32),
        pltpu.VMEM((2, NODES, width), f32),
        pltpu.VMEM((NODES, width), f32),
        pltpu.VMEM((n_lev - 1, NODES, width), f32),
        pltpu.VMEM((3, 2) + tile, f32),
        pltpu.VMEM((3, 2) + tile, f32),
        pltpu.VMEM((2, NODES, width), f32),
        pltpu.VMEM((2, NODES, width), f32),
        pltpu.VMEM((2, 4, 2, 8, HALF), f32),
        pltpu.VMEM((2, 4, 2, 8, HALF), f32),
        pltpu.VMEM((5, NODES, width), f32),
        pltpu.VMEM((2, 768, HALF), f32),
        dma((2,)),
        dma((5,)),
        dma((2, 2, 8)),
        dma((2, 2, 8)),
        dma((n_lev - 1,)),
        dma((n_lev - 1,)),
        dma((4, 2)),
        dma((4, 2)),
        dma((2,)),
        dma((2,)),
    ]
    result, surface = pl.pallas_call(
        functools.partial(kernel, n_elem, n_lev),
        out_shape=(
            jax.ShapeDtypeStruct((800, width), f32),
            jax.ShapeDtypeStruct((NODES, width), f32),
        ),
        in_specs=[pl.BlockSpec(memory_space=pltpu.HBM)] * 5,
        out_specs=(pl.BlockSpec(memory_space=pltpu.VMEM),) * 2,
        scratch_shapes=scratch,
        compiler_params=pltpu.CompilerParams(
            collective_id=0, has_side_effects=True, vmem_limit_bytes=24 * 1024 * 1024
        ),
        name="transport",
    )(
        *[
            pltpu.with_memory_space_constraint(x, pltpu.HBM)
            for x in (
                tracers.reshape(-1, width),
                layer_mass.reshape(-1, width),
                winds.reshape(-1, width),
                metric,
                jnp.transpose(neighbours),
            )
        ]
    )
    result, surface = pl.pallas_call(
        store,
        out_shape=(
            jax.ShapeDtypeStruct(result.shape, f32),
            jax.ShapeDtypeStruct(surface.shape, f32),
        ),
        in_specs=[pl.BlockSpec(memory_space=pltpu.VMEM)] * 2,
        out_specs=(pl.BlockSpec(memory_space=pltpu.HBM),) * 2,
        scratch_shapes=[dma((5,))],
        compiler_params=pltpu.CompilerParams(vmem_limit_bytes=24 * 1024 * 1024),
        name="store",
    )(result, surface)
    return result.reshape(tracers.shape), surface


def solution(mesh):
    placed = (
        P(None, "lev", None, ("members", "elem")),
        P("lev", None, ("members", "elem")),
        P(None, "lev", None, ("members", "elem")),
        P(None, "elem"),
        P("elem", None),
    )
    return jax.shard_map(
        functools.partial(per_device, mesh.shape["elem"], mesh.shape["lev"]),
        mesh=mesh,
        in_specs=placed,
        out_specs=(P(None, "lev", None, ("members", "elem")), P(None, ("members", "elem"))),
        check_vma=False,
    )
```

```python
import functools
import math

import jax
import jax.numpy as jnp
import numpy as np
from jax import lax
from jax.experimental import pallas as pl
from jax.experimental.pallas import tpu as pltpu
from jax.sharding import PartitionSpec as P

MESH = pl.DeviceIdType.MESH
PSIDE = 16
ACROSS = 8
NODES = 16
HALF = 128
time_step = 0.035

OPPOSITE = (1, 0, 3, 2, 7, 6, 5, 4)
CORNERS = ((15, 1, 127), (12, 1, 112), (3, 0, 15), (0, 0, 0))


def lagrange_scale(points, which):
    product = 1.0
    for other in range(4):
        if other != which:
            product = product * (points[which] - points[other])
    return product


def node_tables():
    points = np.array([-1.0, -1.0 / math.sqrt(5.0), 1.0 / math.sqrt(5.0), 1.0])
    weights = np.array([1.0, 5.0, 5.0, 1.0]) / 6.0
    derivative = np.zeros((4, 4))
    for target in range(4):
        for source in range(4):
            if target == source:
                derivative[target, source] = sum(
                    1.0 / (points[target] - points[other]) for other in range(4) if other != target
                )
            else:
                derivative[target, source] = lagrange_scale(points, target) / (
                    lagrange_scale(points, source) * (points[target] - points[source])
                )
    return weights, derivative


WEIGHTS, DERIVATIVE = node_tables()
STIFF = WEIGHTS[:, None] * DERIVATIVE


def weighted_difference(f):
    total, gap = f[0] + f[3], f[3] - f[0]
    inner, inner_gap = f[1] + f[2], f[2] - f[1]
    result = [None] * 4
    for i in range(2):
        q = 0.5 * STIFF[i]
        odd = float(q[3] - q[0]) * gap + float(q[2] - q[1]) * inner_gap
        even = float(q[0] + q[3]) * total + float(q[1] + q[2]) * inner
        result[i] = odd + even
        result[3 - i] = odd - even
    return result


def weighted_tendency(h, a, b):
    f = [a[n] * h[n] for n in range(NODES)]
    g = [b[n] * h[n] for n in range(NODES)]
    rows = [weighted_difference(f[4 * j : 4 * j + 4]) for j in range(4)]
    columns = [weighted_difference(g[i::4]) for i in range(4)]
    return [rows[n // 4][n % 4] + columns[n % 4][n // 4] for n in range(NODES)]


def lanes():
    return lax.broadcasted_iota(jnp.int32, (8, HALF), 1)


def sublanes():
    return lax.broadcasted_iota(jnp.int32, (8, HALF), 0)


def roll(x, shift):
    return pltpu.roll(x, (shift + 2 * HALF) % HALF, 1)


def assembled_in_patch(v):
    lane = lanes()
    column = lane % PSIDE
    for half in range(2):
        for j in range(4):
            left, right = v[half][4 * j], v[half][4 * j + 3]
            v[half][4 * j + 3] = right + jnp.where(column < PSIDE - 1, roll(left, -1), 0.0)
            v[half][4 * j] = left + jnp.where(column > 0, roll(right, 1), 0.0)
    edge = HALF - PSIDE
    for i in range(4):
        low = [v[0][i], v[1][i]]
        high = [v[0][12 + i], v[1][12 + i]]
        down = [roll(low[0], -PSIDE), roll(low[1], -PSIDE)]
        up = [roll(high[0], PSIDE), roll(high[1], PSIDE)]
        v[0][12 + i] = high[0] + jnp.where(lane < edge, down[0], down[1])
        v[1][12 + i] = high[1] + jnp.where(lane < edge, down[1], 0.0)
        v[0][i] = low[0] + jnp.where(lane >= PSIDE, up[0], 0.0)
        v[1][i] = low[1] + jnp.where(lane >= PSIDE, up[1], up[0])
    return v


def lines_of(v, slot):
    lane = lanes()
    column, block = lane % PSIDE, lane // PSIDE
    found = []
    for half in range(2):
        east = west = 0.0
        for j in range(4):
            at = 4 * slot + j
            east = east + jnp.where(column == at, roll(v[half][4 * j + 3], at - (PSIDE - 1)), 0.0)
            west = west + jnp.where(column == at, roll(v[half][4 * j], at), 0.0)
        found += [(0, half, east), (1, half, west)]
    north = south = 0.0
    for i in range(4):
        at = 4 * (slot % 2) + i
        north = north + jnp.where(
            block == at, roll(v[1][12 + i], PSIDE * at - (HALF - PSIDE)), 0.0
        )
        south = south + jnp.where(block == at, roll(v[0][i], PSIDE * at), 0.0)
    return found + [(2, slot // 2, north), (3, slot // 2, south)]


def corners_of(v, slot, corners):
    lane, sub = lanes(), sublanes()
    result = []
    for k, (node, half, where) in enumerate(CORNERS):
        value = jnp.broadcast_to(v[half][node][:, where : where + 1], (8, HALF))
        result.append(corners[k] + jnp.where(lane == 8 * slot + sub, value, 0.0))
    return tuple(result)


def placed_lines(slot, lines):
    lane = lanes()
    column = lane % PSIDE
    found = []
    for half in range(2):
        east, west = lines[0, half], lines[1, half]
        for j in range(4):
            at = 4 * slot + j
            found.append((half, 4 * j + 3, column == PSIDE - 1, roll(east, PSIDE - 1 - at)))
            found.append((half, 4 * j, column == 0, roll(west, -at)))
    north, south = lines[2, slot // 2], lines[3, slot // 2]
    for i in range(4):
        at = 4 * (slot % 2) + i
        found.append(
            (1, 12 + i, lane >= HALF - PSIDE, roll(north, HALF - PSIDE - PSIDE * at))
        )
        found.append((0, i, lane < PSIDE, roll(south, -PSIDE * at)))
    return found


def borders_of(slot, lines, corners):
    lane, sub = lanes(), sublanes()
    extra = [{}, {}]
    found = placed_lines(slot, lines)
    for k, (node, half, where) in enumerate(CORNERS):
        row = jnp.broadcast_to(corners[k], (8, HALF))
        value = jnp.sum(jnp.where(lane == 8 * slot + sub, row, 0.0), axis=1, keepdims=True)
        found.append((half, node, lane == where, value))
    for half, node, mask, value in found:
        part = jnp.where(mask, value, 0.0)
        extra[half][node] = extra[half][node] + part if node in extra[half] else part
    return extra


def permuted(x, table):
    high = x.astype(jnp.bfloat16)
    rest = x - high.astype(jnp.float32)
    middle = rest.astype(jnp.bfloat16)
    low = (rest - middle.astype(jnp.float32)).astype(jnp.bfloat16)
    size = x.shape[0]
    parts = jnp.concatenate([high, middle, low], axis=0)
    y = jnp.dot(parts, table, preferred_element_type=jnp.float32)
    return y[:size] + y[size : 2 * size] + y[2 * size :]


def halves(x):
    return [x[:, :HALF], x[:, HALF:]]


def kernel(
    n_elem,
    n_lev,
    trc,
    thickness,
    winds,
    metric,
    beside,
    result,
    last_rows,
    near,
    raw,
    small_raw,
    small,
    tables,
    state,
    rate,
    coef,
    mixed_coef,
    mass,
    shared,
    scale,
    line_send,
    line_recv,
    corner_send,
    corner_recv,
    thick,
    last,
    inverse,
    column,
    columns,
    ratio,
    ratio_recv,
    last_ratio,
    last_recv,
    edge_send,
    edge_recv,
    delta,
    in_sem,
    small_sem,
    line_ssem,
    line_rsem,
    column_ssem,
    column_rsem,
    ratio_ssem,
    ratio_rsem,
    edge_ssem,
    edge_rsem,
):
    place, level = lax.axis_index("elem"), lax.axis_index("lev")
    width = 2 * HALF
    offsets = (
        1,
        -1,
        ACROSS,
        -ACROSS,
        ACROSS + 1,
        ACROSS - 1,
        1 - ACROSS,
        -1 - ACROSS,
    )
    targets = [{"elem": lax.rem(place + offset + n_elem, n_elem)} for offset in offsets]
    peers = [{"lev": lax.rem(level + k, n_lev)} for k in range(1, n_lev)]

    barrier = pltpu.get_barrier_semaphore()
    for target in targets[2:] + peers + targets[:2]:
        pl.semaphore_signal(barrier, inc=1, device_id=target, device_id_type=MESH)

    near_copy = pltpu.make_async_copy(beside, near, small_sem.at[0])
    near_copy.start()
    pieces = [
        (trc.at[pl.ds(768, 32)], 0, 32),
        (thickness, 32, 32),
        (winds, 64, 64),
        (metric, 128, 16),
    ]
    small_copies = []
    for k, (source, start, size) in enumerate(pieces):
        copy = pltpu.make_async_copy(
            source, small_raw.at[pl.ds(start, size)], small_sem.at[k + 1]
        )
        copy.start()
        small_copies.append(copy)
    in_copies = []
    for half in range(2):
        copy = pltpu.make_async_copy(
            trc.at[pl.ds(0, 768), pl.ds(HALF * half, HALF)], raw.at[half], in_sem.at[half]
        )
        copy.start()
        in_copies.append(copy)

    line_send[...] = jnp.zeros_like(line_send)
    edge_send[...] = jnp.zeros_like(edge_send)

    @pl.when(level == 0)
    def _():
        edge_recv[1] = jnp.zeros_like(edge_recv[1])
        ratio_recv[:, 1] = jnp.zeros_like(ratio_recv[:, 1])
        last_recv[1] = jnp.zeros_like(last_recv[1])

    @pl.when(level == n_lev - 1)
    def _():
        edge_recv[0] = jnp.zeros_like(edge_recv[0])
        ratio_recv[:, 0] = jnp.zeros_like(ratio_recv[:, 0])
        last_recv[0] = jnp.zeros_like(last_recv[0])

    near_copy.wait()
    dot = functools.partial(jnp.dot, preferred_element_type=jnp.float32)
    element = lax.broadcasted_iota(jnp.int32, (width, width), 0)
    own = near[...] - place * width
    spots = []
    for side in (1, 3):
        step = jnp.where(own[side : side + 1, :] == element, 1.0, 0.0).astype(jnp.bfloat16)
        count = dot(jnp.ones((8, width), jnp.bfloat16), step)
        for doubling in range(4):
            count = count + dot(count.astype(jnp.bfloat16), step)
            if doubling < 3:
                step = dot(step, step).astype(jnp.bfloat16)
        spots.append(count)
    spot = (spots[0] + PSIDE * spots[1]).astype(jnp.int32)[0:1, :]
    to_drawn = jnp.where(spot == element, 1.0, 0.0)
    tables[1] = to_drawn.astype(jnp.bfloat16)
    tables[0] = jnp.transpose(to_drawn).astype(jnp.bfloat16)

    for copy in small_copies:
        copy.wait()
    small[...] = permuted(small_raw[...], tables[0])
    node = lax.broadcasted_iota(jnp.int32, (NODES, width), 0)
    point_i, point_j = node % 4, node // 4
    ends, inside = float(WEIGHTS[0]), float(WEIGHTS[1])
    weight_i = jnp.where((point_i == 0) | (point_i == 3), ends, inside)
    weight_j = jnp.where((point_j == 0) | (point_j == 3), ends, inside)
    area = small[pl.ds(128, NODES), :]
    mass[...] = weight_i * weight_j * area
    for l in range(2):
        coef[0, l] = -(weight_j * area) * small[pl.ds(64 + 16 * l, NODES), :]
        coef[1, l] = -(weight_i * area) * small[pl.ds(96 + 16 * l, NODES), :]

    for copy in in_copies:
        copy.wait()

    def take_in(q, carry):
        t, l = (q - 1) // 2, (q - 1) % 2
        x = jnp.concatenate(
            [
                jnp.concatenate(
                    [
                        raw[half, pl.ds(256 * t + 16 * l + n, 8, stride=32), :]
                        for n in range(NODES)
                    ],
                    axis=0,
                )
                for half in range(2)
            ],
            axis=1,
        )
        y = permuted(x, tables[0])
        for n in range(NODES):
            layer = small[pl.ds(32 + 16 * l + n, 1), :]
            state[q, n] = y[8 * n : 8 * n + 8] * layer
        return carry

    lax.fori_loop(1, 7, take_in, 0, unroll=True)
    wide_sub = lax.broadcasted_iota(jnp.int32, (8, width), 0)
    for n in range(NODES):
        tile = jnp.zeros((8, width), jnp.float32)
        for l in range(2):
            layer = small[pl.ds(32 + 16 * l + n, 1), :]
            tile = jnp.where(wide_sub == 2 * l, small[pl.ds(16 * l + n, 1), :] * layer, tile)
            tile = jnp.where(wide_sub == 2 * l + 1, layer, tile)
        state[0, n] = tile
        for k in range(2):
            mixed_coef[k, n] = jnp.where(
                wide_sub < 2, coef[k, 0, pl.ds(n, 1), :], coef[k, 1, pl.ds(n, 1), :]
            )

    def level_coef(l, half):
        at = pl.ds(HALF * half, HALF)
        return [[coef[k, l, pl.ds(n, 1), at] for n in range(NODES)] for k in range(2)]

    def both_coef(half):
        at = pl.ds(HALF * half, HALF)
        return [[mixed_coef[k, n, :, at] for n in range(NODES)] for k in range(2)]

    def load(ref, q):
        return [
            [ref[q, n, :, pl.ds(HALF * half, HALF)] for n in range(NODES)] for half in range(2)
        ]

    def save(ref, q, v):
        for half in range(2):
            for n in range(NODES):
                ref[q, n, :, pl.ds(HALF * half, HALF)] = v[half][n]

    def scaled(half):
        at = pl.ds(HALF * half, HALF)
        return [scale[pl.ds(n, 1), at] for n in range(NODES)]

    def rates_of(q, h, mixed):
        v = []
        for half in range(2):
            a, b = both_coef(half) if mixed else level_coef((q - 1) % 2, half)
            rates = weighted_tendency(h[half], a, b)
            if mixed:
                at = pl.ds(HALF * half, HALF)
                rates = [
                    jnp.where(sublanes() == 4, mass[pl.ds(n, 1), at], rates[n])
                    for n in range(NODES)
                ]
            v.append(rates)
        return assembled_in_patch(v)

    def pack(v, q, stage, group, corners):
        slot = q - slot_base[group]
        for side, half, value in lines_of(v, slot):
            line_send[stage, group, side, half] += value
        return corners_of(v, slot, corners)

    def exchange(stage, group, corners):
        for k in range(4):
            corner_send[stage, group, k] = jnp.sum(corners[k], axis=0, keepdims=True)
        copies = []
        for side in (2, 3, 4, 5, 6, 7, 0, 1):
            if side < 4:
                source = line_send.at[stage, group, side]
                landing = line_recv.at[stage, group, OPPOSITE[side]]
            else:
                source = corner_send.at[stage, group, side - 4]
                landing = corner_recv.at[stage, group, OPPOSITE[side] - 4]
            copy = pltpu.make_async_remote_copy(
                src_ref=source,
                dst_ref=landing,
                send_sem=line_ssem.at[stage, group, side],
                recv_sem=line_rsem.at[stage, group, OPPOSITE[side]],
                device_id=targets[side],
                device_id_type=MESH,
            )
            copy.start()
            copies.append(copy)
        return copies

    def extra_of(q, stage, group):
        rows = [corner_recv[stage, group, k] for k in range(4)]
        return borders_of(q - slot_base[group], line_recv.at[stage, group], rows)

    no_corners = tuple(jnp.zeros((8, HALF), jnp.float32) for _ in range(4))
    tiles_of = ((1, 3), (3, 7))
    slot_base = (0, 3)

    def first(q, corners, group, mixed=False):
        v = rates_of(q, load(state, q), mixed)
        save(rate, q, v)
        return pack(v, q, 0, group, corners)

    first_sends, second_sends = [], []
    for group in range(2):
        corners = first(0, no_corners, 0, True) if group == 0 else no_corners
        corners = lax.fori_loop(
            *tiles_of[group], lambda q, c: first(q, c, group), corners, unroll=True
        )
        if group == 0:
            pl.semaphore_wait(barrier, len(targets) + len(peers))
        first_sends.append(exchange(0, group, corners))

    below = {"lev": lax.rem(level + n_lev - 1, n_lev)}
    above = {"lev": lax.rem(level + 1, n_lev)}
    has_below, has_above = level > 0, level < n_lev - 1

    def ratio_copy(t, l):
        if t == 3:
            source, landing = last_ratio.at[l], last_recv.at[l]
        elif t < 2:
            source, landing = ratio.at[t, l], ratio_recv.at[t, l]
        else:
            nodes = pl.ds(0, 4) if t == 2 else pl.ds(4, NODES - 4)
            source, landing = ratio.at[2, l, nodes], ratio_recv.at[2, l, nodes]
        return pltpu.make_async_remote_copy(
            src_ref=source,
            dst_ref=landing,
            send_sem=ratio_ssem.at[t, l],
            recv_sem=ratio_rsem.at[t, l],
            device_id=below if l == 0 else above,
            device_id_type=MESH,
        )

    def send_ratios(t):
        pl.when(has_below)(lambda: ratio_copy(t, 0).start())
        pl.when(has_above)(lambda: ratio_copy(t, 1).start())

    def edge_copy(l):
        return pltpu.make_async_remote_copy(
            src_ref=edge_send.at[l],
            dst_ref=edge_recv.at[l],
            send_sem=edge_ssem.at[l],
            recv_sem=edge_rsem.at[l],
            device_id=below if l == 0 else above,
            device_id_type=MESH,
        )

    def second(q, corners, group, mixed=False):
        v = load(rate, q)
        extra = extra_of(q, 0, group)
        for half in range(2):
            for n in extra[half]:
                v[half][n] = v[half][n] + extra[half][n]
        if mixed:
            for half in range(2):
                for n in range(NODES):
                    shared[pl.ds(n, 1), pl.ds(HALF * half, HALF)] = v[half][n][4:5, :]
            scale[...] = time_step / shared[...]
        h = load(state, q)
        for half in range(2):
            c = scaled(half)
            for n in range(NODES):
                middle = h[half][n] + c[n] * v[half][n]
                state[q, n, :, pl.ds(HALF * half, HALF)] = h[half][n] + middle
                h[half][n] = middle
        v = rates_of(q, h, mixed)
        h = load(state, q)
        for half in range(2):
            c = scaled(half)
            for n in range(NODES):
                h[half][n] = 0.5 * (h[half][n] + c[n] * v[half][n])
        save(state, q, h)
        if mixed:
            split_mixed(h)
            for l in range(2):
                last_ratio[l] = last[l] * inverse[l]
        else:
            t, l = (q - 1) // 2, (q - 1) % 2
            for half in range(2):
                at = pl.ds(HALF * half, HALF)
                for n in range(NODES):
                    ratio[t, l, n, :, at] = h[half][n] * inverse[l, pl.ds(n, 1), at]
        return pack(v, q, 1, group, corners)

    def split_mixed(h):
        for half in range(2):
            at = pl.ds(HALF * half, HALF)
            for n in range(NODES):
                for l in range(2):
                    last[l, pl.ds(n, 1), at] = h[half][n][2 * l : 2 * l + 1, :]
                    thick[l, pl.ds(n, 1), at] = h[half][n][2 * l + 1 : 2 * l + 2, :]
        for l in range(2):
            inverse[l] = 1.0 / thick[l]

    for group in range(2):
        for copy in first_sends[group]:
            copy.wait_recv()
        corners = second(0, no_corners, 0, True) if group == 0 else no_corners
        for t in ((0,), (1, 2))[group]:
            corners = lax.fori_loop(
                2 * t + 1, 2 * t + 3, lambda q, c: second(q, c, group), corners, unroll=True
            )
            if t == 0:
                send_ratios(3)
            if t < 2:
                send_ratios(t)
        second_sends.append(exchange(1, group, corners))

    def finish(q, group, mixed=False):
        extra = extra_of(q, 1, group)
        h = load(state, q)
        for half in range(2):
            c = scaled(half)
            at = pl.ds(HALF * half, HALF)
            for n in extra[half]:
                h[half][n] = h[half][n] + 0.5 * (c[n] * extra[half][n])
                state[q, n, :, at] = h[half][n]
        return h

    def send_outline(q, h, l, slot, factor):
        r = [[h[half][n] * factor(half, n) for n in range(NODES)] for half in range(2)]
        for side, half, value in lines_of(r, slot):
            edge_send[l, side, half] += value

    def finish_levels(q, carry, group):
        t, l = (q - 1) // 2, (q - 1) % 2
        h = finish(q, group)
        send_outline(
            q, h, l, t, lambda half, n: inverse[l, pl.ds(n, 1), pl.ds(HALF * half, HALF)]
        )
        return carry

    column_copies = []
    for group in range(2):
        for copy in second_sends[group]:
            copy.wait_recv()
        if group == 0:
            h = finish(0, 0)
            split_mixed(h)
            column[...] = thick[0] + thick[1]
            for k, peer in enumerate(peers):
                copy = pltpu.make_async_remote_copy(
                    src_ref=column,
                    dst_ref=columns.at[k],
                    send_sem=column_ssem.at[k],
                    recv_sem=column_rsem.at[k],
                    device_id=peer,
                    device_id_type=MESH,
                )
                copy.start()
                column_copies.append(copy)
            send_ratios(2)
            for l in range(2):
                send_outline(
                    0,
                    h,
                    l,
                    3,
                    lambda half, n: inverse[l, pl.ds(n, 1), pl.ds(HALF * half, HALF)],
                )
        lax.fori_loop(
            *tiles_of[group], lambda q, c: finish_levels(q, c, group), 0, unroll=True
        )
    pl.when(has_below)(lambda: edge_copy(0).start())
    pl.when(has_above)(lambda: edge_copy(1).start())
    send_ratios(4)

    def wait_ratios(t):
        pl.when(has_above)(lambda: ratio_copy(t, 0).wait_recv())
        pl.when(has_below)(lambda: ratio_copy(t, 1).wait_recv())

    def merge_outlines(t):
        wait_ratios(t)
        if t == 2:
            wait_ratios(4)
        for l in range(2):
            found = {}
            for half, n, mask, value in placed_lines(t, edge_recv.at[l]):
                at = pl.ds(HALF * half, HALF)
                before = found.get((half, n))
                if before is None:
                    before = ratio_recv[t, l, n, :, at]
                found[half, n] = jnp.where(mask, value, before)
            for (half, n), value in found.items():
                ratio_recv[t, l, n, :, pl.ds(HALF * half, HALF)] = value

    pl.when(has_above)(lambda: edge_copy(0).wait_recv())
    pl.when(has_below)(lambda: edge_copy(1).wait_recv())
    wait_ratios(3)
    for l in range(2):
        for half, n, mask, value in placed_lines(3, edge_recv.at[l]):
            row, at = pl.ds(n, 1), pl.ds(HALF * half, HALF)
            last_recv[l, row, at] = jnp.where(
                mask[0:1], value[2 * l : 2 * l + 1], last_recv[l, row, at]
            )
    merge_outlines(0)
    merge_outlines(1)

    for copy in column_copies:
        copy.wait_recv()
    own_column = column[...]
    others = jnp.zeros_like(own_column)
    under = jnp.zeros_like(own_column)
    for k in range(1, n_lev):
        part = columns[k - 1]
        others = others + part
        under = under + jnp.where(k <= level, part, 0.0)
    surface_rows = own_column + others
    levels = 2 * n_lev

    def as_float(k):
        return k.astype(jnp.float32)

    for k in range(3):
        edge_level = as_float(2 * level + k)
        fraction = (edge_level + edge_level * (edge_level - 1.0) * (1.0 / (levels - 1))) * (
            0.5 / levels
        )
        if k > 0:
            under = under + thick[k - 1]
        delta[k] = under - surface_rows * fraction
    for l in range(2):
        share = (1.0 + 2.0 * as_float(2 * level + l) * (1.0 / (levels - 1))) * (0.5 / levels)
        delta[3 + l] = 1.0 / (surface_rows * share)

    def remapped(d, carried, own_ratio, ratio_above, ratio_below):
        low = d[0] * jnp.where(d[0] > 0.0, ratio_below, own_ratio[0])
        middle = d[1] * jnp.where(d[1] > 0.0, own_ratio[0], own_ratio[1])
        high = d[2] * jnp.where(d[2] > 0.0, own_ratio[1], ratio_above)
        return (carried[0] + low - middle) * d[3], (carried[1] + middle - high) * d[4]

    d = [delta[k] for k in range(5)]
    first, second = remapped(
        d,
        [last[0], last[1]],
        [last[0] * inverse[0], last[1] * inverse[1]],
        last_recv[0],
        last_recv[1],
    )
    rows = permuted(jnp.concatenate([first, second, surface_rows], axis=0), tables[1])
    last_rows[...] = rows
    for t in range(3):
        if t == 2:
            merge_outlines(2)
        pairs = []
        for n in range(NODES):
            parts = []
            for half in range(2):
                at = pl.ds(HALF * half, HALF)
                d = [delta[k, pl.ds(n, 1), at] for k in range(5)]
                carried = [state[2 * t + 1 + l, n, :, at] for l in range(2)]
                own_ratio = [carried[l] * inverse[l, pl.ds(n, 1), at] for l in range(2)]
                parts.append(
                    remapped(d, carried, own_ratio, ratio_recv[t, 0, n, :, at], ratio_recv[t, 1, n, :, at])
                )
            pairs.append(
                [jnp.concatenate([parts[0][l], parts[1][l]], axis=1) for l in range(2)]
            )
        tiles = permuted(
            jnp.concatenate([pair[l] for l in range(2) for pair in pairs], axis=0), tables[1]
        )
        for k in range(2 * NODES):
            for half in range(2):
                result[half, pl.ds(256 * t + k, 8, stride=32), :] = tiles[
                    8 * k : 8 * k + 8, HALF * half : HALF * half + HALF
                ]
    for copy in sum(first_sends + second_sends, column_copies):
        copy.wait_send()
    for t in range(5):
        pl.when(has_below)(lambda t=t: ratio_copy(t, 0).wait_send())
        pl.when(has_above)(lambda t=t: ratio_copy(t, 1).wait_send())
    pl.when(has_below)(lambda: edge_copy(0).wait_send())
    pl.when(has_above)(lambda: edge_copy(1).wait_send())


def store(result, last_rows, out, surf, sem):
    copies = [
        pltpu.make_async_copy(last_rows.at[pl.ds(32, 16)], surf, sem.at[0]),
        pltpu.make_async_copy(last_rows.at[pl.ds(0, 32)], out.at[pl.ds(768, 32)], sem.at[1]),
    ]
    for half in range(2):
        at = pl.ds(HALF * half, HALF)
        for k in range(2):
            rows = pl.ds(384 * k, 384)
            copies.append(
                pltpu.make_async_copy(
                    result.at[half, rows], out.at[rows, at], sem.at[2 + 2 * half + k]
                )
            )
    for copy in copies:
        copy.start()
    for copy in copies:
        copy.wait()


def per_device(n_elem, n_lev, tracers, layer_mass, winds, metric, neighbours):
    width = metric.shape[-1]
    f32 = jnp.float32
    tile = (NODES, 8, width)
    dma = pltpu.SemaphoreType.DMA
    scratch = [
        pltpu.VMEM((8, width), jnp.int32),
        pltpu.VMEM((2, 768, HALF), f32),
        pltpu.VMEM((144, width), f32),
        pltpu.VMEM((144, width), f32),
        pltpu.VMEM((2, width, width), jnp.bfloat16),
        pltpu.VMEM((7,) + tile, f32),
        pltpu.VMEM((7,) + tile, f32),
        pltpu.VMEM((2, 2, NODES, width), f32),
        pltpu.VMEM((2,) + tile, f32),
        pltpu.VMEM((NODES, width), f32),
        pltpu.VMEM((NODES, width), f32),
        pltpu.VMEM((NODES, width), f32),
        pltpu.VMEM((2, 2, 4, 2, 8, HALF), f32),
        pltpu.VMEM((2, 2, 4, 2, 8, HALF), f32),
        pltpu.VMEM((2, 2, 4, 1, HALF), f32),
        pltpu.VMEM((2, 2, 4, 1, HALF), f32),
        pltpu.VMEM((2, NODES, width), f32),
        pltpu.VMEM((2, NODES, width), f32),
        pltpu.VMEM((2, NODES, width), f32),
        pltpu.VMEM((NODES, width), f32),
        pltpu.VMEM((n_lev - 1, NODES, width), f32),
        pltpu.VMEM((3, 2) + tile, f32),
        pltpu.VMEM((3, 2) + tile, f32),
        pltpu.VMEM((2, NODES, width), f32),
        pltpu.VMEM((2, NODES, width), f32),
        pltpu.VMEM((2, 4, 2, 8, HALF), f32),
        pltpu.VMEM((2, 4, 2, 8, HALF), f32),
        pltpu.VMEM((5, NODES, width), f32),
        dma((2,)),
        dma((5,)),
        dma((2, 2, 8)),
        dma((2, 2, 8)),
        dma((n_lev - 1,)),
        dma((n_lev - 1,)),
        dma((5, 2)),
        dma((5, 2)),
        dma((2,)),
        dma((2,)),
    ]
    result, last_rows = pl.pallas_call(
        functools.partial(kernel, n_elem, n_lev),
        out_shape=(
            jax.ShapeDtypeStruct((2, 768, HALF), f32),
            jax.ShapeDtypeStruct((3 * NODES, width), f32),
        ),
        in_specs=[pl.BlockSpec(memory_space=pltpu.HBM)] * 5,
        out_specs=(pl.BlockSpec(memory_space=pltpu.VMEM),) * 2,
        scratch_shapes=scratch,
        compiler_params=pltpu.CompilerParams(
            collective_id=0, has_side_effects=True, vmem_limit_bytes=24 * 1024 * 1024
        ),
        name="transport",
    )(
        *[
            pltpu.with_memory_space_constraint(x, pltpu.HBM)
            for x in (
                tracers.reshape(-1, width),
                layer_mass.reshape(-1, width),
                winds.reshape(-1, width),
                metric,
                jnp.transpose(neighbours),
            )
        ]
    )
    out, surface = pl.pallas_call(
        store,
        out_shape=(
            jax.ShapeDtypeStruct((800, width), f32),
            jax.ShapeDtypeStruct((NODES, width), f32),
        ),
        in_specs=[pl.BlockSpec(memory_space=pltpu.VMEM)] * 2,
        out_specs=(pl.BlockSpec(memory_space=pltpu.HBM),) * 2,
        scratch_shapes=[dma((6,))],
        compiler_params=pltpu.CompilerParams(vmem_limit_bytes=24 * 1024 * 1024),
        name="store",
    )(result, last_rows)
    return out.reshape(tracers.shape), surface


def solution(mesh):
    placed = (
        P(None, "lev", None, ("members", "elem")),
        P("lev", None, ("members", "elem")),
        P(None, "lev", None, ("members", "elem")),
        P(None, "elem"),
        P("elem", None),
    )
    return jax.shard_map(
        functools.partial(per_device, mesh.shape["elem"], mesh.shape["lev"]),
        mesh=mesh,
        in_specs=placed,
        out_specs=(P(None, "lev", None, ("members", "elem")), P(None, ("members", "elem"))),
        check_vma=False,
    )
```

```python
import functools
import math

import jax
import jax.numpy as jnp
import numpy as np
from jax import lax
from jax.experimental import pallas as pl
from jax.experimental.pallas import tpu as pltpu
from jax.sharding import PartitionSpec as P

MESH = pl.DeviceIdType.MESH
PSIDE = 16
ACROSS = 8
NODES = 16
HALF = 128
time_step = 0.035

OPPOSITE = (1, 0, 3, 2, 7, 6, 5, 4)
CORNERS = ((15, 1, 127), (12, 1, 112), (3, 0, 15), (0, 0, 0))


def lagrange_scale(points, which):
    product = 1.0
    for other in range(4):
        if other != which:
            product = product * (points[which] - points[other])
    return product


def node_tables():
    points = np.array([-1.0, -1.0 / math.sqrt(5.0), 1.0 / math.sqrt(5.0), 1.0])
    weights = np.array([1.0, 5.0, 5.0, 1.0]) / 6.0
    derivative = np.zeros((4, 4))
    for target in range(4):
        for source in range(4):
            if target == source:
                derivative[target, source] = sum(
                    1.0 / (points[target] - points[other]) for other in range(4) if other != target
                )
            else:
                derivative[target, source] = lagrange_scale(points, target) / (
                    lagrange_scale(points, source) * (points[target] - points[source])
                )
    return weights, derivative


WEIGHTS, DERIVATIVE = node_tables()
STIFF = WEIGHTS[:, None] * DERIVATIVE


def weighted_difference(f):
    total, gap = f[0] + f[3], f[3] - f[0]
    inner, inner_gap = f[1] + f[2], f[2] - f[1]
    result = [None] * 4
    for i in range(2):
        q = 0.5 * STIFF[i]
        odd = float(q[3] - q[0]) * gap + float(q[2] - q[1]) * inner_gap
        even = float(q[0] + q[3]) * total + float(q[1] + q[2]) * inner
        result[i] = odd + even
        result[3 - i] = odd - even
    return result


def weighted_tendency(h, a, b):
    f = [a[n] * h[n] for n in range(NODES)]
    g = [b[n] * h[n] for n in range(NODES)]
    rows = [weighted_difference(f[4 * j : 4 * j + 4]) for j in range(4)]
    columns = [weighted_difference(g[i::4]) for i in range(4)]
    return [rows[n // 4][n % 4] + columns[n % 4][n // 4] for n in range(NODES)]


def lanes():
    return lax.broadcasted_iota(jnp.int32, (8, HALF), 1)


def sublanes():
    return lax.broadcasted_iota(jnp.int32, (8, HALF), 0)


def roll(x, shift):
    return pltpu.roll(x, (shift + 2 * HALF) % HALF, 1)


def assembled_in_patch(v):
    lane = lanes()
    column = lane % PSIDE
    for half in range(2):
        for j in range(4):
            left, right = v[half][4 * j], v[half][4 * j + 3]
            v[half][4 * j + 3] = right + jnp.where(column < PSIDE - 1, roll(left, -1), 0.0)
            v[half][4 * j] = left + jnp.where(column > 0, roll(right, 1), 0.0)
    edge = HALF - PSIDE
    for i in range(4):
        low = [v[0][i], v[1][i]]
        high = [v[0][12 + i], v[1][12 + i]]
        down = [roll(low[0], -PSIDE), roll(low[1], -PSIDE)]
        up = [roll(high[0], PSIDE), roll(high[1], PSIDE)]
        v[0][12 + i] = high[0] + jnp.where(lane < edge, down[0], down[1])
        v[1][12 + i] = high[1] + jnp.where(lane < edge, down[1], 0.0)
        v[0][i] = low[0] + jnp.where(lane >= PSIDE, up[0], 0.0)
        v[1][i] = low[1] + jnp.where(lane >= PSIDE, up[1], up[0])
    return v


def lines_of(v, slot):
    lane = lanes()
    column, block = lane % PSIDE, lane // PSIDE
    found = []
    for half in range(2):
        east = west = 0.0
        for j in range(4):
            at = 4 * slot + j
            east = east + jnp.where(column == at, roll(v[half][4 * j + 3], at - (PSIDE - 1)), 0.0)
            west = west + jnp.where(column == at, roll(v[half][4 * j], at), 0.0)
        found += [(0, half, east), (1, half, west)]
    north = south = 0.0
    for i in range(4):
        at = 4 * (slot % 2) + i
        north = north + jnp.where(
            block == at, roll(v[1][12 + i], PSIDE * at - (HALF - PSIDE)), 0.0
        )
        south = south + jnp.where(block == at, roll(v[0][i], PSIDE * at), 0.0)
    return found + [(2, slot // 2, north), (3, slot // 2, south)]


def corners_of(v, slot, corners):
    lane, sub = lanes(), sublanes()
    result = []
    for k, (node, half, where) in enumerate(CORNERS):
        value = jnp.broadcast_to(v[half][node][:, where : where + 1], (8, HALF))
        result.append(corners[k] + jnp.where(lane == 8 * slot + sub, value, 0.0))
    return tuple(result)


def placed_lines(slot, lines):
    lane = lanes()
    column = lane % PSIDE
    found = []
    for half in range(2):
        east, west = lines[0, half], lines[1, half]
        for j in range(4):
            at = 4 * slot + j
            found.append((half, 4 * j + 3, column == PSIDE - 1, roll(east, PSIDE - 1 - at)))
            found.append((half, 4 * j, column == 0, roll(west, -at)))
    north, south = lines[2, slot // 2], lines[3, slot // 2]
    for i in range(4):
        at = 4 * (slot % 2) + i
        found.append(
            (1, 12 + i, lane >= HALF - PSIDE, roll(north, HALF - PSIDE - PSIDE * at))
        )
        found.append((0, i, lane < PSIDE, roll(south, -PSIDE * at)))
    return found


def borders_of(slot, lines, corners):
    lane, sub = lanes(), sublanes()
    extra = [{}, {}]
    found = placed_lines(slot, lines)
    for k, (node, half, where) in enumerate(CORNERS):
        row = jnp.broadcast_to(corners[k], (8, HALF))
        value = jnp.sum(jnp.where(lane == 8 * slot + sub, row, 0.0), axis=1, keepdims=True)
        found.append((half, node, lane == where, value))
    for half, node, mask, value in found:
        part = jnp.where(mask, value, 0.0)
        extra[half][node] = extra[half][node] + part if node in extra[half] else part
    return extra


def permuted(x, table):
    high = x.astype(jnp.bfloat16)
    rest = x - high.astype(jnp.float32)
    middle = rest.astype(jnp.bfloat16)
    low = (rest - middle.astype(jnp.float32)).astype(jnp.bfloat16)
    size = x.shape[0]
    parts = jnp.concatenate([high, middle, low], axis=0)
    y = jnp.dot(parts, table, preferred_element_type=jnp.float32)
    return y[:size] + y[size : 2 * size] + y[2 * size :]


def halves(x):
    return [x[:, :HALF], x[:, HALF:]]


def kernel(
    n_elem,
    n_lev,
    trc,
    thickness,
    winds,
    metric,
    beside,
    result,
    last_rows,
    near,
    raw,
    small_raw,
    small,
    tables,
    state,
    rate,
    coef,
    mixed_coef,
    mass,
    shared,
    scale,
    line_send,
    line_recv,
    corner_send,
    corner_recv,
    thick,
    last,
    inverse,
    column,
    columns,
    ratio,
    ratio_recv,
    last_ratio,
    last_recv,
    edge_send,
    edge_recv,
    delta,
    in_sem,
    small_sem,
    line_ssem,
    line_rsem,
    column_ssem,
    column_rsem,
    ratio_ssem,
    ratio_rsem,
    edge_ssem,
    edge_rsem,
):
    place, level = lax.axis_index("elem"), lax.axis_index("lev")
    width = 2 * HALF
    offsets = (
        1,
        -1,
        ACROSS,
        -ACROSS,
        ACROSS + 1,
        ACROSS - 1,
        1 - ACROSS,
        -1 - ACROSS,
    )
    targets = [{"elem": lax.rem(place + offset + n_elem, n_elem)} for offset in offsets]
    peers = [{"lev": lax.rem(level + k, n_lev)} for k in range(1, n_lev)]

    barrier = pltpu.get_barrier_semaphore()
    for target in targets[2:] + peers + targets[:2]:
        pl.semaphore_signal(barrier, inc=1, device_id=target, device_id_type=MESH)

    near_copy = pltpu.make_async_copy(beside, near, small_sem.at[0])
    near_copy.start()
    pieces = [
        (trc.at[pl.ds(768, 32)], 0, 32),
        (thickness, 32, 32),
        (winds, 64, 64),
        (metric, 128, 16),
    ]
    small_copies = []
    for k, (source, start, size) in enumerate(pieces):
        copy = pltpu.make_async_copy(
            source, small_raw.at[pl.ds(start, size)], small_sem.at[k + 1]
        )
        copy.start()
        small_copies.append(copy)
    in_copies = []
    for half in range(2):
        copy = pltpu.make_async_copy(
            trc.at[pl.ds(0, 768), pl.ds(HALF * half, HALF)], raw.at[half], in_sem.at[half]
        )
        copy.start()
        in_copies.append(copy)

    line_send[...] = jnp.zeros_like(line_send)
    edge_send[...] = jnp.zeros_like(edge_send)

    @pl.when(level == 0)
    def _():
        edge_recv[1] = jnp.zeros_like(edge_recv[1])
        ratio_recv[:, 1] = jnp.zeros_like(ratio_recv[:, 1])
        last_recv[1] = jnp.zeros_like(last_recv[1])

    @pl.when(level == n_lev - 1)
    def _():
        edge_recv[0] = jnp.zeros_like(edge_recv[0])
        ratio_recv[:, 0] = jnp.zeros_like(ratio_recv[:, 0])
        last_recv[0] = jnp.zeros_like(last_recv[0])

    near_copy.wait()
    dot = functools.partial(jnp.dot, preferred_element_type=jnp.float32)
    element = lax.broadcasted_iota(jnp.int32, (width, width), 0)
    own = near[...] - place * width
    spots = []
    for side in (1, 3):
        step = jnp.where(own[side : side + 1, :] == element, 1.0, 0.0).astype(jnp.bfloat16)
        count = dot(jnp.ones((8, width), jnp.bfloat16), step)
        for doubling in range(4):
            count = count + dot(count.astype(jnp.bfloat16), step)
            if doubling < 3:
                step = dot(step, step).astype(jnp.bfloat16)
        spots.append(count)
    spot = (spots[0] + PSIDE * spots[1]).astype(jnp.int32)[0:1, :]
    to_drawn = jnp.where(spot == element, 1.0, 0.0)
    tables[1] = to_drawn.astype(jnp.bfloat16)
    tables[0] = jnp.transpose(to_drawn).astype(jnp.bfloat16)

    for copy in small_copies:
        copy.wait()
    small[...] = permuted(small_raw[...], tables[0])
    node = lax.broadcasted_iota(jnp.int32, (NODES, width), 0)
    point_i, point_j = node % 4, node // 4
    ends, inside = float(WEIGHTS[0]), float(WEIGHTS[1])
    weight_i = jnp.where((point_i == 0) | (point_i == 3), ends, inside)
    weight_j = jnp.where((point_j == 0) | (point_j == 3), ends, inside)
    area = small[pl.ds(128, NODES), :]
    mass[...] = weight_i * weight_j * area
    for l in range(2):
        coef[0, l] = -(weight_j * area) * small[pl.ds(64 + 16 * l, NODES), :]
        coef[1, l] = -(weight_i * area) * small[pl.ds(96 + 16 * l, NODES), :]

    for copy in in_copies:
        copy.wait()

    def take_in(q, carry):
        t, l = (q - 1) // 2, (q - 1) % 2
        x = jnp.concatenate(
            [
                jnp.concatenate(
                    [
                        raw[half, pl.ds(256 * t + 16 * l + n, 8, stride=32), :]
                        for n in range(NODES)
                    ],
                    axis=0,
                )
                for half in range(2)
            ],
            axis=1,
        )
        y = permuted(x, tables[0])
        for n in range(NODES):
            layer = small[pl.ds(32 + 16 * l + n, 1), :]
            state[q, n] = y[8 * n : 8 * n + 8] * layer
        return carry

    lax.fori_loop(1, 7, take_in, 0, unroll=True)
    wide_sub = lax.broadcasted_iota(jnp.int32, (8, width), 0)
    for n in range(NODES):
        tile = jnp.zeros((8, width), jnp.float32)
        for l in range(2):
            layer = small[pl.ds(32 + 16 * l + n, 1), :]
            tile = jnp.where(wide_sub == 2 * l, small[pl.ds(16 * l + n, 1), :] * layer, tile)
            tile = jnp.where(wide_sub == 2 * l + 1, layer, tile)
        state[0, n] = tile
        for k in range(2):
            mixed_coef[k, n] = jnp.where(
                wide_sub < 2, coef[k, 0, pl.ds(n, 1), :], coef[k, 1, pl.ds(n, 1), :]
            )

    def level_coef(l, half):
        at = pl.ds(HALF * half, HALF)
        return [[coef[k, l, pl.ds(n, 1), at] for n in range(NODES)] for k in range(2)]

    def both_coef(half):
        at = pl.ds(HALF * half, HALF)
        return [[mixed_coef[k, n, :, at] for n in range(NODES)] for k in range(2)]

    def load(ref, q):
        return [
            [ref[q, n, :, pl.ds(HALF * half, HALF)] for n in range(NODES)] for half in range(2)
        ]

    def save(ref, q, v):
        for half in range(2):
            for n in range(NODES):
                ref[q, n, :, pl.ds(HALF * half, HALF)] = v[half][n]

    def scaled(half):
        at = pl.ds(HALF * half, HALF)
        return [scale[pl.ds(n, 1), at] for n in range(NODES)]

    def rates_of(q, h, mixed):
        v = []
        for half in range(2):
            a, b = both_coef(half) if mixed else level_coef((q - 1) % 2, half)
            rates = weighted_tendency(h[half], a, b)
            if mixed:
                at = pl.ds(HALF * half, HALF)
                rates = [
                    jnp.where(sublanes() == 4, mass[pl.ds(n, 1), at], rates[n])
                    for n in range(NODES)
                ]
            v.append(rates)
        return assembled_in_patch(v)

    def pack(v, q, stage, group, corners):
        slot = q - slot_base[group]
        for side, half, value in lines_of(v, slot):
            line_send[stage, group, side, half] += value
        return corners_of(v, slot, corners)

    def exchange(stage, group, corners):
        for k in range(4):
            corner_send[stage, group, k] = jnp.sum(corners[k], axis=0, keepdims=True)
        copies = []
        for side in (2, 3, 4, 5, 6, 7, 0, 1):
            if side < 4:
                source = line_send.at[stage, group, side]
                landing = line_recv.at[stage, group, OPPOSITE[side]]
            else:
                source = corner_send.at[stage, group, side - 4]
                landing = corner_recv.at[stage, group, OPPOSITE[side] - 4]
            copy = pltpu.make_async_remote_copy(
                src_ref=source,
                dst_ref=landing,
                send_sem=line_ssem.at[stage, group, side],
                recv_sem=line_rsem.at[stage, group, OPPOSITE[side]],
                device_id=targets[side],
                device_id_type=MESH,
            )
            copy.start()
            copies.append(copy)
        return copies

    def extra_of(q, stage, group):
        rows = [corner_recv[stage, group, k] for k in range(4)]
        return borders_of(q - slot_base[group], line_recv.at[stage, group], rows)

    no_corners = tuple(jnp.zeros((8, HALF), jnp.float32) for _ in range(4))
    tiles_of = ((1, 3), (3, 7))
    slot_base = (0, 3)

    def first(q, corners, group, mixed=False):
        v = rates_of(q, load(state, q), mixed)
        save(rate, q, v)
        return pack(v, q, 0, group, corners)

    first_sends, second_sends = [], []
    for group in range(2):
        corners = first(0, no_corners, 0, True) if group == 0 else no_corners
        corners = lax.fori_loop(
            *tiles_of[group], lambda q, c: first(q, c, group), corners, unroll=True
        )
        if group == 0:
            pl.semaphore_wait(barrier, len(targets) + len(peers))
        first_sends.append(exchange(0, group, corners))

    below = {"lev": lax.rem(level + n_lev - 1, n_lev)}
    above = {"lev": lax.rem(level + 1, n_lev)}
    has_below, has_above = level > 0, level < n_lev - 1

    def ratio_copy(t, l):
        if t == 3:
            source, landing = last_ratio.at[l], last_recv.at[l]
        elif t < 2:
            source, landing = ratio.at[t, l], ratio_recv.at[t, l]
        else:
            nodes = pl.ds(0, 4) if t == 2 else pl.ds(4, NODES - 4)
            source, landing = ratio.at[2, l, nodes], ratio_recv.at[2, l, nodes]
        return pltpu.make_async_remote_copy(
            src_ref=source,
            dst_ref=landing,
            send_sem=ratio_ssem.at[t, l],
            recv_sem=ratio_rsem.at[t, l],
            device_id=below if l == 0 else above,
            device_id_type=MESH,
        )

    def send_ratios(t):
        pl.when(has_below)(lambda: ratio_copy(t, 0).start())
        pl.when(has_above)(lambda: ratio_copy(t, 1).start())

    def edge_copy(l):
        return pltpu.make_async_remote_copy(
            src_ref=edge_send.at[l],
            dst_ref=edge_recv.at[l],
            send_sem=edge_ssem.at[l],
            recv_sem=edge_rsem.at[l],
            device_id=below if l == 0 else above,
            device_id_type=MESH,
        )

    def second(q, corners, group, mixed=False):
        v = load(rate, q)
        extra = extra_of(q, 0, group)
        for half in range(2):
            for n in extra[half]:
                v[half][n] = v[half][n] + extra[half][n]
        if mixed:
            for half in range(2):
                for n in range(NODES):
                    shared[pl.ds(n, 1), pl.ds(HALF * half, HALF)] = v[half][n][4:5, :]
            scale[...] = (0.5 * time_step) / shared[...]
        h = load(state, q)
        for half in range(2):
            c = scaled(half)
            for n in range(NODES):
                step = c[n] * v[half][n]
                mean = h[half][n] + step
                state[q, n, :, pl.ds(HALF * half, HALF)] = mean
                h[half][n] = mean + step
        v = rates_of(q, h, mixed)
        h = load(state, q)
        for half in range(2):
            c = scaled(half)
            for n in range(NODES):
                h[half][n] = h[half][n] + c[n] * v[half][n]
        save(state, q, h)
        if mixed:
            split_mixed(h)
            for l in range(2):
                last_ratio[l] = last[l] * inverse[l]
        else:
            t, l = (q - 1) // 2, (q - 1) % 2
            for half in range(2):
                at = pl.ds(HALF * half, HALF)
                for n in range(NODES):
                    ratio[t, l, n, :, at] = h[half][n] * inverse[l, pl.ds(n, 1), at]
        return pack(v, q, 1, group, corners)

    def split_mixed(h):
        for half in range(2):
            at = pl.ds(HALF * half, HALF)
            for n in range(NODES):
                for l in range(2):
                    last[l, pl.ds(n, 1), at] = h[half][n][2 * l : 2 * l + 1, :]
                    thick[l, pl.ds(n, 1), at] = h[half][n][2 * l + 1 : 2 * l + 2, :]
        for l in range(2):
            inverse[l] = 1.0 / thick[l]

    for group in range(2):
        for copy in first_sends[group]:
            copy.wait_recv()
        corners = second(0, no_corners, 0, True) if group == 0 else no_corners
        if group == 0:
            send_ratios(3)
        for t in ((0,), (1, 2))[group]:
            corners = lax.fori_loop(
                2 * t + 1, 2 * t + 3, lambda q, c: second(q, c, group), corners, unroll=True
            )
            if t < 2:
                send_ratios(t)
        second_sends.append(exchange(1, group, corners))

    def finish(q, group, mixed=False):
        extra = extra_of(q, 1, group)
        h = load(state, q)
        for half in range(2):
            c = scaled(half)
            at = pl.ds(HALF * half, HALF)
            for n in extra[half]:
                h[half][n] = h[half][n] + c[n] * extra[half][n]
                state[q, n, :, at] = h[half][n]
        return h

    def send_outline(q, h, l, slot, factor):
        r = [[h[half][n] * factor(half, n) for n in range(NODES)] for half in range(2)]
        for side, half, value in lines_of(r, slot):
            edge_send[l, side, half] += value

    def finish_levels(q, carry, group):
        t, l = (q - 1) // 2, (q - 1) % 2
        h = finish(q, group)
        send_outline(
            q, h, l, t, lambda half, n: inverse[l, pl.ds(n, 1), pl.ds(HALF * half, HALF)]
        )
        return carry

    column_copies = []
    for group in range(2):
        for copy in second_sends[group]:
            copy.wait_recv()
        if group == 0:
            h = finish(0, 0)
            split_mixed(h)
            column[...] = thick[0] + thick[1]
            for k, peer in enumerate(peers):
                copy = pltpu.make_async_remote_copy(
                    src_ref=column,
                    dst_ref=columns.at[k],
                    send_sem=column_ssem.at[k],
                    recv_sem=column_rsem.at[k],
                    device_id=peer,
                    device_id_type=MESH,
                )
                copy.start()
                column_copies.append(copy)
            send_ratios(2)
            for l in range(2):
                send_outline(
                    0,
                    h,
                    l,
                    3,
                    lambda half, n: inverse[l, pl.ds(n, 1), pl.ds(HALF * half, HALF)],
                )
        lax.fori_loop(
            *tiles_of[group], lambda q, c: finish_levels(q, c, group), 0, unroll=True
        )
    pl.when(has_below)(lambda: edge_copy(0).start())
    pl.when(has_above)(lambda: edge_copy(1).start())
    send_ratios(4)

    def wait_ratios(t):
        pl.when(has_above)(lambda: ratio_copy(t, 0).wait_recv())
        pl.when(has_below)(lambda: ratio_copy(t, 1).wait_recv())

    def merge_outlines(t):
        wait_ratios(t)
        if t == 2:
            wait_ratios(4)
        for l in range(2):
            found = {}
            for half, n, mask, value in placed_lines(t, edge_recv.at[l]):
                at = pl.ds(HALF * half, HALF)
                before = found.get((half, n))
                if before is None:
                    before = ratio_recv[t, l, n, :, at]
                found[half, n] = jnp.where(mask, value, before)
            for (half, n), value in found.items():
                ratio_recv[t, l, n, :, pl.ds(HALF * half, HALF)] = value

    pl.when(has_above)(lambda: edge_copy(0).wait_recv())
    pl.when(has_below)(lambda: edge_copy(1).wait_recv())
    wait_ratios(3)
    for l in range(2):
        for half, n, mask, value in placed_lines(3, edge_recv.at[l]):
            row, at = pl.ds(n, 1), pl.ds(HALF * half, HALF)
            last_recv[l, row, at] = jnp.where(
                mask[0:1], value[2 * l : 2 * l + 1], last_recv[l, row, at]
            )
    merge_outlines(0)
    merge_outlines(1)

    for copy in column_copies:
        copy.wait_recv()
    own_column = column[...]
    others = jnp.zeros_like(own_column)
    under = jnp.zeros_like(own_column)
    for k in range(1, n_lev):
        part = columns[k - 1]
        others = others + part
        under = under + jnp.where(k <= level, part, 0.0)
    surface_rows = own_column + others
    levels = 2 * n_lev

    def as_float(k):
        return k.astype(jnp.float32)

    for k in range(3):
        edge_level = as_float(2 * level + k)
        fraction = (edge_level + edge_level * (edge_level - 1.0) * (1.0 / (levels - 1))) * (
            0.5 / levels
        )
        if k > 0:
            under = under + thick[k - 1]
        delta[k] = under - surface_rows * fraction
    for l in range(2):
        share = (1.0 + 2.0 * as_float(2 * level + l) * (1.0 / (levels - 1))) * (0.5 / levels)
        delta[3 + l] = 1.0 / (surface_rows * share)

    def remapped(d, carried, own_ratio, ratio_above, ratio_below):
        low = d[0] * jnp.where(d[0] > 0.0, ratio_below, own_ratio[0])
        middle = d[1] * jnp.where(d[1] > 0.0, own_ratio[0], own_ratio[1])
        high = d[2] * jnp.where(d[2] > 0.0, own_ratio[1], ratio_above)
        return (carried[0] + low - middle) * d[3], (carried[1] + middle - high) * d[4]

    d = [delta[k] for k in range(5)]
    first, second = remapped(
        d,
        [last[0], last[1]],
        [last[0] * inverse[0], last[1] * inverse[1]],
        last_recv[0],
        last_recv[1],
    )
    rows = permuted(jnp.concatenate([first, second, surface_rows], axis=0), tables[1])
    last_rows[...] = rows
    for t in range(3):
        if t == 2:
            merge_outlines(2)
        pairs = []
        for n in range(NODES):
            parts = []
            for half in range(2):
                at = pl.ds(HALF * half, HALF)
                d = [delta[k, pl.ds(n, 1), at] for k in range(5)]
                carried = [state[2 * t + 1 + l, n, :, at] for l in range(2)]
                own_ratio = [carried[l] * inverse[l, pl.ds(n, 1), at] for l in range(2)]
                parts.append(
                    remapped(d, carried, own_ratio, ratio_recv[t, 0, n, :, at], ratio_recv[t, 1, n, :, at])
                )
            pairs.append(
                [jnp.concatenate([parts[0][l], parts[1][l]], axis=1) for l in range(2)]
            )
        tiles = permuted(
            jnp.concatenate([pair[l] for l in range(2) for pair in pairs], axis=0), tables[1]
        )
        for k in range(2 * NODES):
            for half in range(2):
                result[half, pl.ds(256 * t + k, 8, stride=32), :] = tiles[
                    8 * k : 8 * k + 8, HALF * half : HALF * half + HALF
                ]
    for copy in sum(first_sends + second_sends, column_copies):
        copy.wait_send()
    for t in range(5):
        pl.when(has_below)(lambda t=t: ratio_copy(t, 0).wait_send())
        pl.when(has_above)(lambda t=t: ratio_copy(t, 1).wait_send())
    pl.when(has_below)(lambda: edge_copy(0).wait_send())
    pl.when(has_above)(lambda: edge_copy(1).wait_send())


def store(result, last_rows, out, surf, sem):
    copies = [
        pltpu.make_async_copy(last_rows.at[pl.ds(32, 16)], surf, sem.at[0]),
        pltpu.make_async_copy(last_rows.at[pl.ds(0, 32)], out.at[pl.ds(768, 32)], sem.at[1]),
    ]
    for half in range(2):
        at = pl.ds(HALF * half, HALF)
        for k in range(2):
            rows = pl.ds(384 * k, 384)
            copies.append(
                pltpu.make_async_copy(
                    result.at[half, rows], out.at[rows, at], sem.at[2 + 2 * half + k]
                )
            )
    for copy in copies:
        copy.start()
    for copy in copies:
        copy.wait()


def per_device(n_elem, n_lev, tracers, layer_mass, winds, metric, neighbours):
    width = metric.shape[-1]
    f32 = jnp.float32
    tile = (NODES, 8, width)
    dma = pltpu.SemaphoreType.DMA
    scratch = [
        pltpu.VMEM((8, width), jnp.int32),
        pltpu.VMEM((2, 768, HALF), f32),
        pltpu.VMEM((144, width), f32),
        pltpu.VMEM((144, width), f32),
        pltpu.VMEM((2, width, width), jnp.bfloat16),
        pltpu.VMEM((7,) + tile, f32),
        pltpu.VMEM((7,) + tile, f32),
        pltpu.VMEM((2, 2, NODES, width), f32),
        pltpu.VMEM((2,) + tile, f32),
        pltpu.VMEM((NODES, width), f32),
        pltpu.VMEM((NODES, width), f32),
        pltpu.VMEM((NODES, width), f32),
        pltpu.VMEM((2, 2, 4, 2, 8, HALF), f32),
        pltpu.VMEM((2, 2, 4, 2, 8, HALF), f32),
        pltpu.VMEM((2, 2, 4, 1, HALF), f32),
        pltpu.VMEM((2, 2, 4, 1, HALF), f32),
        pltpu.VMEM((2, NODES, width), f32),
        pltpu.VMEM((2, NODES, width), f32),
        pltpu.VMEM((2, NODES, width), f32),
        pltpu.VMEM((NODES, width), f32),
        pltpu.VMEM((n_lev - 1, NODES, width), f32),
        pltpu.VMEM((3, 2) + tile, f32),
        pltpu.VMEM((3, 2) + tile, f32),
        pltpu.VMEM((2, NODES, width), f32),
        pltpu.VMEM((2, NODES, width), f32),
        pltpu.VMEM((2, 4, 2, 8, HALF), f32),
        pltpu.VMEM((2, 4, 2, 8, HALF), f32),
        pltpu.VMEM((5, NODES, width), f32),
        dma((2,)),
        dma((5,)),
        dma((2, 2, 8)),
        dma((2, 2, 8)),
        dma((n_lev - 1,)),
        dma((n_lev - 1,)),
        dma((5, 2)),
        dma((5, 2)),
        dma((2,)),
        dma((2,)),
    ]
    result, last_rows = pl.pallas_call(
        functools.partial(kernel, n_elem, n_lev),
        out_shape=(
            jax.ShapeDtypeStruct((2, 768, HALF), f32),
            jax.ShapeDtypeStruct((3 * NODES, width), f32),
        ),
        in_specs=[pl.BlockSpec(memory_space=pltpu.HBM)] * 5,
        out_specs=(pl.BlockSpec(memory_space=pltpu.VMEM),) * 2,
        scratch_shapes=scratch,
        compiler_params=pltpu.CompilerParams(
            collective_id=0, has_side_effects=True, vmem_limit_bytes=24 * 1024 * 1024
        ),
        name="transport",
    )(
        *[
            pltpu.with_memory_space_constraint(x, pltpu.HBM)
            for x in (
                tracers.reshape(-1, width),
                layer_mass.reshape(-1, width),
                winds.reshape(-1, width),
                metric,
                jnp.transpose(neighbours),
            )
        ]
    )
    out, surface = pl.pallas_call(
        store,
        out_shape=(
            jax.ShapeDtypeStruct((800, width), f32),
            jax.ShapeDtypeStruct((NODES, width), f32),
        ),
        in_specs=[pl.BlockSpec(memory_space=pltpu.VMEM)] * 2,
        out_specs=(pl.BlockSpec(memory_space=pltpu.HBM),) * 2,
        scratch_shapes=[dma((6,))],
        compiler_params=pltpu.CompilerParams(vmem_limit_bytes=24 * 1024 * 1024),
        name="store",
    )(result, last_rows)
    return out.reshape(tracers.shape), surface


def solution(mesh):
    placed = (
        P(None, "lev", None, ("members", "elem")),
        P("lev", None, ("members", "elem")),
        P(None, "lev", None, ("members", "elem")),
        P(None, "elem"),
        P("elem", None),
    )
    return jax.shard_map(
        functools.partial(per_device, mesh.shape["elem"], mesh.shape["lev"]),
        mesh=mesh,
        in_specs=placed,
        out_specs=(P(None, "lev", None, ("members", "elem")), P(None, ("members", "elem"))),
        check_vma=False,
    )
```

```python
import functools
import math

import jax
import jax.numpy as jnp
import numpy as np
from jax import lax
from jax.experimental import pallas as pl
from jax.experimental.pallas import tpu as pltpu
from jax.sharding import PartitionSpec as P

MESH = pl.DeviceIdType.MESH
PSIDE = 16
ACROSS = 8
NODES = 16
HALF = 128
time_step = 0.035

OPPOSITE = (1, 0, 3, 2, 7, 6, 5, 4)
CORNERS = ((15, 1, 127), (12, 1, 112), (3, 0, 15), (0, 0, 0))


def lagrange_scale(points, which):
    product = 1.0
    for other in range(4):
        if other != which:
            product = product * (points[which] - points[other])
    return product


def node_tables():
    points = np.array([-1.0, -1.0 / math.sqrt(5.0), 1.0 / math.sqrt(5.0), 1.0])
    weights = np.array([1.0, 5.0, 5.0, 1.0]) / 6.0
    derivative = np.zeros((4, 4))
    for target in range(4):
        for source in range(4):
            if target == source:
                derivative[target, source] = sum(
                    1.0 / (points[target] - points[other]) for other in range(4) if other != target
                )
            else:
                derivative[target, source] = lagrange_scale(points, target) / (
                    lagrange_scale(points, source) * (points[target] - points[source])
                )
    return weights, derivative


WEIGHTS, DERIVATIVE = node_tables()
STIFF = WEIGHTS[:, None] * DERIVATIVE


def weighted_difference(f):
    total, gap = f[0] + f[3], f[3] - f[0]
    inner, inner_gap = f[1] + f[2], f[2] - f[1]
    result = [None] * 4
    for i in range(2):
        q = 0.5 * STIFF[i]
        odd = float(q[3] - q[0]) * gap + float(q[2] - q[1]) * inner_gap
        even = float(q[0] + q[3]) * total + float(q[1] + q[2]) * inner
        result[i] = odd + even
        result[3 - i] = odd - even
    return result


def weighted_tendency(h, a, b):
    f = [a[n] * h[n] for n in range(NODES)]
    g = [b[n] * h[n] for n in range(NODES)]
    rows = [weighted_difference(f[4 * j : 4 * j + 4]) for j in range(4)]
    columns = [weighted_difference(g[i::4]) for i in range(4)]
    return [rows[n // 4][n % 4] + columns[n % 4][n // 4] for n in range(NODES)]


def lanes():
    return lax.broadcasted_iota(jnp.int32, (8, HALF), 1)


def sublanes():
    return lax.broadcasted_iota(jnp.int32, (8, HALF), 0)


def roll(x, shift):
    return pltpu.roll(x, (shift + 2 * HALF) % HALF, 1)


def assembled_in_patch(v):
    lane = lanes()
    column = lane % PSIDE
    for half in range(2):
        for j in range(4):
            left, right = v[half][4 * j], v[half][4 * j + 3]
            v[half][4 * j + 3] = right + jnp.where(column < PSIDE - 1, roll(left, -1), 0.0)
            v[half][4 * j] = left + jnp.where(column > 0, roll(right, 1), 0.0)
    edge = HALF - PSIDE
    for i in range(4):
        low = [v[0][i], v[1][i]]
        high = [v[0][12 + i], v[1][12 + i]]
        down = [roll(low[0], -PSIDE), roll(low[1], -PSIDE)]
        up = [roll(high[0], PSIDE), roll(high[1], PSIDE)]
        v[0][12 + i] = high[0] + jnp.where(lane < edge, down[0], down[1])
        v[1][12 + i] = high[1] + jnp.where(lane < edge, down[1], 0.0)
        v[0][i] = low[0] + jnp.where(lane >= PSIDE, up[0], 0.0)
        v[1][i] = low[1] + jnp.where(lane >= PSIDE, up[1], up[0])
    return v


def lines_of(v, slot):
    lane = lanes()
    column, block = lane % PSIDE, lane // PSIDE
    found = []
    for half in range(2):
        east = west = 0.0
        for j in range(4):
            at = 4 * slot + j
            east = east + jnp.where(column == at, roll(v[half][4 * j + 3], at - (PSIDE - 1)), 0.0)
            west = west + jnp.where(column == at, roll(v[half][4 * j], at), 0.0)
        found += [(0, half, east), (1, half, west)]
    north = south = 0.0
    for i in range(4):
        at = 4 * (slot % 2) + i
        north = north + jnp.where(
            block == at, roll(v[1][12 + i], PSIDE * at - (HALF - PSIDE)), 0.0
        )
        south = south + jnp.where(block == at, roll(v[0][i], PSIDE * at), 0.0)
    return found + [(2, slot // 2, north), (3, slot // 2, south)]


def corners_of(v, slot, corners):
    lane, sub = lanes(), sublanes()
    result = []
    for k, (node, half, where) in enumerate(CORNERS):
        value = jnp.broadcast_to(v[half][node][:, where : where + 1], (8, HALF))
        result.append(corners[k] + jnp.where(lane == 8 * slot + sub, value, 0.0))
    return tuple(result)


def placed_lines(slot, lines):
    lane = lanes()
    column = lane % PSIDE
    found = []
    for half in range(2):
        east, west = lines[0, half], lines[1, half]
        for j in range(4):
            at = 4 * slot + j
            found.append((half, 4 * j + 3, column == PSIDE - 1, roll(east, PSIDE - 1 - at)))
            found.append((half, 4 * j, column == 0, roll(west, -at)))
    north, south = lines[2, slot // 2], lines[3, slot // 2]
    for i in range(4):
        at = 4 * (slot % 2) + i
        found.append(
            (1, 12 + i, lane >= HALF - PSIDE, roll(north, HALF - PSIDE - PSIDE * at))
        )
        found.append((0, i, lane < PSIDE, roll(south, -PSIDE * at)))
    return found


def borders_of(slot, lines, corners):
    lane, sub = lanes(), sublanes()
    extra = [{}, {}]
    found = placed_lines(slot, lines)
    for k, (node, half, where) in enumerate(CORNERS):
        row = jnp.broadcast_to(corners[k], (8, HALF))
        value = jnp.sum(jnp.where(lane == 8 * slot + sub, row, 0.0), axis=1, keepdims=True)
        found.append((half, node, lane == where, value))
    for half, node, mask, value in found:
        part = jnp.where(mask, value, 0.0)
        extra[half][node] = extra[half][node] + part if node in extra[half] else part
    return extra


def permuted(x, table):
    high = x.astype(jnp.bfloat16)
    rest = x - high.astype(jnp.float32)
    middle = rest.astype(jnp.bfloat16)
    low = (rest - middle.astype(jnp.float32)).astype(jnp.bfloat16)
    size = x.shape[0]
    parts = jnp.concatenate([high, middle, low], axis=0)
    y = jnp.dot(parts, table, preferred_element_type=jnp.float32)
    return y[:size] + y[size : 2 * size] + y[2 * size :]


def halves(x):
    return [x[:, :HALF], x[:, HALF:]]


def kernel(
    n_elem,
    n_lev,
    trc,
    thickness,
    winds,
    metric,
    beside,
    result,
    last_rows,
    near,
    raw,
    small_raw,
    small,
    tables,
    state,
    rate,
    coef,
    mixed_coef,
    mass,
    shared,
    scale,
    line_send,
    line_recv,
    corner_send,
    corner_recv,
    thick,
    last,
    inverse,
    column,
    columns,
    ratio,
    ratio_recv,
    last_ratio,
    last_recv,
    edge_send,
    edge_recv,
    delta,
    in_sem,
    small_sem,
    line_ssem,
    line_rsem,
    column_ssem,
    column_rsem,
    ratio_ssem,
    ratio_rsem,
    edge_ssem,
    edge_rsem,
):
    place, level = lax.axis_index("elem"), lax.axis_index("lev")
    width = 2 * HALF
    offsets = (
        1,
        -1,
        ACROSS,
        -ACROSS,
        ACROSS + 1,
        ACROSS - 1,
        1 - ACROSS,
        -1 - ACROSS,
    )
    targets = [{"elem": lax.rem(place + offset + n_elem, n_elem)} for offset in offsets]
    peers = [{"lev": lax.rem(level + k, n_lev)} for k in range(1, n_lev)]

    barrier = pltpu.get_barrier_semaphore()
    for target in targets[2:] + peers + targets[:2]:
        pl.semaphore_signal(barrier, inc=1, device_id=target, device_id_type=MESH)

    near_copy = pltpu.make_async_copy(beside, near, small_sem.at[0])
    near_copy.start()
    pieces = [
        (trc.at[pl.ds(768, 32)], 0, 32),
        (thickness, 32, 32),
        (winds, 64, 64),
        (metric, 128, 16),
    ]
    small_copies = []
    for k, (source, start, size) in enumerate(pieces):
        copy = pltpu.make_async_copy(
            source, small_raw.at[pl.ds(start, size)], small_sem.at[k + 1]
        )
        copy.start()
        small_copies.append(copy)
    in_copies = []
    for half in range(2):
        copy = pltpu.make_async_copy(
            trc.at[pl.ds(0, 768), pl.ds(HALF * half, HALF)], raw.at[half], in_sem.at[half]
        )
        copy.start()
        in_copies.append(copy)

    line_send[...] = jnp.zeros_like(line_send)
    edge_send[...] = jnp.zeros_like(edge_send)

    @pl.when(level == 0)
    def _():
        edge_recv[1] = jnp.zeros_like(edge_recv[1])
        ratio_recv[:, 1] = jnp.zeros_like(ratio_recv[:, 1])
        last_recv[1] = jnp.zeros_like(last_recv[1])

    @pl.when(level == n_lev - 1)
    def _():
        edge_recv[0] = jnp.zeros_like(edge_recv[0])
        ratio_recv[:, 0] = jnp.zeros_like(ratio_recv[:, 0])
        last_recv[0] = jnp.zeros_like(last_recv[0])

    near_copy.wait()
    dot = functools.partial(jnp.dot, preferred_element_type=jnp.float32)
    element = lax.broadcasted_iota(jnp.int32, (width, width), 0)
    own = near[...] - place * width
    spots = []
    for side in (1, 3):
        step = jnp.where(own[side : side + 1, :] == element, 1.0, 0.0).astype(jnp.bfloat16)
        count = dot(jnp.ones((8, width), jnp.bfloat16), step)
        for doubling in range(4):
            count = count + dot(count.astype(jnp.bfloat16), step)
            if doubling < 3:
                step = dot(step, step).astype(jnp.bfloat16)
        spots.append(count)
    spot = (spots[0] + PSIDE * spots[1]).astype(jnp.int32)[0:1, :]
    to_drawn = jnp.where(spot == element, 1.0, 0.0)
    tables[1] = to_drawn.astype(jnp.bfloat16)
    tables[0] = jnp.transpose(to_drawn).astype(jnp.bfloat16)

    for copy in small_copies:
        copy.wait()
    small[...] = permuted(small_raw[...], tables[0])
    node = lax.broadcasted_iota(jnp.int32, (NODES, width), 0)
    point_i, point_j = node % 4, node // 4
    ends, inside = float(WEIGHTS[0]), float(WEIGHTS[1])
    weight_i = jnp.where((point_i == 0) | (point_i == 3), ends, inside)
    weight_j = jnp.where((point_j == 0) | (point_j == 3), ends, inside)
    area = small[pl.ds(128, NODES), :]
    mass[...] = weight_i * weight_j * area
    for l in range(2):
        coef[0, l] = -(weight_j * area) * small[pl.ds(64 + 16 * l, NODES), :]
        coef[1, l] = -(weight_i * area) * small[pl.ds(96 + 16 * l, NODES), :]

    for copy in in_copies:
        copy.wait()

    def take_in(q, carry):
        t, l = (q - 1) // 2, (q - 1) % 2
        x = jnp.concatenate(
            [
                jnp.concatenate(
                    [
                        raw[half, pl.ds(256 * t + 16 * l + n, 8, stride=32), :]
                        for n in range(NODES)
                    ],
                    axis=0,
                )
                for half in range(2)
            ],
            axis=1,
        )
        y = permuted(x, tables[0])
        for n in range(NODES):
            layer = small[pl.ds(32 + 16 * l + n, 1), :]
            state[q, n] = y[8 * n : 8 * n + 8] * layer
        return carry

    lax.fori_loop(1, 7, take_in, 0, unroll=True)
    wide_sub = lax.broadcasted_iota(jnp.int32, (8, width), 0)
    for n in range(NODES):
        tile = jnp.zeros((8, width), jnp.float32)
        for l in range(2):
            layer = small[pl.ds(32 + 16 * l + n, 1), :]
            tile = jnp.where(wide_sub == 2 * l, small[pl.ds(16 * l + n, 1), :] * layer, tile)
            tile = jnp.where(wide_sub == 2 * l + 1, layer, tile)
        state[0, n] = tile
        for k in range(2):
            mixed_coef[k, n] = jnp.where(
                wide_sub < 2, coef[k, 0, pl.ds(n, 1), :], coef[k, 1, pl.ds(n, 1), :]
            )

    def level_coef(l, half):
        at = pl.ds(HALF * half, HALF)
        return [[coef[k, l, pl.ds(n, 1), at] for n in range(NODES)] for k in range(2)]

    def both_coef(half):
        at = pl.ds(HALF * half, HALF)
        return [[mixed_coef[k, n, :, at] for n in range(NODES)] for k in range(2)]

    def load(ref, q):
        return [
            [ref[q, n, :, pl.ds(HALF * half, HALF)] for n in range(NODES)] for half in range(2)
        ]

    def save(ref, q, v):
        for half in range(2):
            for n in range(NODES):
                ref[q, n, :, pl.ds(HALF * half, HALF)] = v[half][n]

    def scaled(half):
        at = pl.ds(HALF * half, HALF)
        return [scale[pl.ds(n, 1), at] for n in range(NODES)]

    def rates_of(q, h, mixed):
        v = []
        for half in range(2):
            a, b = both_coef(half) if mixed else level_coef((q - 1) % 2, half)
            rates = weighted_tendency(h[half], a, b)
            if mixed:
                at = pl.ds(HALF * half, HALF)
                rates = [
                    jnp.where(sublanes() == 4, mass[pl.ds(n, 1), at], rates[n])
                    for n in range(NODES)
                ]
            v.append(rates)
        return assembled_in_patch(v)

    def pack(v, q, stage, group, corners):
        slot = q - slot_base[group]
        for side, half, value in lines_of(v, slot):
            line_send[stage, group, side, half] += value
        return corners_of(v, slot, corners)

    def exchange(stage, group, corners):
        for k in range(4):
            corner_send[stage, group, k] = jnp.sum(corners[k], axis=0, keepdims=True)
        copies = []
        for side in (2, 3, 4, 5, 6, 7, 0, 1):
            if side < 4:
                source = line_send.at[stage, group, side]
                landing = line_recv.at[stage, group, OPPOSITE[side]]
            else:
                source = corner_send.at[stage, group, side - 4]
                landing = corner_recv.at[stage, group, OPPOSITE[side] - 4]
            copy = pltpu.make_async_remote_copy(
                src_ref=source,
                dst_ref=landing,
                send_sem=line_ssem.at[stage, group, side],
                recv_sem=line_rsem.at[stage, group, OPPOSITE[side]],
                device_id=targets[side],
                device_id_type=MESH,
            )
            copy.start()
            copies.append(copy)
        return copies

    def extra_of(q, stage, group):
        rows = [corner_recv[stage, group, k] for k in range(4)]
        return borders_of(q - slot_base[group], line_recv.at[stage, group], rows)

    no_corners = tuple(jnp.zeros((8, HALF), jnp.float32) for _ in range(4))
    tiles_of = ((1, 3), (3, 7))
    slot_base = (0, 3)

    def first(q, corners, group, mixed=False):
        v = rates_of(q, load(state, q), mixed)
        save(rate, q, v)
        return pack(v, q, 0, group, corners)

    first_sends, second_sends = [], []
    for group in range(2):
        corners = first(0, no_corners, 0, True) if group == 0 else no_corners
        corners = lax.fori_loop(
            *tiles_of[group], lambda q, c: first(q, c, group), corners, unroll=True
        )
        if group == 0:
            pl.semaphore_wait(barrier, len(targets) + len(peers))
        first_sends.append(exchange(0, group, corners))

    below = {"lev": lax.rem(level + n_lev - 1, n_lev)}
    above = {"lev": lax.rem(level + 1, n_lev)}
    has_below, has_above = level > 0, level < n_lev - 1

    def ratio_copy(t, l):
        if t == 3:
            source, landing = last_ratio.at[l], last_recv.at[l]
        elif t < 2:
            source, landing = ratio.at[t, l], ratio_recv.at[t, l]
        else:
            nodes = pl.ds(0, 4) if t == 2 else pl.ds(4, NODES - 4)
            source, landing = ratio.at[2, l, nodes], ratio_recv.at[2, l, nodes]
        return pltpu.make_async_remote_copy(
            src_ref=source,
            dst_ref=landing,
            send_sem=ratio_ssem.at[t, l],
            recv_sem=ratio_rsem.at[t, l],
            device_id=below if l == 0 else above,
            device_id_type=MESH,
        )

    def send_ratios(t):
        pl.when(has_below)(lambda: ratio_copy(t, 0).start())
        pl.when(has_above)(lambda: ratio_copy(t, 1).start())

    def edge_copy(l):
        return pltpu.make_async_remote_copy(
            src_ref=edge_send.at[l],
            dst_ref=edge_recv.at[l],
            send_sem=edge_ssem.at[l],
            recv_sem=edge_rsem.at[l],
            device_id=below if l == 0 else above,
            device_id_type=MESH,
        )

    def second(q, corners, group, mixed=False):
        v = load(rate, q)
        extra = extra_of(q, 0, group)
        for half in range(2):
            for n in extra[half]:
                v[half][n] = v[half][n] + extra[half][n]
        if mixed:
            for half in range(2):
                for n in range(NODES):
                    shared[pl.ds(n, 1), pl.ds(HALF * half, HALF)] = v[half][n][4:5, :]
            scale[...] = (0.5 * time_step) / shared[...]
        h = load(state, q)
        for half in range(2):
            c = scaled(half)
            for n in range(NODES):
                step = c[n] * v[half][n]
                mean = h[half][n] + step
                state[q, n, :, pl.ds(HALF * half, HALF)] = mean
                h[half][n] = mean + step
        v = rates_of(q, h, mixed)
        if group == 1:
            save(rate, q, v)
        else:
            settle(q, v, mixed)
        return pack(v, q, 1, group, corners)

    def settle(q, v, mixed=False):
        h = load(state, q)
        for half in range(2):
            c = scaled(half)
            for n in range(NODES):
                h[half][n] = h[half][n] + c[n] * v[half][n]
        save(state, q, h)
        if mixed:
            split_mixed(h)
            for l in range(2):
                last_ratio[l] = last[l] * inverse[l]
        else:
            t, l = (q - 1) // 2, (q - 1) % 2
            for half in range(2):
                at = pl.ds(HALF * half, HALF)
                for n in range(NODES):
                    ratio[t, l, n, :, at] = h[half][n] * inverse[l, pl.ds(n, 1), at]

    def split_mixed(h):
        for half in range(2):
            at = pl.ds(HALF * half, HALF)
            for n in range(NODES):
                for l in range(2):
                    last[l, pl.ds(n, 1), at] = h[half][n][2 * l : 2 * l + 1, :]
                    thick[l, pl.ds(n, 1), at] = h[half][n][2 * l + 1 : 2 * l + 2, :]
        for l in range(2):
            inverse[l] = 1.0 / thick[l]

    for group in range(2):
        for copy in first_sends[group]:
            copy.wait_recv()
        corners = second(0, no_corners, 0, True) if group == 0 else no_corners
        if group == 0:
            send_ratios(3)
        corners = lax.fori_loop(
            *tiles_of[group], lambda q, c: second(q, c, group), corners, unroll=True
        )
        if group == 0:
            send_ratios(0)
        second_sends.append(exchange(1, group, corners))

    def settle_step(q, carry):
        settle(q, load(rate, q))
        return carry

    lax.fori_loop(3, 5, settle_step, 0, unroll=True)
    send_ratios(1)
    lax.fori_loop(5, 7, settle_step, 0, unroll=True)

    def finish(q, group, mixed=False):
        extra = extra_of(q, 1, group)
        h = load(state, q)
        for half in range(2):
            c = scaled(half)
            at = pl.ds(HALF * half, HALF)
            for n in extra[half]:
                h[half][n] = h[half][n] + c[n] * extra[half][n]
                state[q, n, :, at] = h[half][n]
        return h

    def send_outline(q, h, l, slot, factor):
        r = [[h[half][n] * factor(half, n) for n in range(NODES)] for half in range(2)]
        for side, half, value in lines_of(r, slot):
            edge_send[l, side, half] += value

    def finish_levels(q, carry, group):
        t, l = (q - 1) // 2, (q - 1) % 2
        h = finish(q, group)
        send_outline(
            q, h, l, t, lambda half, n: inverse[l, pl.ds(n, 1), pl.ds(HALF * half, HALF)]
        )
        return carry

    column_copies = []
    for group in range(2):
        for copy in second_sends[group]:
            copy.wait_recv()
        if group == 0:
            h = finish(0, 0)
            split_mixed(h)
            column[...] = thick[0] + thick[1]
            for k, peer in enumerate(peers):
                copy = pltpu.make_async_remote_copy(
                    src_ref=column,
                    dst_ref=columns.at[k],
                    send_sem=column_ssem.at[k],
                    recv_sem=column_rsem.at[k],
                    device_id=peer,
                    device_id_type=MESH,
                )
                copy.start()
                column_copies.append(copy)
            send_ratios(2)
            for l in range(2):
                send_outline(
                    0,
                    h,
                    l,
                    3,
                    lambda half, n: inverse[l, pl.ds(n, 1), pl.ds(HALF * half, HALF)],
                )
        lax.fori_loop(
            *tiles_of[group], lambda q, c: finish_levels(q, c, group), 0, unroll=True
        )
    pl.when(has_below)(lambda: edge_copy(0).start())
    pl.when(has_above)(lambda: edge_copy(1).start())
    send_ratios(4)

    def wait_ratios(t):
        pl.when(has_above)(lambda: ratio_copy(t, 0).wait_recv())
        pl.when(has_below)(lambda: ratio_copy(t, 1).wait_recv())

    def merge_outlines(t):
        wait_ratios(t)
        if t == 2:
            wait_ratios(4)
        for l in range(2):
            found = {}
            for half, n, mask, value in placed_lines(t, edge_recv.at[l]):
                at = pl.ds(HALF * half, HALF)
                before = found.get((half, n))
                if before is None:
                    before = ratio_recv[t, l, n, :, at]
                found[half, n] = jnp.where(mask, value, before)
            for (half, n), value in found.items():
                ratio_recv[t, l, n, :, pl.ds(HALF * half, HALF)] = value

    pl.when(has_above)(lambda: edge_copy(0).wait_recv())
    pl.when(has_below)(lambda: edge_copy(1).wait_recv())
    wait_ratios(3)
    for l in range(2):
        for half, n, mask, value in placed_lines(3, edge_recv.at[l]):
            row, at = pl.ds(n, 1), pl.ds(HALF * half, HALF)
            last_recv[l, row, at] = jnp.where(
                mask[0:1], value[2 * l : 2 * l + 1], last_recv[l, row, at]
            )
    merge_outlines(0)
    merge_outlines(1)

    for copy in column_copies:
        copy.wait_recv()
    own_column = column[...]
    others = jnp.zeros_like(own_column)
    under = jnp.zeros_like(own_column)
    for k in range(1, n_lev):
        part = columns[k - 1]
        others = others + part
        under = under + jnp.where(k <= level, part, 0.0)
    surface_rows = own_column + others
    levels = 2 * n_lev

    def as_float(k):
        return k.astype(jnp.float32)

    for k in range(3):
        edge_level = as_float(2 * level + k)
        fraction = (edge_level + edge_level * (edge_level - 1.0) * (1.0 / (levels - 1))) * (
            0.5 / levels
        )
        if k > 0:
            under = under + thick[k - 1]
        delta[k] = under - surface_rows * fraction
    for l in range(2):
        share = (1.0 + 2.0 * as_float(2 * level + l) * (1.0 / (levels - 1))) * (0.5 / levels)
        delta[3 + l] = 1.0 / (surface_rows * share)

    def remapped(d, carried, own_ratio, ratio_above, ratio_below):
        low = d[0] * jnp.where(d[0] > 0.0, ratio_below, own_ratio[0])
        middle = d[1] * jnp.where(d[1] > 0.0, own_ratio[0], own_ratio[1])
        high = d[2] * jnp.where(d[2] > 0.0, own_ratio[1], ratio_above)
        return (carried[0] + low - middle) * d[3], (carried[1] + middle - high) * d[4]

    d = [delta[k] for k in range(5)]
    first, second = remapped(
        d,
        [last[0], last[1]],
        [last[0] * inverse[0], last[1] * inverse[1]],
        last_recv[0],
        last_recv[1],
    )
    rows = permuted(jnp.concatenate([first, second, surface_rows], axis=0), tables[1])
    last_rows[...] = rows
    for t in range(3):
        if t == 2:
            merge_outlines(2)
        pairs = []
        for n in range(NODES):
            parts = []
            for half in range(2):
                at = pl.ds(HALF * half, HALF)
                d = [delta[k, pl.ds(n, 1), at] for k in range(5)]
                carried = [state[2 * t + 1 + l, n, :, at] for l in range(2)]
                own_ratio = [carried[l] * inverse[l, pl.ds(n, 1), at] for l in range(2)]
                parts.append(
                    remapped(d, carried, own_ratio, ratio_recv[t, 0, n, :, at], ratio_recv[t, 1, n, :, at])
                )
            pairs.append(
                [jnp.concatenate([parts[0][l], parts[1][l]], axis=1) for l in range(2)]
            )
        tiles = permuted(
            jnp.concatenate([pair[l] for l in range(2) for pair in pairs], axis=0), tables[1]
        )
        for k in range(2 * NODES):
            for half in range(2):
                result[half, pl.ds(256 * t + k, 8, stride=32), :] = tiles[
                    8 * k : 8 * k + 8, HALF * half : HALF * half + HALF
                ]
    for copy in sum(first_sends + second_sends, column_copies):
        copy.wait_send()
    for t in range(5):
        pl.when(has_below)(lambda t=t: ratio_copy(t, 0).wait_send())
        pl.when(has_above)(lambda t=t: ratio_copy(t, 1).wait_send())
    pl.when(has_below)(lambda: edge_copy(0).wait_send())
    pl.when(has_above)(lambda: edge_copy(1).wait_send())


def store(result, last_rows, out, surf, sem):
    copies = [
        pltpu.make_async_copy(last_rows.at[pl.ds(32, 16)], surf, sem.at[0]),
        pltpu.make_async_copy(last_rows.at[pl.ds(0, 32)], out.at[pl.ds(768, 32)], sem.at[1]),
    ]
    for half in range(2):
        at = pl.ds(HALF * half, HALF)
        for k in range(2):
            rows = pl.ds(384 * k, 384)
            copies.append(
                pltpu.make_async_copy(
                    result.at[half, rows], out.at[rows, at], sem.at[2 + 2 * half + k]
                )
            )
    for copy in copies:
        copy.start()
    for copy in copies:
        copy.wait()


def per_device(n_elem, n_lev, tracers, layer_mass, winds, metric, neighbours):
    width = metric.shape[-1]
    f32 = jnp.float32
    tile = (NODES, 8, width)
    dma = pltpu.SemaphoreType.DMA
    scratch = [
        pltpu.VMEM((8, width), jnp.int32),
        pltpu.VMEM((2, 768, HALF), f32),
        pltpu.VMEM((144, width), f32),
        pltpu.VMEM((144, width), f32),
        pltpu.VMEM((2, width, width), jnp.bfloat16),
        pltpu.VMEM((7,) + tile, f32),
        pltpu.VMEM((7,) + tile, f32),
        pltpu.VMEM((2, 2, NODES, width), f32),
        pltpu.VMEM((2,) + tile, f32),
        pltpu.VMEM((NODES, width), f32),
        pltpu.VMEM((NODES, width), f32),
        pltpu.VMEM((NODES, width), f32),
        pltpu.VMEM((2, 2, 4, 2, 8, HALF), f32),
        pltpu.VMEM((2, 2, 4, 2, 8, HALF), f32),
        pltpu.VMEM((2, 2, 4, 1, HALF), f32),
        pltpu.VMEM((2, 2, 4, 1, HALF), f32),
        pltpu.VMEM((2, NODES, width), f32),
        pltpu.VMEM((2, NODES, width), f32),
        pltpu.VMEM((2, NODES, width), f32),
        pltpu.VMEM((NODES, width), f32),
        pltpu.VMEM((n_lev - 1, NODES, width), f32),
        pltpu.VMEM((3, 2) + tile, f32),
        pltpu.VMEM((3, 2) + tile, f32),
        pltpu.VMEM((2, NODES, width), f32),
        pltpu.VMEM((2, NODES, width), f32),
        pltpu.VMEM((2, 4, 2, 8, HALF), f32),
        pltpu.VMEM((2, 4, 2, 8, HALF), f32),
        pltpu.VMEM((5, NODES, width), f32),
        dma((2,)),
        dma((5,)),
        dma((2, 2, 8)),
        dma((2, 2, 8)),
        dma((n_lev - 1,)),
        dma((n_lev - 1,)),
        dma((5, 2)),
        dma((5, 2)),
        dma((2,)),
        dma((2,)),
    ]
    result, last_rows = pl.pallas_call(
        functools.partial(kernel, n_elem, n_lev),
        out_shape=(
            jax.ShapeDtypeStruct((2, 768, HALF), f32),
            jax.ShapeDtypeStruct((3 * NODES, width), f32),
        ),
        in_specs=[pl.BlockSpec(memory_space=pltpu.HBM)] * 5,
        out_specs=(pl.BlockSpec(memory_space=pltpu.VMEM),) * 2,
        scratch_shapes=scratch,
        compiler_params=pltpu.CompilerParams(
            collective_id=0, has_side_effects=True, vmem_limit_bytes=24 * 1024 * 1024
        ),
        name="transport",
    )(
        *[
            pltpu.with_memory_space_constraint(x, pltpu.HBM)
            for x in (
                tracers.reshape(-1, width),
                layer_mass.reshape(-1, width),
                winds.reshape(-1, width),
                metric,
                jnp.transpose(neighbours),
            )
        ]
    )
    out, surface = pl.pallas_call(
        store,
        out_shape=(
            jax.ShapeDtypeStruct((800, width), f32),
            jax.ShapeDtypeStruct((NODES, width), f32),
        ),
        in_specs=[pl.BlockSpec(memory_space=pltpu.VMEM)] * 2,
        out_specs=(pl.BlockSpec(memory_space=pltpu.HBM),) * 2,
        scratch_shapes=[dma((6,))],
        compiler_params=pltpu.CompilerParams(vmem_limit_bytes=24 * 1024 * 1024),
        name="store",
    )(result, last_rows)
    return out.reshape(tracers.shape), surface


def solution(mesh):
    placed = (
        P(None, "lev", None, ("members", "elem")),
        P("lev", None, ("members", "elem")),
        P(None, "lev", None, ("members", "elem")),
        P(None, "elem"),
        P("elem", None),
    )
    return jax.shard_map(
        functools.partial(per_device, mesh.shape["elem"], mesh.shape["lev"]),
        mesh=mesh,
        in_specs=placed,
        out_specs=(P(None, "lev", None, ("members", "elem")), P(None, ("members", "elem"))),
        check_vma=False,
    )
```
